256 devices in a mesh: dp: 2 (over y_lo), seq: 32 (over z, y_hi, core), chan: 4 (over x).
Axes of the slice: x: 4, y: 4 (y_hi: 2, y_lo: 2; y = y_hi * 2 + y_lo), z: 8, core: 2. Of those that a mesh axis runs over, the one named last changes fastest.
Arguments:
- layer_input: bfloat16 [2, 4096, 2560], P('dp', ('seq', 'chan')), may hold values from -24 to 24
- inner_weight: bfloat16 [2560, 2560], P(None, 'chan'), may hold values from -0.125 to 0.125
- mixer_weight: bfloat16 [2560, 256], replicated, may hold values from -0.01171875 to 0.01171875
- step_weight: bfloat16 [2560, 40], P(None, 'chan'), may hold values from -0.125 to 0.125
- conv_inner: float32 [4, 2560], P(None, 'chan'), may hold values from -3 to 3
- conv_mixer: float32 [4, 256], replicated, may hold values from -3 to 3
- step_bias: float32 [40], P('chan'), may hold values from -2 to 1
- decay_log: float32 [40], P('chan'), as said below
- skip_gain: float32 [40], P('chan'), may hold values from 0.5 to 1.5
- output_grad: bfloat16 [2, 4096, 2560], P('dp', 'seq', 'chan'), may hold values from -6 to 6
Outputs:
- input_grad: bfloat16 [2, 4096, 2560], P('dp', ('seq', 'chan'))
- inner_weight_grad: float32 [2560, 2560], P(('dp', 'seq'), 'chan')
- mixer_weight_grad: float32 [2560, 256], P(('dp', 'seq', 'chan'))
- step_weight_grad: float32 [2560, 40], P(('dp', 'seq'), 'chan')
The draws below stay inside these ranges and needn't reach their ends.
Inputs may be any that keep to these rules, and one draw needn't show every extreme that they name: exp(decay_log) is at least 0.2 / 4096.
All inputs are finite; a program needn't handle non-finite values.
Results may differ from the reference program's by a relative error of at most 0.014.
Values may be sent and summed in bfloat16 or wider, within the bound.
A program may use at most 128 MiB of HBM per device.

```python
import math
import jax
import jax.numpy as jnp
from jax import lax

D = 2560
HEADS = 40
HDIM = 64
STATE = 128
KW = 4
BATCH = 2
LENGTH = 4096
TOKENS = 8192
INNER = 2560


def draw_decay_log(key, part):
    base = jax.random.fold_in(key, 71)
    order_key, slow_key, fast_key = jax.random.split(base, 3)
    ranks = jax.random.permutation(order_key, HEADS)
    slow_count = HEADS // 2
    is_slow = ranks < slow_count
    slow_rate = jnp.exp(jax.random.uniform(slow_key, (HEADS,), jnp.float32, jnp.log(0.2), jnp.log(2.0))) / LENGTH
    fast_rate = jnp.exp(jax.random.uniform(fast_key, (HEADS,), jnp.float32, jnp.log(0.02), jnp.log(0.06)))
    return jnp.log(jnp.where(is_slow, slow_rate, fast_rate)).astype(jnp.float32)


def spiked(entries, own_key, source, target, parts, factor):
    def block_of(dim):
        return (jnp.arange(entries.shape[dim]) // (entries.shape[dim] // parts)).reshape((-1,) + (1,) * (entries.ndim - 1 - dim))

    first = jax.random.permutation(own_key, parts)[block_of(target)]
    other_side = (block_of(target) + parts // 2) % parts
    return jnp.where((block_of(source) == first) | (block_of(source) == other_side), factor * entries, entries)


def shard_levels(key, dims, cuts, least, top_value):
    gain = 1.0
    for position, shards_of in cuts:
        steps = jax.random.uniform(jax.random.fold_in(jax.random.fold_in(key, 6), position), (shards_of,), jnp.float32, least / len(cuts), top_value / len(cuts))
        gain = gain * jnp.repeat(jnp.exp(steps), dims[position] // shards_of).reshape((-1,) + (1,) * (len(dims) - 1 - position))
    return gain


def gaussian(stream_key, shape, width, most, cuts=(), held_as=jnp.bfloat16):
    values = jax.random.normal(stream_key, shape, jnp.float32) * width
    if len(cuts) > 0:
        values = shard_levels(stream_key, shape, cuts, -0.22, 0.18) * values
    return jnp.clip(values, min=-most, max=most).astype(held_as)


def noise_with(own_key, dims, width, most, cuts, heavy, kind=jnp.bfloat16):
    drawn = width * jax.random.normal(own_key, dims, jnp.float32)
    if cuts:
        drawn = drawn * shard_levels(own_key, dims, cuts, -0.22, 0.18)
    return jnp.clip(spiked(drawn, jax.random.fold_in(own_key, 3), *heavy), -most, most).astype(kind)


def setup_inputs(seed: int = 0) -> dict:
    splits = jax.random.split(jax.random.key(seed), 11)
    return {
        "layer_input": noise_with(splits[0], (BATCH, LENGTH, D), 1.0, 24.0, ((0, 2), (1, 128)), (1, 2, 128, 5.5)),
        "inner_weight": gaussian(splits[1], (D, INNER), D ** -0.5, 0.125, ((1, 4),)),
        "mixer_weight": gaussian(splits[2], (D, 2 * STATE), (0.1 / D ** 0.5), 0.01171875),
        "step_weight": gaussian(splits[3], (D, HEADS), D ** -0.5, 0.125, ((1, 4),)),
        "conv_inner": gaussian(splits[4], (KW, INNER), KW ** -0.5, 3.0, ((1, 4),), jnp.float32),
        "conv_mixer": gaussian(splits[5], (KW, 2 * STATE), KW ** -0.5, 3.0, (), jnp.float32),
        "step_bias": jnp.clip(-2.0 + 3.0 * jax.random.uniform(splits[6], (HEADS,), jnp.float32) ** shard_levels(splits[6], (HEADS,), ((0, 4),), -0.2, 0.2), -2.0, 1.0),
        "decay_log": draw_decay_log(jax.random.fold_in(splits[10], 71), 0),
        "skip_gain": jnp.clip(0.5 + 1.0 * jax.random.uniform(splits[8], (HEADS,), jnp.float32) ** shard_levels(splits[8], (HEADS,), ((0, 4),), -0.2, 0.2), 0.5, 1.5),
        "output_grad": gaussian(splits[9], (BATCH, LENGTH, INNER), 1.0, 6.0, ((0, 2), (1, 32), (2, 4))),
    }


block_tokens = 256

def conv_silu(inputs, history, kernel):
    length = inputs.shape[0]
    padded = jnp.concatenate([history, inputs], axis=0)
    summed = kernel[0][None, :] * padded[0:length]
    for offset in range(1, kernel.shape[0]):
        summed = summed + kernel[offset][None, :] * padded[offset:offset + length]
    return jax.nn.silu(summed)

def activations(inner_proj, mixer_proj, step_raw, inner_hist, mixer_hist, conv_inner, conv_mixer, step_bias, decay_log):
    length = inner_proj.shape[0]
    head_count = step_bias.shape[0]
    state_width = mixer_proj.shape[1] // 2
    inner_act = conv_silu(inner_proj, inner_hist, conv_inner).reshape(length, head_count, -1)
    mixer_act = conv_silu(mixer_proj, mixer_hist, conv_mixer)
    step_size = jax.nn.softplus(step_raw + step_bias[None, :])
    log_decay = -step_size * jnp.exp(decay_log)[None, :]
    return (inner_act, mixer_act[:, :state_width], mixer_act[:, state_width:], step_size, log_decay)

def spanned_scan(inner_act, input_mix, output_mix, step_size, log_decay, skip_gain, initial):
    length, head_count, head_dim = inner_act.shape
    block_len = min(block_tokens, length)
    blocks = length // block_len
    highest = lax.Precision.HIGHEST

    def to_blocks(values):
        return values.reshape((blocks, block_len) + values.shape[1:])

    def advance(carry_state, pieces):
        part_inner, part_input, part_output, part_step, part_decay = pieces
        cumulative = jnp.cumsum(part_decay, axis=0)
        scores = jnp.dot(part_output, part_input.T, precision=highest)
        causal = (jnp.arange(block_len)[:, None] >= jnp.arange(block_len)[None, :])[:, :, None]
        spread = cumulative[:, None, :] - cumulative[None, :, :]
        weights = jnp.where(causal, jnp.exp(jnp.where(causal, spread, 0.0)), 0.0)
        weights = weights * scores[:, :, None] * part_step[None, :, :]
        within = jnp.einsum('ijh,jhp->ihp', weights, part_inner, precision=highest)
        carried = jnp.exp(cumulative)[:, :, None] * jnp.einsum('in,hpn->ihp', part_output, carry_state, precision=highest)
        result = within + carried + skip_gain[None, :, None] * part_inner
        tail_weight = jnp.exp(cumulative[-1][None, :] - cumulative) * part_step
        update_term = jnp.einsum('jh,jhp,jn->hpn', tail_weight, part_inner, part_input, precision=highest)
        carry_state = jnp.exp(cumulative[-1])[:, None, None] * carry_state + update_term
        return (carry_state, result)
    final, results = lax.scan(jax.checkpoint(advance), initial, (to_blocks(inner_act), to_blocks(input_mix), to_blocks(output_mix), to_blocks(step_size), to_blocks(log_decay)))
    return (results.reshape(length, head_count, head_dim), final)

def contract_rows(left_rows, right_rows):
    return lax.dot_general(left_rows, right_rows, (((0,), (0,)), ((), ())), preferred_element_type=jnp.float32)

def project_back(gradient, weight):
    return lax.dot_general(gradient, weight, (((1,), (1,)), ((), ())), preferred_element_type=jnp.float32)

def reference(layer_input, inner_weight, mixer_weight, step_weight, conv_inner, conv_mixer, step_bias, decay_log, skip_gain, output_grad):
    history_len = KW - 1
    highest = lax.Precision.HIGHEST
    inner_acc = jnp.zeros((D, INNER), jnp.float32)
    mixer_acc = jnp.zeros((D, 2 * STATE), jnp.float32)
    step_acc = jnp.zeros((D, HEADS), jnp.float32)
    input_grads = []
    zero_inner = jnp.zeros((history_len, INNER), jnp.float32)
    zero_mixer = jnp.zeros((history_len, 2 * STATE), jnp.float32)
    initial = jnp.zeros((HEADS, HDIM, STATE), jnp.float32)
    for batch_row in range(BATCH):
        tokens = layer_input[batch_row]
        inner_proj = jnp.dot(tokens, inner_weight, preferred_element_type=jnp.float32).astype(jnp.bfloat16)
        mixer_proj = jnp.dot(tokens, mixer_weight, preferred_element_type=jnp.float32).astype(jnp.bfloat16)
        step_raw = jnp.dot(tokens, step_weight, preferred_element_type=jnp.float32)
        inner_wide = lax.optimization_barrier(inner_proj).astype(jnp.float32)
        mixer_wide = lax.optimization_barrier(mixer_proj).astype(jnp.float32)

        def layer(inner_in, mixer_in, step_in):
            acts = activations(inner_in, mixer_in, step_in, zero_inner, zero_mixer, conv_inner, conv_mixer, step_bias, decay_log)
            result, final = spanned_scan(acts[0], acts[1], acts[2], acts[3], acts[4], skip_gain, initial)
            return result.reshape(LENGTH, INNER)
        unused, pull = jax.vjp(layer, inner_wide, mixer_wide, step_raw)
        grad_inner, grad_mixer, grad_step = pull(output_grad[batch_row].astype(jnp.float32))
        grad_inner = grad_inner.astype(jnp.bfloat16)
        grad_step = grad_step.astype(jnp.bfloat16)
        summed = project_back(grad_inner, inner_weight) + project_back(grad_step, step_weight)
        summed = summed + lax.dot_general(grad_mixer, mixer_weight.astype(jnp.float32), (((1,), (1,)), ((), ())), precision=highest)
        input_grads.append(summed.astype(jnp.bfloat16))
        inner_acc = inner_acc + contract_rows(tokens, grad_inner)
        step_acc = step_acc + contract_rows(tokens, grad_step)
        mixer_acc = mixer_acc + lax.dot_general(tokens.astype(jnp.float32), grad_mixer, (((0,), (0,)), ((), ())), precision=highest)
    norm_factor = 1.0 / math.sqrt(TOKENS)
    return (jnp.stack(input_grads, axis=0), inner_acc * norm_factor, mixer_acc * norm_factor, step_acc * norm_factor)
```

```python
import functools
import math

import jax
import jax.numpy as jnp
from jax import lax
from jax.experimental import pallas as pl
from jax.experimental.pallas import tpu as pltpu
from jax.sharding import Mesh
from jax.sharding import PartitionSpec as P

D = 2560
HDIM = 64
HEADS = 5
INNER = HEADS * HDIM
STATE = 128
TOK = 256
PRE = 16
EXT = TOK + PRE
NZ = 8
ROWS = 80
CHUNK = 48
F32 = jnp.float32
BF16 = jnp.bfloat16
SEQ = ("seq_0", "seq_1", "seq_2")
DP_SEQ = ("dp", "seq_0", "seq_1", "seq_2")
SEQ_CHAN = ("seq_0", "seq_1", "seq_2", "chan")
DP_SEQ_CHAN = ("dp", "seq_0", "seq_1", "seq_2", "chan")
MESH = pl.DeviceIdType.MESH
VM = pl.BlockSpec(memory_space=pltpu.VMEM)
LIMIT = 60 * 1024 * 1024


def roll(v, shift):
    return pltpu.roll(v, shift % v.shape[0], 0)


def mm(a, b):
    return jnp.dot(a, b, preferred_element_type=F32)


def mm_t(a, b):
    return lax.dot_general(a, b, (((1,), (1,)), ((), ())), preferred_element_type=F32)


def t_mm(a, b):
    return lax.dot_general(a, b, (((0,), (0,)), ((), ())), preferred_element_type=F32)


def exact(a, b):
    return jnp.dot(a, b, preferred_element_type=F32, precision=lax.Precision.HIGHEST)


def iota(shape, dim):
    return lax.broadcasted_iota(jnp.int32, shape, dim)


def one_hot(cond):
    return jnp.where(cond, 1.0, 0.0).astype(F32)


def head_expand():
    return one_hot(iota((128, INNER), 1) // HDIM == iota((128, INNER), 0))


def head_sum():
    return one_hot(iota((INNER, 128), 0) // HDIM == iota((INNER, 128), 1))


def head_pick(core):
    return one_hot(
        (iota((10, 128), 0) == iota((10, 128), 1) + HEADS * core) & (iota((10, 128), 1) < HEADS)
    )


def half_of(v, core):
    return jnp.where(core == 0, v[:, :INNER], v[:, INNER:])


def conv(v, k):
    return k[3:4] * v + k[2:3] * roll(v, 1) + k[1:2] * roll(v, 2) + k[0:1] * roll(v, 3)


def conv_back(g, k):
    return k[3:4] * g + k[2:3] * roll(g, -1) + k[1:2] * roll(g, -2) + k[0:1] * roll(g, -3)


def gather_kernel(piece, og, xe, ogx, local_sem, ssem, rsem, tsem):
    z, yh, c, x = (lax.axis_index(a) for a in SEQ_CHAN)
    right, left = lax.rem(x + 1, 4), lax.rem(x + 3, 4)
    sib = 1 - c
    q = z * 2 + yh
    nq, pq = lax.rem(q + 1, 2 * NZ), lax.rem(q + 2 * NZ - 1, 2 * NZ)
    barrier = pltpu.get_barrier_semaphore()

    def tell(**where):
        pl.semaphore_signal(barrier, inc=1, device_id=where, device_id_type=MESH)

    tell(chan=right)
    tell(chan=left)
    tell(seq_2=sib)

    @pl.when(c == 1)
    def _():
        tell(seq_0=pq // 2, seq_1=lax.rem(pq, 2), chan=3)

    pl.semaphore_wait(barrier, jnp.where((c == 1) & (x == 3), 7, 3))

    def slot(core, chan, half=None):
        base = PRE + (core * 4 + chan) * 32
        if half is None:
            return xe.at[pl.ds(pl.multiple_of(base, 16), 32), :]
        return xe.at[pl.ds(pl.multiple_of(base + 16 * half, 16), 16), :]

    def copy(src, dst, k, **where):
        return pltpu.make_async_remote_copy(
            src_ref=src, dst_ref=dst, send_sem=ssem.at[k], recv_sem=rsem.at[k],
            device_id=where, device_id_type=MESH,
        )

    def half(h):
        return piece.at[pl.ds(16 * h, 16), :]

    own = pltpu.make_async_copy(piece, slot(c, x), local_sem.at[0])
    own_og = pltpu.make_async_copy(og, ogx.at[c], local_sem.at[1])
    r0 = copy(half(0), slot(c, x, 0), 0, chan=right)
    l1 = copy(half(1), slot(c, x, 1), 1, chan=left)
    r1 = copy(half(1), slot(c, x, 1), 2, chan=right)
    l0 = copy(half(0), slot(c, x, 0), 3, chan=left)
    sp = copy(piece, slot(c, x), 4, seq_2=sib)
    so = copy(og, ogx.at[c], 5, seq_2=sib)
    for d in (r0, l1):
        d.start()

    def tails(chan):
        return pltpu.make_async_remote_copy(
            src_ref=half(1), dst_ref=xe.at[pl.ds(0, 16), :], send_sem=tsem.at[chan],
            recv_sem=rsem.at[6],
            device_id={"seq_0": nq // 2, "seq_1": lax.rem(nq, 2), "chan": chan},
            device_id_type=MESH,
        )

    @pl.when((c == 1) & (x == 3))
    def _():
        for chan in range(4):
            tails(chan).start()

    for d in (r1, l0, sp, so):
        d.start()
    own.start()
    own_og.start()
    far = lax.rem(x + 2, 4)
    in_r0 = copy(half(0), slot(c, left, 0), 0, chan=right)
    in_r1 = copy(half(1), slot(c, left, 1), 2, chan=right)
    in_l1 = copy(half(1), slot(c, right, 1), 1, chan=left)
    in_l0 = copy(half(0), slot(c, right, 0), 3, chan=left)
    rr = copy(slot(c, left, 0), slot(c, left, 0), 7, chan=right)
    ll = copy(slot(c, right, 1), slot(c, right, 1), 8, chan=left)
    in_r0.wait_recv()
    rr.start()
    in_l1.wait_recv()
    ll.start()
    in_r1.wait_recv()
    s_left = copy(slot(c, left), slot(c, left), 9, seq_2=sib)
    s_left.start()
    in_l0.wait_recv()
    s_right = copy(slot(c, right), slot(c, right), 10, seq_2=sib)
    s_right.start()
    tail_on = copy(xe.at[pl.ds(0, 16), :], xe.at[pl.ds(0, 16), :], 12, seq_2=sib)

    @pl.when(c == 1)
    def _():
        tails(0).wait_recv()
        tail_on.start()

    in_rr = copy(half(0), slot(c, far, 0), 7, chan=right)
    in_ll = copy(half(1), slot(c, far, 1), 8, chan=left)
    in_rr.wait_recv()
    in_ll.wait_recv()
    s_far = copy(slot(c, far), slot(c, far), 11, seq_2=sib)
    s_far.start()
    copy(piece, slot(sib, x), 4, seq_2=sib).wait_recv()
    copy(og, ogx.at[sib], 5, seq_2=sib).wait_recv()
    copy(piece, slot(sib, left), 9, seq_2=sib).wait_recv()
    copy(piece, slot(sib, right), 10, seq_2=sib).wait_recv()
    copy(piece, slot(sib, far), 11, seq_2=sib).wait_recv()

    @pl.when(c == 0)
    def _():
        tail_on.wait_recv()

    for d in (r0, l1, r1, l0, sp, so, rr, ll, s_left, s_right, s_far):
        d.wait_send()

    @pl.when(c == 1)
    def _():
        tail_on.wait_send()

    @pl.when((c == 1) & (x == 3))
    def _():
        for chan in range(4):
            tails(chan).wait_send()

    own.wait()
    own_og.wait()


def gather(piece, og):
    return pl.pallas_call(
        gather_kernel,
        out_shape=(
            jax.ShapeDtypeStruct((EXT, D), BF16),
            jax.ShapeDtypeStruct((2, TOK // 2, 2 * INNER), BF16),
        ),
        in_specs=[VM, VM],
        out_specs=(VM, VM),
        scratch_shapes=[
            pltpu.SemaphoreType.DMA((2,)),
            pltpu.SemaphoreType.DMA((13,)),
            pltpu.SemaphoreType.DMA((13,)),
            pltpu.SemaphoreType.DMA((4,)),
        ],
        compiler_params=pltpu.CompilerParams(collective_id=0, has_side_effects=True),
        name="gather",
    )(piece, og)


def forward_kernel(
    xe, ogx, wi, wm, ws, ci, cm, bias, dlog,
    xa_o, zi_o, zm_o, dt_o, cum_o, sr_o, og_o, wih_o, send_o,
):
    z, yh, c = (lax.axis_index(a) for a in SEQ)
    flag = jnp.where(z * 2 + yh == 0, 0.0, 1.0).astype(F32)
    pick = head_pick(c)
    wih = half_of(wi[...], c)
    wih_o[...] = wih
    xv = xe[...]
    keep = jnp.where(iota((EXT, 1), 0) < PRE, flag, 1.0)

    def masked(v):
        return jnp.where(keep > 0.0, v.astype(BF16).astype(F32), 0.0)

    pi = masked(mm(xv, wih))
    pm = masked(mm(xv, wm[...]))
    sr = exact(mm(xv, ws[...])[PRE:], pick)
    zi = conv(pi, half_of(ci[...], c))[PRE:]
    zm = conv(pm, cm[...])[PRE:]
    xa = zi * jax.nn.sigmoid(zi)
    ma = zm * jax.nn.sigmoid(zm)
    srb = sr + exact(bias[...], pick)
    dt = jnp.maximum(srb, 0.0) + jnp.log1p(jnp.exp(-jnp.abs(srb)))
    rate = exact(jnp.exp(dlog[...]), pick)
    a = -dt * rate
    tri = one_hot(iota((TOK, TOK), 0) >= iota((TOK, TOK), 1))
    cum = exact(tri, a)
    tot = cum[TOK - 1 : TOK]
    og = half_of(ogx[...].reshape(TOK, 2 * INNER), c)
    ex = head_expand()
    xt = (xa * exact(dt * jnp.exp(tot - cum), ex)).astype(BF16)
    yt = (og.astype(F32) * exact(jnp.exp(cum), ex)).astype(BF16)
    f_loc = t_mm(xt, ma[:, :STATE].astype(BF16))
    g_loc = t_mm(yt, ma[:, STATE:].astype(BF16))
    diag = jnp.where(iota((8, 128), 0) == iota((8, 128), 1), tot, 0.0)
    dm = exact(diag, jnp.ones((128, 128), F32))
    hi = dm.astype(BF16).astype(F32)
    drow = jnp.where(iota((8, 128), 1) < 64, hi, dm - hi)
    for zz in range(NZ):
        for which, v in ((0, f_loc), (1, g_loc)):
            rows = [v[h * HDIM + zz * 8 : h * HDIM + zz * 8 + 8] for h in range(HEADS)]
            send_o[zz * 2 + which] = jnp.concatenate(rows + [drow], axis=0).astype(BF16)
    xa_o[...] = xa
    zi_o[...] = zi
    zm_o[...] = zm
    dt_o[...] = dt
    cum_o[...] = cum
    sr_o[...] = srb
    og_o[...] = og


def forward(*args):
    return pl.pallas_call(
        forward_kernel,
        out_shape=(
            jax.ShapeDtypeStruct((TOK, INNER), F32),
            jax.ShapeDtypeStruct((TOK, INNER), F32),
            jax.ShapeDtypeStruct((TOK, 2 * STATE), F32),
            jax.ShapeDtypeStruct((TOK, 128), F32),
            jax.ShapeDtypeStruct((TOK, 128), F32),
            jax.ShapeDtypeStruct((TOK, 128), F32),
            jax.ShapeDtypeStruct((TOK, INNER), BF16),
            jax.ShapeDtypeStruct((D, INNER), BF16),
            jax.ShapeDtypeStruct((2 * NZ, CHUNK, STATE), BF16),
        ),
        in_specs=[VM] * 9,
        out_specs=(VM,) * 9,
        compiler_params=pltpu.CompilerParams(vmem_limit_bytes=LIMIT),
        name="forward",
    )(*args)


def state_kernel(send, out, recv, back, local_sem, s1, r1, s2, r2):
    z, yh = lax.axis_index("seq_0"), lax.axis_index("seq_1")
    n = 2 * NZ
    me = z * 2 + yh
    barrier = pltpu.get_barrier_semaphore()

    def at(q):
        return {"seq_0": q // 2, "seq_1": lax.rem(q, 2)}

    for off in range(1, n):
        pl.semaphore_signal(
            barrier, inc=1, device_id=at(lax.rem(me + off, n)), device_id_type=MESH
        )
    pl.semaphore_wait(barrier, n - 1)

    def push(src, dst, ss, rs, off):
        to = lax.rem(me + off, n)
        return pltpu.make_async_remote_copy(
            src_ref=src.at[to], dst_ref=dst.at[me], send_sem=ss.at[off], recv_sem=rs.at[off],
            device_id=at(to), device_id_type=MESH,
        )

    def pull(src, dst, ss, rs, off):
        origin = lax.rem(me + n - off, n)
        return pltpu.make_async_remote_copy(
            src_ref=src.at[origin], dst_ref=dst.at[origin], send_sem=ss.at[off],
            recv_sem=rs.at[off], device_id=at(origin), device_id_type=MESH,
        )

    first = [push(send, recv, s1, r1, off) for off in range(1, n)]
    for d in first:
        d.start()
    own = pltpu.make_async_copy(send.at[me], recv.at[me], local_sem.at[0])
    own.start()
    own.wait()
    for off in range(1, n):
        pull(send, recv, s1, r1, off).wait_recv()
    run = jnp.zeros((HEADS * 8, STATE), F32)
    for j in range(n):
        k = jnp.where(yh == 0, j, n - 1 - j)
        got = recv[k].astype(F32)
        rows = got[HEADS * 8 :]
        rows = rows + pltpu.roll(rows, 64, 1)
        decay = jnp.exp(rows)
        back[k] = jnp.concatenate([run, rows], axis=0).astype(BF16)
        wide = jnp.concatenate(
            [jnp.broadcast_to(decay[h : h + 1], (8, STATE)) for h in range(HEADS)], axis=0
        )
        run = wide * run + got[: HEADS * 8]
    second = [push(back, out, s2, r2, off) for off in range(1, n)]
    for d in second:
        d.start()
    own = pltpu.make_async_copy(back.at[me], out.at[me], local_sem.at[1])
    own.start()
    own.wait()
    for off in range(1, n):
        pull(back, out, s2, r2, off).wait_recv()
    for d in first + second:
        d.wait_send()


def states(send):
    n = 2 * NZ
    return pl.pallas_call(
        state_kernel,
        out_shape=jax.ShapeDtypeStruct((n, CHUNK, STATE), BF16),
        in_specs=[VM],
        out_specs=VM,
        scratch_shapes=[
            pltpu.VMEM((n, CHUNK, STATE), BF16),
            pltpu.VMEM((n, CHUNK, STATE), BF16),
            pltpu.SemaphoreType.DMA((2,)),
            pltpu.SemaphoreType.DMA((n,)),
            pltpu.SemaphoreType.DMA((n,)),
            pltpu.SemaphoreType.DMA((n,)),
            pltpu.SemaphoreType.DMA((n,)),
        ],
        compiler_params=pltpu.CompilerParams(collective_id=1, has_side_effects=True),
        name="states",
    )(send)


def backward_kernel(
    xa_r, zi_r, zm_r, dt_r, cum_r, sr_r, og_r, st, ci, cm, dlog, skip,
    gi_o, gm_o, ds_o, gmt_o,
):
    z, yh, c = (lax.axis_index(a) for a in SEQ)
    flag = jnp.where(z * 2 + yh == 0, 0.0, 1.0).astype(F32)
    pick = head_pick(c)
    ex, hs = head_expand(), head_sum()
    xa, zi, zm = xa_r[...], zi_r[...], zm_r[...]
    dt, cum = dt_r[...], cum_r[...]
    og = og_r[...]
    dy = og.astype(F32)
    rate = exact(jnp.exp(dlog[...]), pick)
    skp = exact(skip[...], pick)
    tot = cum[TOK - 1 : TOK]
    ecum = exact(jnp.exp(cum), ex)
    etail = exact(jnp.exp(tot - cum), ex)
    dte = exact(dt, ex)

    def collect(which):
        blocks = [st[2 * zz + which].astype(F32) for zz in range(NZ)]
        rows = [blocks[zz][h * 8 : h * 8 + 8] for h in range(HEADS) for zz in range(NZ)]
        return jnp.concatenate(rows, axis=0)

    h0, ge = collect(0), collect(1)
    h0b, geb = h0.astype(BF16), ge.astype(BF16)
    sz = jax.nn.sigmoid(zm)
    ma = zm * sz
    bm, cmx = ma[:, :STATE].astype(BF16), ma[:, STATE:].astype(BF16)
    xdt = xa * dte
    xdtb = xdt.astype(BF16)
    xdtf = xdtb.astype(F32)
    scores = mm_t(cmx, bm)
    causal = iota((TOK, TOK), 0) >= iota((TOK, TOK), 1)
    cumt = cum.T
    dscore = jnp.zeros((TOK, TOK), F32)
    ys, us = [], []
    for h in range(HEADS):
        cols = slice(h * HDIM, (h + 1) * HDIM)
        decay = jnp.exp(jnp.where(causal, cum[:, h : h + 1] - cumt[h : h + 1, :], -1e30))
        m = (decay * scores).astype(BF16)
        ys.append(mm(m, xdtb[:, cols]))
        us.append(t_mm(m, og[:, cols]))
        dscore = dscore + decay * mm_t(og[:, cols], xdtb[:, cols])
    y = jnp.concatenate(ys, axis=1) + ecum * mm_t(cmx, h0b)
    ug = etail * mm_t(bm, geb)
    u = jnp.concatenate(us, axis=1) + ug
    dxa = dte * u + exact(skp, ex) * dy
    ddt = exact(xa * u, hs)
    dcum = exact(dy * y - xdtf * u, hs)
    e_sum = jnp.sum(exact(xdtf * ug, hs), axis=0, keepdims=True)
    hg = exact(
        jnp.ones((8, STATE), F32), (h0 * ge).T
    )
    carry = jnp.exp(tot) * exact(hg, hs)[0:1]
    upper = one_hot(iota((TOK, TOK), 0) <= iota((TOK, TOK), 1))
    da = exact(upper, dcum) + e_sum + carry
    dsr = (ddt - rate * da) * jax.nn.sigmoid(sr_r[...])
    dsb = dscore.astype(BF16)
    d_out = mm(dsb, bm) + mm((dy * ecum).astype(BF16), h0b)
    d_in = t_mm(dsb, cmx) + mm((xdt * etail).astype(BF16), geb)
    gm = jnp.concatenate([d_in, d_out], axis=1) * (sz * (1.0 + zm * (1.0 - sz)))
    si = jax.nn.sigmoid(zi)
    gi = dxa * (si * (1.0 + zi * (1.0 - si)))
    keep = jnp.where(iota((EXT, 1), 0) < PRE, flag, 1.0)

    def back(g, k):
        g = jnp.concatenate([jnp.zeros((PRE, g.shape[1]), F32), g], axis=0)
        return jnp.where(keep > 0.0, conv_back(g, k), 0.0).astype(BF16)

    gi_o[...] = back(gi, half_of(ci[...], c))
    gme = back(gm, cm[...])
    gm_o[...] = gme
    ds_o[...] = jnp.concatenate([jnp.zeros((PRE, 128), F32), dsr], axis=0).astype(BF16)
    eye = one_hot(iota((EXT, EXT), 0) == iota((EXT, EXT), 1)).astype(BF16)
    gmt = t_mm(gme, eye).astype(BF16)
    for j in range(8):
        gmt_o[j] = gmt[j * 32 : j * 32 + 32]


def backward(*args):
    return pl.pallas_call(
        backward_kernel,
        out_shape=(
            jax.ShapeDtypeStruct((EXT, INNER), BF16),
            jax.ShapeDtypeStruct((EXT, 2 * STATE), BF16),
            jax.ShapeDtypeStruct((EXT, 128), BF16),
            jax.ShapeDtypeStruct((8, 32, EXT), BF16),
        ),
        in_specs=[VM] * 12,
        out_specs=(VM,) * 4,
        compiler_params=pltpu.CompilerParams(vmem_limit_bytes=LIMIT),
        name="backward",
    )(*args)


def mix_kernel(src, out, local_sem, ss, rs):
    c, x = lax.axis_index("seq_2"), lax.axis_index("chan")
    me = c * 4 + x
    barrier = pltpu.get_barrier_semaphore()

    def at(j):
        return {"seq_2": j // 4, "chan": lax.rem(j, 4)}

    for off in range(1, 8):
        pl.semaphore_signal(
            barrier, inc=1, device_id=at(lax.rem(me + off, 8)), device_id_type=MESH
        )
    pl.semaphore_wait(barrier, 7)
    sends = []
    for off in range(1, 8):
        to = lax.rem(me + off, 8)
        d = pltpu.make_async_remote_copy(
            src_ref=src.at[to], dst_ref=out.at[me], send_sem=ss.at[off], recv_sem=rs.at[off],
            device_id=at(to), device_id_type=MESH,
        )
        d.start()
        sends.append(d)
    own = pltpu.make_async_copy(src.at[me], out.at[me], local_sem)
    own.start()
    own.wait()
    for off in range(1, 8):
        origin = lax.rem(me + 8 - off, 8)
        pltpu.make_async_remote_copy(
            src_ref=src.at[origin], dst_ref=out.at[origin], send_sem=ss.at[off],
            recv_sem=rs.at[off], device_id=at(origin), device_id_type=MESH,
        ).wait_recv()
    for d in sends:
        d.wait_send()


def mix(src):
    return pl.pallas_call(
        mix_kernel,
        out_shape=jax.ShapeDtypeStruct((8, 32, EXT), BF16),
        in_specs=[VM],
        out_specs=VM,
        scratch_shapes=[
            pltpu.SemaphoreType.DMA(()),
            pltpu.SemaphoreType.DMA((8,)),
            pltpu.SemaphoreType.DMA((8,)),
        ],
        compiler_params=pltpu.CompilerParams(collective_id=2, has_side_effects=True),
        name="mix",
    )(src)


def product_kernel(norm, xe, gi_r, gm_r, ds_r, mix_r, wih, wm, ws, ra_o, rb_o, p_o, pb_o):
    c = lax.axis_index("seq_2")
    total = jnp.zeros((32, EXT), F32)
    for j in range(8):
        total = total + mix_r[j].astype(F32)
    place_mix = one_hot(iota((32, 128), 1) == iota((32, 128), 0) + 64).astype(BF16)
    place_step = one_hot(
        (iota((128, 128), 1) == iota((128, 128), 0) + 96) & (iota((128, 128), 0) < HEADS)
    ).astype(BF16)
    gi = gi_r[...]
    ds = ds_r[...]
    last = t_mm(total.astype(BF16), place_mix) + mm(ds, place_step)
    last = last + jnp.concatenate([gi[:, 256:].astype(F32), jnp.zeros((EXT, 64), F32)], axis=1)
    rhs = jnp.concatenate([gi[:, :256], last.astype(BF16)], axis=1)
    for b in range(4):
        r = (t_mm(xe[:, b * 640 : (b + 1) * 640], rhs) * norm).astype(BF16)
        for g in range(8):
            dp, zz, yh = b // 2, (b % 2) * 4 + g // 2, g % 2
            block = r[g * ROWS : (g + 1) * ROWS]
            ra_o[zz, yh * 2 + dp] = block[:, :128]
            rb_o[yh * 2 + dp, zz] = block[:, 128:]
    pick = head_pick(c).astype(BF16)
    ds10 = mm_t(ds, pick).astype(BF16)
    gm = gm_r[...]
    for b in range(4):
        rows = slice(b * 640, (b + 1) * 640)
        part = mm_t(gi, wih[rows]) + mm_t(gm, wm[rows]) + mm_t(ds10, ws[rows])
        part = part.astype(BF16)
        pb_o[:, rows] = part[:PRE]
        for j in range(8):
            p_o[j, :, rows] = part[PRE + j * 32 : PRE + j * 32 + 32]


def products(norm, *args):
    return pl.pallas_call(
        functools.partial(product_kernel, norm),
        out_shape=(
            jax.ShapeDtypeStruct((NZ, 4, ROWS, 128), BF16),
            jax.ShapeDtypeStruct((4, NZ, ROWS, 256), BF16),
            jax.ShapeDtypeStruct((8, 32, D), BF16),
            jax.ShapeDtypeStruct((PRE, D), BF16),
        ),
        in_specs=[VM] * 8,
        out_specs=(VM,) * 4,
        compiler_params=pltpu.CompilerParams(vmem_limit_bytes=LIMIT),
        name="products",
    )(*args)


def reduce_kernel(
    ra, rb, p, pb, fin, tiles, pin, pbin,
    ain, bin_, sa, sb, a2, b2, full,
    lsem, sa1, ra1, sb1, rb1, sp, rp, sq, rq, sa2, ra2, sb2, rb2, sf, rf,
):
    dp = lax.axis_index("dp")
    z, yh, c, x = (lax.axis_index(a) for a in SEQ_CHAN)
    y = yh * 2 + dp
    j8 = c * 4 + x
    q = z * 2 + yh
    nq, pq = lax.rem(q + 1, 2 * NZ), lax.rem(q + 2 * NZ - 1, 2 * NZ)
    barrier = pltpu.get_barrier_semaphore()

    def at_z(k):
        return {"seq_0": k}

    def at_y(k):
        return {"seq_1": k // 2, "dp": lax.rem(k, 2)}

    def at_j(k):
        return {"seq_2": k // 4, "chan": lax.rem(k, 4)}

    def tell(where):
        pl.semaphore_signal(barrier, inc=1, device_id=where, device_id_type=MESH)

    for off in range(1, NZ):
        tell(at_z(lax.rem(z + off, NZ)))
    for off in range(1, 4):
        tell(at_y(lax.rem(y + off, 4)))
    for off in range(1, 8):
        tell(at_j(lax.rem(j8 + off, 8)))

    @pl.when((c == 1) & (x == 3))
    def _():
        for k in range(8):
            tell({"seq_0": nq // 2, "seq_1": lax.rem(nq, 2), "seq_2": k // 4, "chan": k % 4})

    pl.semaphore_wait(barrier, NZ - 1 + 3 + 7 + 1)

    def send(src, dst, me, n, at, ss, rs, off):
        to = lax.rem(me + off, n)
        return pltpu.make_async_remote_copy(
            src_ref=src.at[to], dst_ref=dst.at[me], send_sem=ss.at[off], recv_sem=rs.at[off],
            device_id=at(to), device_id_type=MESH,
        )

    def arrive(src, dst, me, n, at, ss, rs, off):
        origin = lax.rem(me + n - off, n)
        return pltpu.make_async_remote_copy(
            src_ref=src.at[origin], dst_ref=dst.at[origin], send_sem=ss.at[off],
            recv_sem=rs.at[off], device_id=at(origin), device_id_type=MESH,
        )

    za = (ra, ain, z, NZ, at_z, sa1, ra1)
    yb = (rb, bin_, y, 4, at_y, sb1, rb1)
    xp = (p, pin, j8, 8, at_j, sp, rp)
    sends = [send(*yb, off) for off in (2, 1, 3)]
    sends += [send(*za, off) for off in (4, 3, 5, 2, 6, 1, 7)]
    sends += [send(*xp, off) for off in range(1, 8)]
    edge = pltpu.make_async_remote_copy(
        src_ref=pb, dst_ref=pbin.at[j8], send_sem=sq, recv_sem=rq.at[j8],
        device_id={"seq_0": pq // 2, "seq_1": lax.rem(pq, 2), "seq_2": 1, "chan": 3},
        device_id_type=MESH,
    )
    for d in sends:
        d.start()
    edge.start()
    own_a = pltpu.make_async_copy(ra.at[z], ain.at[z], lsem.at[0])
    own_b = pltpu.make_async_copy(rb.at[y], bin_.at[y], lsem.at[1])
    own_p = pltpu.make_async_copy(p.at[j8], pin.at[j8], lsem.at[2])
    for d in (own_a, own_b, own_p):
        d.start()
    own_a.wait()
    for off in range(1, NZ):
        arrive(*za, off).wait_recv()
    for k in range(4):
        acc = ain[0, k].astype(F32)
        for i in range(1, NZ):
            acc = acc + ain[i, k].astype(F32)
        sa[k] = acc.astype(BF16)
    ya = (sa, a2, y, 4, at_y, sa2, ra2)
    zb = (sb, b2, z, NZ, at_z, sb2, rb2)
    more = [send(*ya, off) for off in (2, 1, 3)]
    for d in more:
        d.start()
    own_b.wait()
    for off in range(1, 4):
        arrive(*yb, off).wait_recv()
    for k in range(NZ):
        acc = bin_[0, k].astype(F32)
        for i in range(1, 4):
            acc = acc + bin_[i, k].astype(F32)
        sb[k] = acc.astype(BF16)
    last = [send(*zb, off) for off in (4, 3, 5, 2, 6, 1, 7)]
    for d in last:
        d.start()
    own_sa = pltpu.make_async_copy(sa.at[y], a2.at[y], lsem.at[3])
    own_sb = pltpu.make_async_copy(sb.at[z], b2.at[z], lsem.at[4])
    own_sa.start()
    own_sb.start()
    own_sa.wait()
    own_sb.wait()
    for off in range(1, 4):
        arrive(*ya, off).wait_recv()
    for off in range(1, NZ):
        arrive(*zb, off).wait_recv()
    acc_a = a2[0].astype(F32)
    for i in range(1, 4):
        acc_a = acc_a + a2[i].astype(F32)
    acc_b = b2[0].astype(F32)
    for i in range(1, NZ):
        acc_b = acc_b + b2[i].astype(F32)
    for k in range(2):
        rows = slice(k * 40, (k + 1) * 40)
        full[k, :, :128] = acc_a[rows]
        full[k, :, 128:] = acc_b[rows]
    sib = 1 - c
    swap = pltpu.make_async_remote_copy(
        src_ref=full.at[sib], dst_ref=fin.at[c], send_sem=sf.at[0], recv_sem=rf.at[0],
        device_id={"seq_2": sib}, device_id_type=MESH,
    )
    swap_in = pltpu.make_async_remote_copy(
        src_ref=full.at[sib], dst_ref=fin.at[sib], send_sem=sf.at[0], recv_sem=rf.at[0],
        device_id={"seq_2": sib}, device_id_type=MESH,
    )
    swap.start()
    outs = []
    for off in range(1, 8):
        to = lax.rem(j8 + off, 8)
        d = pltpu.make_async_remote_copy(
            src_ref=full.at[to // 4, :, pl.ds(256, 128)], dst_ref=tiles.at[j8],
            send_sem=sf.at[off], recv_sem=rf.at[off], device_id=at_j(to), device_id_type=MESH,
        )
        d.start()
        outs.append(d)
    keep = pltpu.make_async_copy(full.at[c], fin.at[c], lsem.at[5])
    keep_t = pltpu.make_async_copy(
        full.at[c, :, pl.ds(256, 128)], tiles.at[j8], lsem.at[6]
    )
    keep.start()
    keep_t.start()
    own_p.wait()
    for off in range(1, 8):
        arrive(*xp, off).wait_recv()

    @pl.when((c == 1) & (x == 3))
    def _():
        for k in range(8):
            pltpu.make_async_remote_copy(
                src_ref=pb, dst_ref=pbin.at[k], send_sem=sq, recv_sem=rq.at[k],
                device_id={"seq_2": 0}, device_id_type=MESH,
            ).wait_recv()

    keep.wait()
    keep_t.wait()
    swap_in.wait_recv()
    for off in range(1, 8):
        origin = lax.rem(j8 + 8 - off, 8)
        pltpu.make_async_remote_copy(
            src_ref=full.at[c, :, pl.ds(256, 128)], dst_ref=tiles.at[origin],
            send_sem=sf.at[off], recv_sem=rf.at[off], device_id=at_j(origin),
            device_id_type=MESH,
        ).wait_recv()
    for d in sends + more + last + outs + [edge, swap]:
        d.wait_send()


def reductions(ra, rb, p, pb):
    dma = pltpu.SemaphoreType.DMA
    return pl.pallas_call(
        reduce_kernel,
        out_shape=(
            jax.ShapeDtypeStruct((2, 40, 384), F32),
            jax.ShapeDtypeStruct((8, 40, 128), F32),
            jax.ShapeDtypeStruct((8, 32, D), BF16),
            jax.ShapeDtypeStruct((8, PRE, D), BF16),
        ),
        in_specs=[VM] * 4,
        out_specs=(VM,) * 4,
        scratch_shapes=[
            pltpu.VMEM((NZ, 4, ROWS, 128), BF16),
            pltpu.VMEM((4, NZ, ROWS, 256), BF16),
            pltpu.VMEM((4, ROWS, 128), BF16),
            pltpu.VMEM((NZ, ROWS, 256), BF16),
            pltpu.VMEM((4, ROWS, 128), BF16),
            pltpu.VMEM((NZ, ROWS, 256), BF16),
            pltpu.VMEM((2, 40, 384), F32),
            dma((7,)), dma((8,)), dma((8,)), dma((4,)), dma((4,)), dma((8,)), dma((8,)),
            dma(()), dma((8,)), dma((4,)), dma((4,)), dma((8,)), dma((8,)), dma((8,)), dma((8,)),
        ],
        compiler_params=pltpu.CompilerParams(
            collective_id=3, has_side_effects=True, vmem_limit_bytes=LIMIT
        ),
        name="reductions",
    )(ra, rb, p, pb)


def finish_kernel(fin, tiles, pin, pbin, ig_o, iw_o, mw_o, sw_o):
    z, yh, c, x = (lax.axis_index(a) for a in SEQ_CHAN)
    for k in range(2):
        iw_o[:, k * INNER : (k + 1) * INNER] = fin[k, :, :INNER]
        sw_o[:, k * HEADS : (k + 1) * HEADS] = fin[k, :, 352 : 352 + HEADS]
    rows = one_hot(iota((10, 40), 1) == iota((10, 40), 0) + 10 * x)
    for j in range(8):
        mw_o[:, j * 32 : (j + 1) * 32] = exact(rows, tiles[j])[:, 64:96]
    acc = pin[0].astype(F32)
    for j in range(1, 8):
        acc = acc + pin[j].astype(F32)
    ig_o[...] = acc.astype(BF16)

    @pl.when((c == 1) & (x == 3))
    def _():
        edge = pbin[0].astype(F32)
        for j in range(1, 8):
            edge = edge + pbin[j].astype(F32)
        ig_o[16:, :] = (acc[16:] + roll(edge, 0)).astype(BF16)


def finish(*args):
    return pl.pallas_call(
        finish_kernel,
        out_shape=(
            jax.ShapeDtypeStruct((32, D), BF16),
            jax.ShapeDtypeStruct((40, 2 * INNER), F32),
            jax.ShapeDtypeStruct((10, 2 * STATE), F32),
            jax.ShapeDtypeStruct((40, 2 * HEADS), F32),
        ),
        in_specs=[VM] * 4,
        out_specs=(VM,) * 4,
        compiler_params=pltpu.CompilerParams(vmem_limit_bytes=LIMIT),
        name="finish",
    )(*args)


def body(
    layer_input,
    inner_weight,
    mixer_weight,
    step_weight,
    conv_inner,
    conv_mixer,
    step_bias,
    decay_log,
    skip_gain,
    output_grad,
):
    norm = 1.0 / math.sqrt(8192)
    bias, dlog, skip = (v.reshape(1, -1) for v in (step_bias, decay_log, skip_gain))
    xe, ogx = gather(layer_input[0], output_grad[0])
    xa, zi, zm, dt, cum, sr, og, wih, send = forward(
        xe, ogx, inner_weight, mixer_weight, step_weight, conv_inner, conv_mixer, bias, dlog
    )
    st = states(send)
    gi, gm, ds, gmt = backward(
        xa, zi, zm, dt, cum, sr, og, st, conv_inner, conv_mixer, dlog, skip
    )
    mixed = mix(gmt)
    ra, rb, p, pb = products(norm, xe, gi, gm, ds, mixed, wih, mixer_weight, step_weight)
    fin, tiles, pin, pbin = reductions(ra, rb, p, pb)
    ig, iw, mw, sw = finish(fin, tiles, pin, pbin)
    return ig[None], iw, mw, sw


def solution(mesh):
    split = Mesh(
        mesh.devices.reshape(mesh.shape["dp"], 8, 2, 2, mesh.shape["chan"]),
        ("dp", "seq_0", "seq_1", "seq_2", "chan"),
    )
    placed = (
        P("dp", SEQ_CHAN, None),
        P(None, "chan"),
        P(),
        P(None, "chan"),
        P(None, "chan"),
        P(),
        P("chan"),
        P("chan"),
        P("chan"),
        P("dp", SEQ, "chan"),
    )
    return jax.shard_map(
        body,
        mesh=split,
        in_specs=placed,
        out_specs=(
            P("dp", SEQ_CHAN, None),
            P(DP_SEQ, "chan"),
            P(DP_SEQ_CHAN, None),
            P(DP_SEQ, "chan"),
        ),
        check_vma=False,
    )
```

```python
import functools
import math

import jax
import jax.numpy as jnp
from jax import lax
from jax.experimental import pallas as pl
from jax.experimental.pallas import tpu as pltpu
from jax.sharding import Mesh
from jax.sharding import PartitionSpec as P

D = 2560
HDIM = 64
HEADS = 5
INNER = HEADS * HDIM
STATE = 128
TOK = 256
PRE = 16
EXT = TOK + PRE
NZ = 8
ROWS = 80
CHUNK = 48
F32 = jnp.float32
BF16 = jnp.bfloat16
SEQ = ("seq_0", "seq_1", "seq_2")
DP_SEQ = ("dp", "seq_0", "seq_1", "seq_2")
SEQ_CHAN = ("seq_0", "seq_1", "seq_2", "chan")
DP_SEQ_CHAN = ("dp", "seq_0", "seq_1", "seq_2", "chan")
MESH = pl.DeviceIdType.MESH
VM = pl.BlockSpec(memory_space=pltpu.VMEM)
LIMIT = 60 * 1024 * 1024


def roll(v, shift):
    return pltpu.roll(v, shift % v.shape[0], 0)


def mm(a, b):
    return jnp.dot(a, b, preferred_element_type=F32)


def mm_t(a, b):
    return lax.dot_general(a, b, (((1,), (1,)), ((), ())), preferred_element_type=F32)


def t_mm(a, b):
    return lax.dot_general(a, b, (((0,), (0,)), ((), ())), preferred_element_type=F32)


def exact(a, b):
    return jnp.dot(a, b, preferred_element_type=F32, precision=lax.Precision.HIGHEST)


def iota(shape, dim):
    return lax.broadcasted_iota(jnp.int32, shape, dim)


def one_hot(cond):
    return jnp.where(cond, 1.0, 0.0).astype(F32)


def head_expand():
    return one_hot(iota((128, INNER), 1) // HDIM == iota((128, INNER), 0))


def head_sum():
    return one_hot(iota((INNER, 128), 0) // HDIM == iota((INNER, 128), 1))


def head_pick(core):
    return one_hot(
        (iota((10, 128), 0) == iota((10, 128), 1) + HEADS * core) & (iota((10, 128), 1) < HEADS)
    )


def half_of(v, core):
    return jnp.where(core == 0, v[:, :INNER], v[:, INNER:])


def conv(v, k):
    return k[3:4] * v + k[2:3] * roll(v, 1) + k[1:2] * roll(v, 2) + k[0:1] * roll(v, 3)


def conv_back(g, k):
    return k[3:4] * g + k[2:3] * roll(g, -1) + k[1:2] * roll(g, -2) + k[0:1] * roll(g, -3)


def gather_kernel(piece, og, xe, ogx, local_sem, ssem, rsem, tsem):
    z, yh, c, x = (lax.axis_index(a) for a in SEQ_CHAN)
    right, left = lax.rem(x + 1, 4), lax.rem(x + 3, 4)
    sib = 1 - c
    q = z * 2 + yh
    nq, pq = lax.rem(q + 1, 2 * NZ), lax.rem(q + 2 * NZ - 1, 2 * NZ)
    barrier = pltpu.get_barrier_semaphore()

    def tell(**where):
        pl.semaphore_signal(barrier, inc=1, device_id=where, device_id_type=MESH)

    tell(chan=right)
    tell(chan=left)
    tell(seq_2=sib)

    @pl.when(c == 1)
    def _():
        tell(seq_0=pq // 2, seq_1=lax.rem(pq, 2), chan=3)

    pl.semaphore_wait(barrier, jnp.where((c == 1) & (x == 3), 7, 3))

    def slot(core, chan, half=None):
        base = PRE + (core * 4 + chan) * 32
        if half is None:
            return xe.at[pl.ds(pl.multiple_of(base, 16), 32), :]
        return xe.at[pl.ds(pl.multiple_of(base + 16 * half, 16), 16), :]

    def copy(src, dst, k, **where):
        return pltpu.make_async_remote_copy(
            src_ref=src, dst_ref=dst, send_sem=ssem.at[k], recv_sem=rsem.at[k],
            device_id=where, device_id_type=MESH,
        )

    def half(h):
        return piece.at[pl.ds(16 * h, 16), :]

    own = pltpu.make_async_copy(piece, slot(c, x), local_sem.at[0])
    own_og = pltpu.make_async_copy(og, ogx.at[c], local_sem.at[1])
    r0 = copy(half(0), slot(c, x, 0), 0, chan=right)
    l1 = copy(half(1), slot(c, x, 1), 1, chan=left)
    r1 = copy(half(1), slot(c, x, 1), 2, chan=right)
    l0 = copy(half(0), slot(c, x, 0), 3, chan=left)
    sp = copy(piece, slot(c, x), 4, seq_2=sib)
    so = copy(og, ogx.at[c], 5, seq_2=sib)
    for d in (r0, l1):
        d.start()

    def tails(chan):
        return pltpu.make_async_remote_copy(
            src_ref=half(1), dst_ref=xe.at[pl.ds(0, 16), :], send_sem=tsem.at[chan],
            recv_sem=rsem.at[6],
            device_id={"seq_0": nq // 2, "seq_1": lax.rem(nq, 2), "chan": chan},
            device_id_type=MESH,
        )

    @pl.when((c == 1) & (x == 3))
    def _():
        for chan in range(4):
            tails(chan).start()

    for d in (r1, l0, sp, so):
        d.start()
    own.start()
    own_og.start()
    far = lax.rem(x + 2, 4)
    in_r0 = copy(half(0), slot(c, left, 0), 0, chan=right)
    in_r1 = copy(half(1), slot(c, left, 1), 2, chan=right)
    in_l1 = copy(half(1), slot(c, right, 1), 1, chan=left)
    in_l0 = copy(half(0), slot(c, right, 0), 3, chan=left)
    rr = copy(slot(c, left, 0), slot(c, left, 0), 7, chan=right)
    ll = copy(slot(c, right, 1), slot(c, right, 1), 8, chan=left)
    in_r0.wait_recv()
    rr.start()
    in_l1.wait_recv()
    ll.start()
    in_r1.wait_recv()
    s_left = copy(slot(c, left), slot(c, left), 9, seq_2=sib)
    s_left.start()
    in_l0.wait_recv()
    s_right = copy(slot(c, right), slot(c, right), 10, seq_2=sib)
    s_right.start()
    tail_on = copy(xe.at[pl.ds(0, 16), :], xe.at[pl.ds(0, 16), :], 12, seq_2=sib)

    @pl.when(c == 1)
    def _():
        tails(0).wait_recv()
        tail_on.start()

    in_rr = copy(half(0), slot(c, far, 0), 7, chan=right)
    in_ll = copy(half(1), slot(c, far, 1), 8, chan=left)
    in_rr.wait_recv()
    in_ll.wait_recv()
    s_far = copy(slot(c, far), slot(c, far), 11, seq_2=sib)
    s_far.start()
    copy(piece, slot(sib, x), 4, seq_2=sib).wait_recv()
    copy(og, ogx.at[sib], 5, seq_2=sib).wait_recv()
    copy(piece, slot(sib, left), 9, seq_2=sib).wait_recv()
    copy(piece, slot(sib, right), 10, seq_2=sib).wait_recv()
    copy(piece, slot(sib, far), 11, seq_2=sib).wait_recv()

    @pl.when(c == 0)
    def _():
        tail_on.wait_recv()

    for d in (r0, l1, r1, l0, sp, so, rr, ll, s_left, s_right, s_far):
        d.wait_send()

    @pl.when(c == 1)
    def _():
        tail_on.wait_send()

    @pl.when((c == 1) & (x == 3))
    def _():
        for chan in range(4):
            tails(chan).wait_send()

    own.wait()
    own_og.wait()


def gather(piece, og):
    return pl.pallas_call(
        gather_kernel,
        out_shape=(
            jax.ShapeDtypeStruct((EXT, D), BF16),
            jax.ShapeDtypeStruct((2, TOK // 2, 2 * INNER), BF16),
        ),
        in_specs=[VM, VM],
        out_specs=(VM, VM),
        scratch_shapes=[
            pltpu.SemaphoreType.DMA((2,)),
            pltpu.SemaphoreType.DMA((13,)),
            pltpu.SemaphoreType.DMA((13,)),
            pltpu.SemaphoreType.DMA((4,)),
        ],
        compiler_params=pltpu.CompilerParams(collective_id=0, has_side_effects=True),
        name="gather",
    )(piece, og)


def forward_kernel(
    xe, ogx, wi, wm, ws, ci, cm, bias, dlog,
    xa_o, zi_o, zm_o, dt_o, cum_o, sr_o, og_o, wih_o, send_o,
):
    z, yh, c = (lax.axis_index(a) for a in SEQ)
    flag = jnp.where(z * 2 + yh == 0, 0.0, 1.0).astype(F32)
    pick = head_pick(c)
    wih = half_of(wi[...], c)
    wih_o[...] = wih
    xv = xe[...]
    keep = jnp.where(iota((EXT, 1), 0) < PRE, flag, 1.0)

    def masked(v):
        return jnp.where(keep > 0.0, v.astype(BF16).astype(F32), 0.0)

    pi = masked(mm(xv, wih))
    pm = masked(mm(xv, wm[...]))
    sr = exact(mm(xv, ws[...])[PRE:], pick)
    zi = conv(pi, half_of(ci[...], c))[PRE:]
    zm = conv(pm, cm[...])[PRE:]
    xa = zi * jax.nn.sigmoid(zi)
    ma = zm * jax.nn.sigmoid(zm)
    srb = sr + exact(bias[...], pick)
    dt = jnp.maximum(srb, 0.0) + jnp.log1p(jnp.exp(-jnp.abs(srb)))
    rate = exact(jnp.exp(dlog[...]), pick)
    a = -dt * rate
    tri = one_hot(iota((TOK, TOK), 0) >= iota((TOK, TOK), 1))
    cum = exact(tri, a)
    tot = cum[TOK - 1 : TOK]
    og = half_of(ogx[...].reshape(TOK, 2 * INNER), c)
    ex = head_expand()
    xt = (xa * exact(dt * jnp.exp(tot - cum), ex)).astype(BF16)
    yt = (og.astype(F32) * exact(jnp.exp(cum), ex)).astype(BF16)
    f_loc = t_mm(xt, ma[:, :STATE].astype(BF16))
    g_loc = t_mm(yt, ma[:, STATE:].astype(BF16))
    diag = jnp.where(iota((8, 128), 0) == iota((8, 128), 1), tot, 0.0)
    dm = exact(diag, jnp.ones((128, 128), F32))
    hi = dm.astype(BF16).astype(F32)
    drow = jnp.where(iota((8, 128), 1) < 64, hi, dm - hi)
    for zz in range(NZ):
        for which, v in ((0, f_loc), (1, g_loc)):
            rows = [v[h * HDIM + zz * 8 : h * HDIM + zz * 8 + 8] for h in range(HEADS)]
            send_o[zz * 2 + which] = jnp.concatenate(rows + [drow], axis=0).astype(BF16)
    xa_o[...] = xa
    zi_o[...] = zi
    zm_o[...] = zm
    dt_o[...] = dt
    cum_o[...] = cum
    sr_o[...] = srb
    og_o[...] = og


def forward(*args):
    return pl.pallas_call(
        forward_kernel,
        out_shape=(
            jax.ShapeDtypeStruct((TOK, INNER), F32),
            jax.ShapeDtypeStruct((TOK, INNER), F32),
            jax.ShapeDtypeStruct((TOK, 2 * STATE), F32),
            jax.ShapeDtypeStruct((TOK, 128), F32),
            jax.ShapeDtypeStruct((TOK, 128), F32),
            jax.ShapeDtypeStruct((TOK, 128), F32),
            jax.ShapeDtypeStruct((TOK, INNER), BF16),
            jax.ShapeDtypeStruct((D, INNER), BF16),
            jax.ShapeDtypeStruct((2 * NZ, CHUNK, STATE), BF16),
        ),
        in_specs=[VM] * 9,
        out_specs=(VM,) * 9,
        compiler_params=pltpu.CompilerParams(vmem_limit_bytes=LIMIT),
        name="forward",
    )(*args)


def state_kernel(send, out, recv, back, local_sem, s1, r1, s2, r2):
    z, yh = lax.axis_index("seq_0"), lax.axis_index("seq_1")
    n = 2 * NZ
    me = z * 2 + yh
    barrier = pltpu.get_barrier_semaphore()

    def at(q):
        return {"seq_0": q // 2, "seq_1": lax.rem(q, 2)}

    for off in range(1, n):
        pl.semaphore_signal(
            barrier, inc=1, device_id=at(lax.rem(me + off, n)), device_id_type=MESH
        )
    pl.semaphore_wait(barrier, n - 1)

    def push(src, dst, ss, rs, off):
        to = lax.rem(me + off, n)
        return pltpu.make_async_remote_copy(
            src_ref=src.at[to], dst_ref=dst.at[me], send_sem=ss.at[off], recv_sem=rs.at[off],
            device_id=at(to), device_id_type=MESH,
        )

    def pull(src, dst, ss, rs, off):
        origin = lax.rem(me + n - off, n)
        return pltpu.make_async_remote_copy(
            src_ref=src.at[origin], dst_ref=dst.at[origin], send_sem=ss.at[off],
            recv_sem=rs.at[off], device_id=at(origin), device_id_type=MESH,
        )

    first = [push(send, recv, s1, r1, off) for off in range(1, n)]
    for d in first:
        d.start()
    own = pltpu.make_async_copy(send.at[me], recv.at[me], local_sem.at[0])
    own.start()
    own.wait()
    for off in range(1, n):
        pull(send, recv, s1, r1, off).wait_recv()
    run = jnp.zeros((HEADS * 8, STATE), F32)
    for j in range(n):
        k = jnp.where(yh == 0, j, n - 1 - j)
        got = recv[k].astype(F32)
        rows = got[HEADS * 8 :]
        rows = rows + pltpu.roll(rows, 64, 1)
        decay = jnp.exp(rows)
        back[k] = jnp.concatenate([run, rows], axis=0).astype(BF16)
        wide = jnp.concatenate(
            [jnp.broadcast_to(decay[h : h + 1], (8, STATE)) for h in range(HEADS)], axis=0
        )
        run = wide * run + got[: HEADS * 8]
    second = [push(back, out, s2, r2, off) for off in range(1, n)]
    for d in second:
        d.start()
    own = pltpu.make_async_copy(back.at[me], out.at[me], local_sem.at[1])
    own.start()
    own.wait()
    for off in range(1, n):
        pull(back, out, s2, r2, off).wait_recv()
    for d in first + second:
        d.wait_send()


def states(send):
    n = 2 * NZ
    return pl.pallas_call(
        state_kernel,
        out_shape=jax.ShapeDtypeStruct((n, CHUNK, STATE), BF16),
        in_specs=[VM],
        out_specs=VM,
        scratch_shapes=[
            pltpu.VMEM((n, CHUNK, STATE), BF16),
            pltpu.VMEM((n, CHUNK, STATE), BF16),
            pltpu.SemaphoreType.DMA((2,)),
            pltpu.SemaphoreType.DMA((n,)),
            pltpu.SemaphoreType.DMA((n,)),
            pltpu.SemaphoreType.DMA((n,)),
            pltpu.SemaphoreType.DMA((n,)),
        ],
        compiler_params=pltpu.CompilerParams(collective_id=1, has_side_effects=True),
        name="states",
    )(send)


def backward_kernel(
    xa_r, zi_r, zm_r, dt_r, cum_r, sr_r, og_r, st, ci, cm, dlog, skip,
    gi_o, gm_o, ds_o, gmt_o,
):
    z, yh, c = (lax.axis_index(a) for a in SEQ)
    flag = jnp.where(z * 2 + yh == 0, 0.0, 1.0).astype(F32)
    pick = head_pick(c)
    ex, hs = head_expand(), head_sum()
    xa, zi, zm = xa_r[...], zi_r[...], zm_r[...]
    dt, cum = dt_r[...], cum_r[...]
    og = og_r[...]
    dy = og.astype(F32)
    rate = exact(jnp.exp(dlog[...]), pick)
    skp = exact(skip[...], pick)
    tot = cum[TOK - 1 : TOK]
    ecum = exact(jnp.exp(cum), ex)
    etail = exact(jnp.exp(tot - cum), ex)
    dte = exact(dt, ex)

    def collect(which):
        blocks = [st[2 * zz + which].astype(F32) for zz in range(NZ)]
        rows = [blocks[zz][h * 8 : h * 8 + 8] for h in range(HEADS) for zz in range(NZ)]
        return jnp.concatenate(rows, axis=0)

    h0, ge = collect(0), collect(1)
    h0b, geb = h0.astype(BF16), ge.astype(BF16)
    sz = jax.nn.sigmoid(zm)
    ma = zm * sz
    bm, cmx = ma[:, :STATE].astype(BF16), ma[:, STATE:].astype(BF16)
    xdt = xa * dte
    xdtb = xdt.astype(BF16)
    xdtf = xdtb.astype(F32)
    scores = mm_t(cmx, bm)
    causal = iota((TOK, TOK), 0) >= iota((TOK, TOK), 1)
    cumt = cum.T
    dscore = jnp.zeros((TOK, TOK), F32)
    ys, us = [], []
    for h in range(HEADS):
        cols = slice(h * HDIM, (h + 1) * HDIM)
        decay = jnp.exp(jnp.where(causal, cum[:, h : h + 1] - cumt[h : h + 1, :], -1e30))
        m = (decay * scores).astype(BF16)
        ys.append(mm(m, xdtb[:, cols]))
        us.append(t_mm(m, og[:, cols]))
        dscore = dscore + decay * mm_t(og[:, cols], xdtb[:, cols])
    y = jnp.concatenate(ys, axis=1) + ecum * mm_t(cmx, h0b)
    ug = etail * mm_t(bm, geb)
    u = jnp.concatenate(us, axis=1) + ug
    dxa = dte * u + exact(skp, ex) * dy
    ddt = exact(xa * u, hs)
    dcum = exact(dy * y - xdtf * u, hs)
    e_sum = jnp.sum(exact(xdtf * ug, hs), axis=0, keepdims=True)
    hg = exact(
        jnp.ones((8, STATE), F32), (h0 * ge).T
    )
    carry = jnp.exp(tot) * exact(hg, hs)[0:1]
    upper = one_hot(iota((TOK, TOK), 0) <= iota((TOK, TOK), 1))
    da = exact(upper, dcum) + e_sum + carry
    dsr = (ddt - rate * da) * jax.nn.sigmoid(sr_r[...])
    dsb = dscore.astype(BF16)
    d_out = mm(dsb, bm) + mm((dy * ecum).astype(BF16), h0b)
    d_in = t_mm(dsb, cmx) + mm((xdt * etail).astype(BF16), geb)
    gm = jnp.concatenate([d_in, d_out], axis=1) * (sz * (1.0 + zm * (1.0 - sz)))
    si = jax.nn.sigmoid(zi)
    gi = dxa * (si * (1.0 + zi * (1.0 - si)))
    keep = jnp.where(iota((EXT, 1), 0) < PRE, flag, 1.0)

    def back(g, k):
        g = jnp.concatenate([jnp.zeros((PRE, g.shape[1]), F32), g], axis=0)
        return jnp.where(keep > 0.0, conv_back(g, k), 0.0).astype(BF16)

    gi_o[...] = back(gi, half_of(ci[...], c))
    gme = back(gm, cm[...])
    gm_o[...] = gme
    ds_o[...] = jnp.concatenate([jnp.zeros((PRE, 128), F32), dsr], axis=0).astype(BF16)
    eye = one_hot(iota((EXT, EXT), 0) == iota((EXT, EXT), 1)).astype(BF16)
    gmt = t_mm(gme, eye).astype(BF16)
    for j in range(8):
        gmt_o[j] = gmt[j * 32 : j * 32 + 32]


def backward(*args):
    return pl.pallas_call(
        backward_kernel,
        out_shape=(
            jax.ShapeDtypeStruct((EXT, INNER), BF16),
            jax.ShapeDtypeStruct((EXT, 2 * STATE), BF16),
            jax.ShapeDtypeStruct((EXT, 128), BF16),
            jax.ShapeDtypeStruct((8, 32, EXT), BF16),
        ),
        in_specs=[VM] * 12,
        out_specs=(VM,) * 4,
        compiler_params=pltpu.CompilerParams(vmem_limit_bytes=LIMIT),
        name="backward",
    )(*args)


def rows_of(ref, lo, n):
    return ref[lo : lo + n]


def sums_kernel(
    norm, xe, gi_r, gm_r, ds_r, gmt, wih, wm, ws,
    tiles, fb, pown, xin, pbin,
    mixin, rb, yhold, yin, ra, a3, a4, a1, a2, sa, ya, sb, b3, b4, b1, b2, fa, fbs, p, psib, xhold,
    pb, pbsib,
    lsem, ms, mr, ys, yr, zs, zr, qs, qr, xs, xr, es, er, as_, ar, ts, tr, dsem, drem,
):
    dp = lax.axis_index("dp")
    z, yh, c, x = (lax.axis_index(a) for a in SEQ_CHAN)
    y = yh * 2 + dp
    j8 = c * 4 + x
    sib = 1 - c
    q = z * 2 + yh
    nq, pq = lax.rem(q + 1, 2 * NZ), lax.rem(q + 2 * NZ - 1, 2 * NZ)
    barrier = pltpu.get_barrier_semaphore()

    def at_z(off):
        return {"seq_0": lax.rem(z + off + NZ, NZ)}

    def at_y(off):
        k = lax.rem(y + off + 4, 4)
        return {"seq_1": k // 2, "dp": lax.rem(k, 2)}

    def at_x(off):
        return {"chan": lax.rem(x + off + 4, 4)}

    def at_j(k):
        return {"seq_2": k // 4, "chan": lax.rem(k, 4)}

    def tell(where):
        pl.semaphore_signal(barrier, inc=1, device_id=where, device_id_type=MESH)

    for off in (1, -1, 2, -2):
        tell(at_z(off))
    for off in (1, 2, 3):
        tell(at_y(off))
    for off in range(1, 8):
        tell(at_j(lax.rem(j8 + off, 8)))

    @pl.when((c == 1) & (x == 3))
    def _():
        for k in range(4):
            tell({"seq_0": nq // 2, "seq_1": lax.rem(nq, 2), "chan": k})

    pl.semaphore_wait(barrier, jnp.where(c == 1, 15, 14))

    def remote(src, dst, ss, rs, where):
        return pltpu.make_async_remote_copy(
            src_ref=src, dst_ref=dst, send_sem=ss, recv_sem=rs, device_id=where,
            device_id_type=MESH,
        )

    pending = []

    def go(d):
        d.start()
        pending.append(d)
        return d

    for off in range(1, 8):
        to = lax.rem(j8 + off, 8)
        go(remote(gmt.at[to], mixin.at[off], ms.at[off], mr.at[off], at_j(to)))

    gi = gi_r[...]
    rhs = gi[:, :256]

    def inner_rows(side):
        for zhi in range(2):
            base = pl.multiple_of(side * 1280 + zhi * 640, 128)
            r = (t_mm(xe[:, pl.ds(base, 640)], rhs) * norm).astype(BF16)
            for g in range(8):
                for k in range(2):
                    rb[(g % 2) * 2 + side, zhi * 4 + g // 2, k] = r[
                        g * ROWS : (g + 1) * ROWS, k * 128 : (k + 1) * 128
                    ]

    up, down, far = lax.rem(y + 1, 4), lax.rem(y + 3, 4), lax.rem(y + 2, 4)
    lo, hi = pl.ds(0, 4), pl.ds(4, 4)
    inner_rows(dp)
    go(remote(rb.at[far, lo], yhold.at[0], ys.at[0], yr.at[0], at_y(1)))
    go(remote(rb.at[far, hi], yhold.at[1], ys.at[1], yr.at[1], at_y(-1)))
    inner_rows(1 - dp)
    go(remote(rb.at[up, hi], yin.at[0, hi], ys.at[2], yr.at[2], at_y(1)))
    go(remote(rb.at[down, lo], yin.at[1, lo], ys.at[3], yr.at[3], at_y(-1)))

    total = gmt[j8].astype(F32)
    for off in range(1, 8):
        origin = lax.rem(j8 + 8 - off, 8)
        remote(gmt.at[origin], mixin.at[off], ms.at[off], mr.at[off], at_j(origin)).wait_recv()
        total = total + mixin[off].astype(F32)
    place_mix = one_hot(iota((32, 128), 1) == iota((32, 128), 0) + 64).astype(BF16)
    place_step = one_hot(
        (iota((128, 128), 1) == iota((128, 128), 0) + 96) & (iota((128, 128), 0) < HEADS)
    ).astype(BF16)
    ds = ds_r[...]
    last = t_mm(total.astype(BF16), place_mix) + mm(ds, place_step)
    last = last + jnp.concatenate([gi[:, 256:].astype(F32), jnp.zeros((EXT, 64), F32)], axis=1)
    last = last.astype(BF16)
    for b in range(4):
        r = (t_mm(xe[:, b * 640 : (b + 1) * 640], last) * norm).astype(BF16)
        for g in range(8):
            ra[(b % 2) * 4 + g // 2, (g % 2) * 2 + b // 2] = r[g * ROWS : (g + 1) * ROWS]

    def z_first(src, n, r3, r4, r1, s, r):
        h = n // 2
        for k, sign in enumerate((1, -1)):
            part = pl.ds(k * h, h)
            dst = [lax.rem(z + sign * d + NZ, NZ) for d in range(5)]
            go(remote(src.at[dst[4], part], r4.at[k], s.at[4 * k], r.at[4 * k], at_z(2 * sign)))
            go(remote(src.at[dst[3]], r3.at[k], s.at[4 * k + 1], r.at[4 * k + 1], at_z(sign)))
            go(remote(src.at[dst[1]], r1.at[k], s.at[4 * k + 2], r.at[4 * k + 2], at_z(sign)))

    def z_second(src, n, r3, r4, r2, s, r):
        h = n // 2
        for k, sign in enumerate((1, -1)):
            part = pl.ds(k * h, h)
            t = lax.rem(z + 2 * sign + NZ, NZ)
            remote(r3.at[k], r3.at[k], s.at[4 * k + 1], r.at[4 * k + 1], at_z(sign)).wait_recv()
            remote(r4.at[k], r4.at[k], s.at[4 * k], r.at[4 * k], at_z(2 * sign)).wait_recv()
            for i in range(n):
                v = src[t, i].astype(F32) + r3[k, i].astype(F32)
                if k * h <= i < (k + 1) * h:
                    v = v + r4[k, i - k * h].astype(F32)
                r3[k, i] = v.astype(BF16)
            go(remote(r3.at[k], r2.at[k], s.at[4 * k + 3], r.at[4 * k + 3], at_z(2 * sign)))

    def z_last(r1, r2, s, r):
        for k, sign in enumerate((1, -1)):
            remote(r1.at[k], r1.at[k], s.at[4 * k + 2], r.at[4 * k + 2], at_z(sign)).wait_recv()
            remote(r2.at[k], r2.at[k], s.at[4 * k + 3], r.at[4 * k + 3], at_z(2 * sign)).wait_recv()

    z_first(ra, 4, a3, a4, a1, zs, zr)

    pick = head_pick(c).astype(BF16)
    ds10 = mm_t(ds, pick).astype(BF16)
    gm = gm_r[...]
    for b in range(4):
        rows = slice(b * 640, (b + 1) * 640)
        part = mm_t(gi, wih[rows]) + mm_t(gm, wm[rows]) + mm_t(ds10, ws[rows])
        part = part.astype(BF16)
        pb[:, rows] = part[:PRE]
        for j in range(8):
            for k in range(2):
                at = PRE + j * 32 + k * 16
                p[j // 4, j % 4, k, :, rows] = part[at : at + 16]
    go(remote(p.at[sib], psib, dsem.at[0], drem.at[0], {"seq_2": sib}))
    pb_out = remote(pb, pbsib, dsem.at[1], drem.at[1], {"seq_2": sib})

    @pl.when(c == 0)
    def _():
        pb_out.start()

    remote(yhold.at[0], yhold.at[0], ys.at[0], yr.at[0], at_y(1)).wait_recv()
    for i in range(4):
        yhold[0, i] = (rb[up, i].astype(F32) + yhold[0, i].astype(F32)).astype(BF16)
    go(remote(yhold.at[0], yin.at[0, lo], ys.at[4], yr.at[4], at_y(1)))
    remote(yhold.at[1], yhold.at[1], ys.at[1], yr.at[1], at_y(-1)).wait_recv()
    for i in range(4):
        yhold[1, i] = (rb[down, 4 + i].astype(F32) + yhold[1, i].astype(F32)).astype(BF16)
    go(remote(yhold.at[1], yin.at[1, hi], ys.at[5], yr.at[5], at_y(-1)))

    z_second(ra, 4, a3, a4, a2, zs, zr)

    remote(psib, psib, dsem.at[0], drem.at[0], {"seq_2": sib}).wait_recv()
    for k in range(4):
        for h in range(2):
            psib[k, h] = (p[c, k, h].astype(F32) + psib[k, h].astype(F32)).astype(BF16)
    xu, xd, xf = lax.rem(x + 1, 4), lax.rem(x + 3, 4), lax.rem(x + 2, 4)
    go(remote(psib.at[xf, 0], xhold.at[0], xs.at[0], xr.at[0], at_x(1)))
    go(remote(psib.at[xf, 1], xhold.at[1], xs.at[1], xr.at[1], at_x(-1)))
    go(remote(psib.at[xu, 1], xin.at[0, 1], xs.at[2], xr.at[2], at_x(1)))
    go(remote(psib.at[xd, 0], xin.at[1, 0], xs.at[3], xr.at[3], at_x(-1)))
    edge = remote(
        pbsib, pbin.at[x], es, er.at[x],
        {"seq_0": pq // 2, "seq_1": lax.rem(pq, 2), "chan": 3},
    )

    @pl.when(c == 1)
    def _():
        pb_out.wait_recv()
        pbsib[...] = (pb[...].astype(F32) + pbsib[...].astype(F32)).astype(BF16)
        edge.start()

    for k in (2, 4):
        part = hi if k == 2 else lo
        remote(yin.at[0, part], yin.at[0, part], ys.at[k], yr.at[k], at_y(1)).wait_recv()
    for k in (3, 5):
        part = lo if k == 3 else hi
        remote(yin.at[1, part], yin.at[1, part], ys.at[k], yr.at[k], at_y(-1)).wait_recv()
    for i in range(NZ):
        v = rb[y, i].astype(F32) + yin[0, i].astype(F32) + yin[1, i].astype(F32)
        sb[i] = v.astype(BF16)
    z_first(sb, 2, b3, b4, b1, qs, qr)

    z_last(a1, a2, zs, zr)
    for i in range(4):
        v = ra[z, i].astype(F32)
        for k in range(2):
            v = v + a1[k, i].astype(F32) + a2[k, i].astype(F32)
        sa[i] = v.astype(BF16)
    for off in (2, 1, 3):
        to = lax.rem(y + off, 4)
        go(remote(sa.at[to], ya.at[off], as_.at[off], ar.at[off], at_y(off)))

    remote(xhold.at[0], xhold.at[0], xs.at[0], xr.at[0], at_x(1)).wait_recv()
    xhold[0] = (psib[xu, 0].astype(F32) + xhold[0].astype(F32)).astype(BF16)
    go(remote(xhold.at[0], xin.at[0, 0], xs.at[4], xr.at[4], at_x(1)))
    remote(xhold.at[1], xhold.at[1], xs.at[1], xr.at[1], at_x(-1)).wait_recv()
    xhold[1] = (psib[xd, 1].astype(F32) + xhold[1].astype(F32)).astype(BF16)
    go(remote(xhold.at[1], xin.at[1, 1], xs.at[5], xr.at[5], at_x(-1)))
    pown[...] = psib[x]

    z_second(sb, 2, b3, b4, b2, qs, qr)

    v = sa[y].astype(F32)
    for off in range(1, 4):
        remote(ya.at[off], ya.at[off], as_.at[off], ar.at[off], at_y(off)).wait_recv()
        v = v + ya[off].astype(F32)
    fa[0] = v[:40]
    fa[1] = v[40:]
    for off in range(1, 8):
        to = lax.rem(j8 + off, 8)
        go(remote(fa.at[to // 4], tiles.at[j8], ts.at[off], tr.at[off], at_j(to)))
    tiles[j8] = fa[c]

    z_last(b1, b2, qs, qr)
    for i in range(2):
        v = sb[z, i].astype(F32)
        for k in range(2):
            v = v + b1[k, i].astype(F32) + b2[k, i].astype(F32)
        fbs[0, :, i * 128 : (i + 1) * 128] = v[:40]
        fbs[1, :, i * 128 : (i + 1) * 128] = v[40:]
    go(remote(fbs.at[sib], fb.at[c], dsem.at[2], drem.at[2], {"seq_2": sib}))
    fb[c] = fbs[c]

    for k, half in ((2, 1), (4, 0)):
        remote(xin.at[0, half], xin.at[0, half], xs.at[k], xr.at[k], at_x(1)).wait_recv()
    for k, half in ((3, 0), (5, 1)):
        remote(xin.at[1, half], xin.at[1, half], xs.at[k], xr.at[k], at_x(-1)).wait_recv()
    for off in range(1, 8):
        origin = lax.rem(j8 + 8 - off, 8)
        remote(fa.at[c], tiles.at[origin], ts.at[off], tr.at[off], at_j(origin)).wait_recv()

    @pl.when((c == 1) & (x == 3))
    def _():
        for k in range(4):
            remote(pbsib, pbin.at[k], es, er.at[k], {"chan": 0}).wait_recv()

    remote(fbs.at[c], fb.at[sib], dsem.at[2], drem.at[2], {"seq_2": sib}).wait_recv()
    for d in pending:
        d.wait_send()

    @pl.when(c == 0)
    def _():
        pb_out.wait_send()

    @pl.when(c == 1)
    def _():
        edge.wait_send()


def sums(norm, *args):
    dma = pltpu.SemaphoreType.DMA

    def vm(*shape):
        return pltpu.VMEM(shape, BF16)

    return pl.pallas_call(
        functools.partial(sums_kernel, norm),
        out_shape=(
            jax.ShapeDtypeStruct((8, 40, 128), F32),
            jax.ShapeDtypeStruct((2, 40, 256), F32),
            jax.ShapeDtypeStruct((2, 16, D), BF16),
            jax.ShapeDtypeStruct((2, 2, 16, D), BF16),
            jax.ShapeDtypeStruct((4, PRE, D), BF16),
        ),
        in_specs=[VM] * 8,
        out_specs=(VM,) * 5,
        scratch_shapes=[
            vm(8, 32, EXT),
            vm(4, NZ, 2, ROWS, 128), vm(2, 4, 2, ROWS, 128), vm(2, NZ, 2, ROWS, 128),
            vm(NZ, 4, ROWS, 128), vm(2, 4, ROWS, 128), vm(2, 2, ROWS, 128),
            vm(2, 4, ROWS, 128), vm(2, 4, ROWS, 128), vm(4, ROWS, 128), vm(4, ROWS, 128),
            vm(NZ, 2, ROWS, 128), vm(2, 2, ROWS, 128), vm(2, 1, ROWS, 128),
            vm(2, 2, ROWS, 128), vm(2, 2, ROWS, 128),
            pltpu.VMEM((2, 40, 128), F32), pltpu.VMEM((2, 40, 256), F32),
            vm(2, 4, 2, 16, D), vm(4, 2, 16, D), vm(2, 16, D), vm(PRE, D), vm(PRE, D),
            dma((1,)), dma((8,)), dma((8,)), dma((6,)), dma((6,)), dma((8,)), dma((8,)),
            dma((8,)), dma((8,)), dma((6,)), dma((6,)), dma(()), dma((4,)), dma((4,)), dma((4,)),
            dma((8,)), dma((8,)), dma((3,)), dma((3,)),
        ],
        compiler_params=pltpu.CompilerParams(
            collective_id=2, has_side_effects=True, vmem_limit_bytes=LIMIT
        ),
        name="sums",
    )(*args)


def finish_kernel(tiles, fb, pown, xin, pbin, ig_o, iw_o, mw_o, sw_o):
    c, x = lax.axis_index("seq_2"), lax.axis_index("chan")
    for k in range(2):
        iw_o[:, k * INNER : k * INNER + 256] = fb[k]
        own = tiles[k * 4 + x]
        iw_o[:, k * INNER + 256 : (k + 1) * INNER] = own[:, :64]
        sw_o[:, k * HEADS : (k + 1) * HEADS] = own[:, 96 : 96 + HEADS]
    rows = one_hot(iota((10, 40), 1) == iota((10, 40), 0) + 10 * x)
    for j in range(8):
        mw_o[:, j * 32 : (j + 1) * 32] = exact(rows, tiles[j])[:, 64:96]
    for h in range(2):
        acc = pown[h].astype(F32) + xin[0, h].astype(F32) + xin[1, h].astype(F32)
        ig_o[h * 16 : (h + 1) * 16, :] = acc.astype(BF16)

    @pl.when((c == 1) & (x == 3))
    def _():
        edge = pown[1].astype(F32) + xin[0, 1].astype(F32) + xin[1, 1].astype(F32)
        for j in range(4):
            edge = edge + pbin[j].astype(F32)
        ig_o[16:, :] = edge.astype(BF16)


def finish(*args):
    return pl.pallas_call(
        finish_kernel,
        out_shape=(
            jax.ShapeDtypeStruct((32, D), BF16),
            jax.ShapeDtypeStruct((40, 2 * INNER), F32),
            jax.ShapeDtypeStruct((10, 2 * STATE), F32),
            jax.ShapeDtypeStruct((40, 2 * HEADS), F32),
        ),
        in_specs=[VM] * 5,
        out_specs=(VM,) * 4,
        compiler_params=pltpu.CompilerParams(vmem_limit_bytes=LIMIT),
        name="finish",
    )(*args)


def body(
    layer_input,
    inner_weight,
    mixer_weight,
    step_weight,
    conv_inner,
    conv_mixer,
    step_bias,
    decay_log,
    skip_gain,
    output_grad,
):
    norm = 1.0 / math.sqrt(8192)
    bias, dlog, skip = (v.reshape(1, -1) for v in (step_bias, decay_log, skip_gain))
    xe, ogx = gather(layer_input[0], output_grad[0])
    xa, zi, zm, dt, cum, sr, og, wih, send = forward(
        xe, ogx, inner_weight, mixer_weight, step_weight, conv_inner, conv_mixer, bias, dlog
    )
    st = states(send)
    gi, gm, ds, gmt = backward(
        xa, zi, zm, dt, cum, sr, og, st, conv_inner, conv_mixer, dlog, skip
    )
    parts = sums(norm, xe, gi, gm, ds, gmt, wih, mixer_weight, step_weight)
    ig, iw, mw, sw = finish(*parts)
    return ig[None], iw, mw, sw


def solution(mesh):
    split = Mesh(
        mesh.devices.reshape(mesh.shape["dp"], 8, 2, 2, mesh.shape["chan"]),
        ("dp", "seq_0", "seq_1", "seq_2", "chan"),
    )
    placed = (
        P("dp", SEQ_CHAN, None),
        P(None, "chan"),
        P(),
        P(None, "chan"),
        P(None, "chan"),
        P(),
        P("chan"),
        P("chan"),
        P("chan"),
        P("dp", SEQ, "chan"),
    )
    return jax.shard_map(
        body,
        mesh=split,
        in_specs=placed,
        out_specs=(
            P("dp", SEQ_CHAN, None),
            P(DP_SEQ, "chan"),
            P(DP_SEQ_CHAN, None),
            P(DP_SEQ, "chan"),
        ),
        check_vma=False,
    )
```

```python
import functools
import math

import jax
import jax.numpy as jnp
from jax import lax
from jax.experimental import pallas as pl
from jax.experimental.pallas import tpu as pltpu
from jax.sharding import Mesh
from jax.sharding import PartitionSpec as P

D = 2560
HDIM = 64
HEADS = 5
INNER = HEADS * HDIM
STATE = 128
TOK = 256
PRE = 16
EXT = TOK + PRE
NZ = 8
ROWS = 80
CHUNK = 48
F32 = jnp.float32
BF16 = jnp.bfloat16
SEQ = ("seq_0", "seq_1", "seq_2")
DP_SEQ = ("dp", "seq_0", "seq_1", "seq_2")
SEQ_CHAN = ("seq_0", "seq_1", "seq_2", "chan")
DP_SEQ_CHAN = ("dp", "seq_0", "seq_1", "seq_2", "chan")
MESH = pl.DeviceIdType.MESH
VM = pl.BlockSpec(memory_space=pltpu.VMEM)
LIMIT = 48 * 1024 * 1024


def roll(v, shift):
    return pltpu.roll(v, shift % v.shape[0], 0)


def mm(a, b):
    return jnp.dot(a, b, preferred_element_type=F32)


def mm_t(a, b):
    return lax.dot_general(a, b, (((1,), (1,)), ((), ())), preferred_element_type=F32)


def t_mm(a, b):
    return lax.dot_general(a, b, (((0,), (0,)), ((), ())), preferred_element_type=F32)


def exact(a, b):
    return jnp.dot(a, b, preferred_element_type=F32, precision=lax.Precision.HIGHEST)


def iota(shape, dim):
    return lax.broadcasted_iota(jnp.int32, shape, dim)


def one_hot(cond):
    return jnp.where(cond, 1.0, 0.0).astype(F32)


def head_expand():
    return one_hot(iota((128, INNER), 1) // HDIM == iota((128, INNER), 0))


def head_sum():
    return one_hot(iota((INNER, 128), 0) // HDIM == iota((INNER, 128), 1))


def head_pick(core):
    return one_hot(
        (iota((10, 128), 0) == iota((10, 128), 1) + HEADS * core) & (iota((10, 128), 1) < HEADS)
    )


def half_of(v, core):
    return jnp.where(core == 0, v[:, :INNER], v[:, INNER:])


def conv(v, k):
    return k[3:4] * v + k[2:3] * roll(v, 1) + k[1:2] * roll(v, 2) + k[0:1] * roll(v, 3)


def conv_back(g, k):
    return k[3:4] * g + k[2:3] * roll(g, -1) + k[1:2] * roll(g, -2) + k[0:1] * roll(g, -3)


def gather_phase(xe, ogx, ssem, rsem, tsem):
    z, yh, c, x = (lax.axis_index(a) for a in SEQ_CHAN)
    right, left = lax.rem(x + 1, 4), lax.rem(x + 3, 4)
    sib = 1 - c
    q = z * 2 + yh
    nq, pq = lax.rem(q + 1, 2 * NZ), lax.rem(q + 2 * NZ - 1, 2 * NZ)
    def slot(core, chan, half=None):
        base = PRE + (core * 4 + chan) * 32
        if half is None:
            return xe.at[pl.ds(pl.multiple_of(base, 16), 32), :]
        return xe.at[pl.ds(pl.multiple_of(base + 16 * half, 16), 16), :]

    def copy(src, dst, k, **where):
        return pltpu.make_async_remote_copy(
            src_ref=src, dst_ref=dst, send_sem=ssem.at[k], recv_sem=rsem.at[k],
            device_id=where, device_id_type=MESH,
        )

    mine = slot(c, x)
    own_og = ogx.at[c]

    def half(h):
        return slot(c, x, h)

    r0 = copy(half(0), slot(c, x, 0), 0, chan=right)
    l1 = copy(half(1), slot(c, x, 1), 1, chan=left)
    r1 = copy(half(1), slot(c, x, 1), 2, chan=right)
    l0 = copy(half(0), slot(c, x, 0), 3, chan=left)
    sp = copy(mine, mine, 4, seq_2=sib)
    so = copy(own_og, own_og, 5, seq_2=sib)
    for d in (r0, l1):
        d.start()

    def tails(chan):
        return pltpu.make_async_remote_copy(
            src_ref=half(1), dst_ref=xe.at[pl.ds(0, 16), :], send_sem=tsem.at[chan],
            recv_sem=rsem.at[6],
            device_id={"seq_0": nq // 2, "seq_1": lax.rem(nq, 2), "chan": chan},
            device_id_type=MESH,
        )

    @pl.when((c == 1) & (x == 3))
    def _():
        for chan in range(4):
            tails(chan).start()

    for d in (r1, l0, sp, so):
        d.start()
    far = lax.rem(x + 2, 4)
    in_r0 = copy(half(0), slot(c, left, 0), 0, chan=right)
    in_r1 = copy(half(1), slot(c, left, 1), 2, chan=right)
    in_l1 = copy(half(1), slot(c, right, 1), 1, chan=left)
    in_l0 = copy(half(0), slot(c, right, 0), 3, chan=left)
    rr = copy(slot(c, left, 0), slot(c, left, 0), 7, chan=right)
    ll = copy(slot(c, right, 1), slot(c, right, 1), 8, chan=left)
    in_r0.wait_recv()
    rr.start()
    in_l1.wait_recv()
    ll.start()
    in_r1.wait_recv()
    s_left = copy(slot(c, left), slot(c, left), 9, seq_2=sib)
    s_left.start()
    in_l0.wait_recv()
    s_right = copy(slot(c, right), slot(c, right), 10, seq_2=sib)
    s_right.start()
    tail_on = copy(xe.at[pl.ds(0, 16), :], xe.at[pl.ds(0, 16), :], 12, seq_2=sib)

    @pl.when(c == 1)
    def _():
        tails(0).wait_recv()
        tail_on.start()

    in_rr = copy(half(0), slot(c, far, 0), 7, chan=right)
    in_ll = copy(half(1), slot(c, far, 1), 8, chan=left)
    in_rr.wait_recv()
    in_ll.wait_recv()
    s_far = copy(slot(c, far), slot(c, far), 11, seq_2=sib)
    s_far.start()
    copy(mine, slot(sib, x), 4, seq_2=sib).wait_recv()
    copy(own_og, ogx.at[sib], 5, seq_2=sib).wait_recv()
    copy(mine, slot(sib, left), 9, seq_2=sib).wait_recv()
    copy(mine, slot(sib, right), 10, seq_2=sib).wait_recv()
    copy(mine, slot(sib, far), 11, seq_2=sib).wait_recv()

    @pl.when(c == 0)
    def _():
        tail_on.wait_recv()

    for d in (r0, l1, r1, l0, sp, so, rr, ll, s_left, s_right, s_far):
        d.wait_send()

    @pl.when(c == 1)
    def _():
        tail_on.wait_send()

    @pl.when((c == 1) & (x == 3))
    def _():
        for chan in range(4):
            tails(chan).wait_send()


def forward_phase(xe, ogx, wi, wm, ws, ci, cm, bias, dlog, wih_o, send_o):
    z, yh, c = (lax.axis_index(a) for a in SEQ)
    flag = jnp.where(z * 2 + yh == 0, 0.0, 1.0).astype(F32)
    pick = head_pick(c)
    wih = half_of(wi[...], c)
    wih_o[...] = wih
    xv = xe[...]
    keep = jnp.where(iota((EXT, 1), 0) < PRE, flag, 1.0)

    def masked(v):
        return jnp.where(keep > 0.0, v.astype(BF16).astype(F32), 0.0)

    pi = masked(mm(xv, wih))
    pm = masked(mm(xv, wm[...]))
    sr = exact(mm_t(xv, ws[...])[PRE:], pick)
    zi = conv(pi, half_of(ci[...], c))[PRE:]
    zm = conv(pm, cm[...])[PRE:]
    xa = zi * jax.nn.sigmoid(zi)
    ma = zm * jax.nn.sigmoid(zm)
    srb = sr + exact(bias[...], pick)
    dt = jnp.maximum(srb, 0.0) + jnp.log1p(jnp.exp(-jnp.abs(srb)))
    rate = exact(jnp.exp(dlog[...]), pick)
    a = -dt * rate
    tri = one_hot(iota((TOK, TOK), 0) >= iota((TOK, TOK), 1))
    cum = exact(tri, a)
    tot = cum[TOK - 1 : TOK]
    og = half_of(ogx[...].reshape(TOK, 2 * INNER), c)
    ex = head_expand()
    xt = (xa * exact(dt * jnp.exp(tot - cum), ex)).astype(BF16)
    yt = (og.astype(F32) * exact(jnp.exp(cum), ex)).astype(BF16)
    f_loc = t_mm(xt, ma[:, :STATE].astype(BF16))
    g_loc = t_mm(yt, ma[:, STATE:].astype(BF16))
    diag = jnp.where(iota((8, 128), 0) == iota((8, 128), 1), tot, 0.0)
    dm = exact(diag, jnp.ones((128, 128), F32))
    hi = dm.astype(BF16).astype(F32)
    drow = jnp.where(iota((8, 128), 1) < 64, hi, dm - hi)
    for zz in range(NZ):
        for which, v in ((0, f_loc), (1, g_loc)):
            rows = [v[h * HDIM + zz * 8 : h * HDIM + zz * 8 + 8] for h in range(HEADS)]
            send_o[zz * 2 + which] = jnp.concatenate(rows + [drow], axis=0).astype(BF16)
    return xa, zi, zm, dt, cum, srb, og


def state_phases(send, out, recv, back, local_sem, s1, r1, s2, r2):
    z, yh = lax.axis_index("seq_0"), lax.axis_index("seq_1")
    n = 2 * NZ
    me = z * 2 + yh
    def at(q):
        return {"seq_0": q // 2, "seq_1": lax.rem(q, 2)}

    def push(src, dst, ss, rs, off):
        to = lax.rem(me + off, n)
        return pltpu.make_async_remote_copy(
            src_ref=src.at[to], dst_ref=dst.at[me], send_sem=ss.at[off], recv_sem=rs.at[off],
            device_id=at(to), device_id_type=MESH,
        )

    def pull(src, dst, ss, rs, off):
        origin = lax.rem(me + n - off, n)
        return pltpu.make_async_remote_copy(
            src_ref=src.at[origin], dst_ref=dst.at[origin], send_sem=ss.at[off],
            recv_sem=rs.at[off], device_id=at(origin), device_id_type=MESH,
        )

    first = [push(send, recv, s1, r1, off) for off in range(1, n)]
    second = [push(back, out, s2, r2, off) for off in range(1, n)]

    def begin():
        for d in first:
            d.start()
        own = pltpu.make_async_copy(send.at[me], recv.at[me], local_sem.at[0])
        own.start()
        own.wait()

    def turn():
        for off in range(1, n):
            pull(send, recv, s1, r1, off).wait_recv()
        run = jnp.zeros((HEADS * 8, STATE), F32)
        for j in range(n):
            k = jnp.where(yh == 0, j, n - 1 - j)
            got = recv[k].astype(F32)
            rows = got[HEADS * 8 :]
            rows = rows + pltpu.roll(rows, 64, 1)
            decay = jnp.exp(rows)
            back[k] = jnp.concatenate([run, rows], axis=0).astype(BF16)
            wide = jnp.concatenate(
                [jnp.broadcast_to(decay[h : h + 1], (8, STATE)) for h in range(HEADS)], axis=0
            )
            run = wide * run + got[: HEADS * 8]
        for d in second:
            d.start()
        own = pltpu.make_async_copy(back.at[me], out.at[me], local_sem.at[1])
        own.start()
        own.wait()

    def end():
        for off in range(1, n):
            pull(back, out, s2, r2, off).wait_recv()
        for d in first + second:
            d.wait_send()

    return begin, turn, end


def local_phase(acts, dlog, skip):
    c = lax.axis_index("seq_2")
    pick = head_pick(c)
    ex = head_expand()
    xa, zi, zm, dt, cum, srb, og = acts
    dy = og.astype(F32)
    rate = exact(jnp.exp(dlog[...]), pick)
    skp = exact(skip[...], pick)
    tot = cum[TOK - 1 : TOK]
    ecum = exact(jnp.exp(cum), ex)
    etail = exact(jnp.exp(tot - cum), ex)
    dte = exact(dt, ex)
    sz = jax.nn.sigmoid(zm)
    ma = zm * sz
    bm, cmx = ma[:, :STATE].astype(BF16), ma[:, STATE:].astype(BF16)
    xdt = xa * dte
    xdtb = xdt.astype(BF16)
    xdtf = xdtb.astype(F32)
    scores = mm_t(cmx, bm)
    causal = iota((TOK, TOK), 0) >= iota((TOK, TOK), 1)
    cumt = cum.T
    dscore = jnp.zeros((TOK, TOK), F32)
    ys, us = [], []
    for h in range(HEADS):
        cols = slice(h * HDIM, (h + 1) * HDIM)
        decay = jnp.exp(jnp.where(causal, cum[:, h : h + 1] - cumt[h : h + 1, :], -1e30))
        m = (decay * scores).astype(BF16)
        ys.append(mm(m, xdtb[:, cols]))
        us.append(t_mm(m, og[:, cols]))
        dscore = dscore + decay * mm_t(og[:, cols], xdtb[:, cols])
    return (
        jnp.concatenate(ys, axis=1), jnp.concatenate(us, axis=1), dscore.astype(BF16), bm, cmx, sz,
        xdt, xdtf, dy, rate, exact(skp, ex), tot, ecum, etail, dte,
    )


def carried_phase(acts, local, st, ci, cm, gi_o, gm_o, ds_o, gmt_o):
    z, yh, c = (lax.axis_index(a) for a in SEQ)
    flag = jnp.where(z * 2 + yh == 0, 0.0, 1.0).astype(F32)
    hs = head_sum()
    xa, zi, zm, dt, cum, srb, og = acts
    y_loc, u_loc, dsb, bm, cmx, sz, xdt, xdtf, dy, rate, skp, tot, ecum, etail, dte = local
    def collect(which):
        blocks = [st[2 * zz + which].astype(F32) for zz in range(NZ)]
        rows = [blocks[zz][h * 8 : h * 8 + 8] for h in range(HEADS) for zz in range(NZ)]
        return jnp.concatenate(rows, axis=0)

    h0, ge = collect(0), collect(1)
    h0b, geb = h0.astype(BF16), ge.astype(BF16)
    y = y_loc + ecum * mm_t(cmx, h0b)
    ug = etail * mm_t(bm, geb)
    u = u_loc + ug
    dxa = dte * u + skp * dy
    ddt = exact(xa * u, hs)
    dcum = exact(dy * y - xdtf * u, hs)
    e_sum = jnp.sum(exact(xdtf * ug, hs), axis=0, keepdims=True)
    hg = exact(
        jnp.ones((8, STATE), F32), (h0 * ge).T
    )
    carry = jnp.exp(tot) * exact(hg, hs)[0:1]
    upper = one_hot(iota((TOK, TOK), 0) <= iota((TOK, TOK), 1))
    da = exact(upper, dcum) + e_sum + carry
    dsr = (ddt - rate * da) * jax.nn.sigmoid(srb)
    d_out = mm(dsb, bm) + mm((dy * ecum).astype(BF16), h0b)
    d_in = t_mm(dsb, cmx) + mm((xdt * etail).astype(BF16), geb)
    gm = jnp.concatenate([d_in, d_out], axis=1) * (sz * (1.0 + zm * (1.0 - sz)))
    si = jax.nn.sigmoid(zi)
    gi = dxa * (si * (1.0 + zi * (1.0 - si)))
    keep = jnp.where(iota((EXT, 1), 0) < PRE, flag, 1.0)

    def back(g, k):
        g = jnp.concatenate([jnp.zeros((PRE, g.shape[1]), F32), g], axis=0)
        return jnp.where(keep > 0.0, conv_back(g, k), 0.0).astype(BF16)

    gi_o[...] = back(gi, half_of(ci[...], c))
    gme = back(gm, cm[...])
    gm_o[...] = gme
    ds_o[...] = jnp.concatenate([jnp.zeros((PRE, 128), F32), dsr], axis=0).astype(BF16)
    eye = one_hot(iota((EXT, EXT), 0) == iota((EXT, EXT), 1)).astype(BF16)
    gmt = t_mm(gme, eye).astype(BF16)
    for j in range(8):
        gmt_o[j] = gmt[j * 32 : j * 32 + 32]


def sums_phase(
    norm, xe, gi_r, gm_r, ds_r, gmt, wih, wm, ws,
    tiles, fb, pown, xin, pbin,
    mixin, rb, yhold, yin, ra, a3, a4, a1, a2, sa, ya, sb, b3, b4, b1, b2, fa, fbs, p, psib, xhold,
    pb, pbsib,
    ms, mr, ys, yr, zs, zr, qs, qr, xs, xr, es, er, as_, ar, ts, tr, dsem, drem,
):
    dp = lax.axis_index("dp")
    z, yh, c, x = (lax.axis_index(a) for a in SEQ_CHAN)
    y = yh * 2 + dp
    j8 = c * 4 + x
    sib = 1 - c
    q = z * 2 + yh
    nq, pq = lax.rem(q + 1, 2 * NZ), lax.rem(q + 2 * NZ - 1, 2 * NZ)
    def at_z(off):
        return {"seq_0": lax.rem(z + off + NZ, NZ)}

    def at_y(off):
        k = lax.rem(y + off + 4, 4)
        return {"seq_1": k // 2, "dp": lax.rem(k, 2)}

    def at_x(off):
        return {"chan": lax.rem(x + off + 4, 4)}

    def at_j(k):
        return {"seq_2": k // 4, "chan": lax.rem(k, 4)}

    def remote(src, dst, ss, rs, where):
        return pltpu.make_async_remote_copy(
            src_ref=src, dst_ref=dst, send_sem=ss, recv_sem=rs, device_id=where,
            device_id_type=MESH,
        )

    pending = []

    def go(d):
        d.start()
        pending.append(d)
        return d

    for off in range(1, 8):
        to = lax.rem(j8 + off, 8)
        go(remote(gmt.at[to], mixin.at[off], ms.at[off], mr.at[off], at_j(to)))

    gi = gi_r[...]
    rhs = gi[:, :256]

    def inner_rows(side):
        for zhi in range(2):
            base = pl.multiple_of(side * 1280 + zhi * 640, 128)
            r = (t_mm(xe[:, pl.ds(base, 640)], rhs) * norm).astype(BF16)
            for g in range(8):
                for k in range(2):
                    rb[(g % 2) * 2 + side, zhi * 4 + g // 2, k] = r[
                        g * ROWS : (g + 1) * ROWS, k * 128 : (k + 1) * 128
                    ]

    up, down, far = lax.rem(y + 1, 4), lax.rem(y + 3, 4), lax.rem(y + 2, 4)
    lo, hi = pl.ds(0, 4), pl.ds(4, 4)
    inner_rows(dp)
    go(remote(rb.at[far, lo], yhold.at[0], ys.at[0], yr.at[0], at_y(1)))
    go(remote(rb.at[far, hi], yhold.at[1], ys.at[1], yr.at[1], at_y(-1)))
    inner_rows(1 - dp)
    go(remote(rb.at[up, hi], yin.at[0, hi], ys.at[2], yr.at[2], at_y(1)))
    go(remote(rb.at[down, lo], yin.at[1, lo], ys.at[3], yr.at[3], at_y(-1)))

    total = gmt[j8].astype(F32)
    for off in range(1, 8):
        origin = lax.rem(j8 + 8 - off, 8)
        remote(gmt.at[origin], mixin.at[off], ms.at[off], mr.at[off], at_j(origin)).wait_recv()
        total = total + mixin[off].astype(F32)
    place_mix = one_hot(iota((32, 128), 1) == iota((32, 128), 0) + 64).astype(BF16)
    place_step = one_hot(
        (iota((128, 128), 1) == iota((128, 128), 0) + 96) & (iota((128, 128), 0) < HEADS)
    ).astype(BF16)
    ds = ds_r[...]
    last = t_mm(total.astype(BF16), place_mix) + mm(ds, place_step)
    last = last + jnp.concatenate([gi[:, 256:].astype(F32), jnp.zeros((EXT, 64), F32)], axis=1)
    last = last.astype(BF16)
    for b in range(4):
        r = (t_mm(xe[:, b * 640 : (b + 1) * 640], last) * norm).astype(BF16)
        for g in range(8):
            ra[(b % 2) * 4 + g // 2, (g % 2) * 2 + b // 2] = r[g * ROWS : (g + 1) * ROWS]

    def z_first(src, n, r3, r4, r1, s, r):
        h = n // 2
        for k, sign in enumerate((1, -1)):
            part = pl.ds(k * h, h)
            dst = [lax.rem(z + sign * d + NZ, NZ) for d in range(5)]
            go(remote(src.at[dst[4], part], r4.at[k], s.at[4 * k], r.at[4 * k], at_z(2 * sign)))
            go(remote(src.at[dst[3]], r3.at[k], s.at[4 * k + 1], r.at[4 * k + 1], at_z(sign)))
            go(remote(src.at[dst[1]], r1.at[k], s.at[4 * k + 2], r.at[4 * k + 2], at_z(sign)))

    def z_second(src, n, r3, r4, r2, s, r):
        h = n // 2
        for k, sign in enumerate((1, -1)):
            part = pl.ds(k * h, h)
            t = lax.rem(z + 2 * sign + NZ, NZ)
            remote(r3.at[k], r3.at[k], s.at[4 * k + 1], r.at[4 * k + 1], at_z(sign)).wait_recv()
            remote(r4.at[k], r4.at[k], s.at[4 * k], r.at[4 * k], at_z(2 * sign)).wait_recv()
            for i in range(n):
                v = src[t, i].astype(F32) + r3[k, i].astype(F32)
                if k * h <= i < (k + 1) * h:
                    v = v + r4[k, i - k * h].astype(F32)
                r3[k, i] = v.astype(BF16)
            go(remote(r3.at[k], r2.at[k], s.at[4 * k + 3], r.at[4 * k + 3], at_z(2 * sign)))

    def z_last(r1, r2, s, r):
        for k, sign in enumerate((1, -1)):
            remote(r1.at[k], r1.at[k], s.at[4 * k + 2], r.at[4 * k + 2], at_z(sign)).wait_recv()
            remote(r2.at[k], r2.at[k], s.at[4 * k + 3], r.at[4 * k + 3], at_z(2 * sign)).wait_recv()

    z_first(ra, 4, a3, a4, a1, zs, zr)

    pick = head_pick(c).astype(BF16)
    ds10 = mm_t(ds, pick).astype(BF16)
    gm = gm_r[...]
    for b in range(4):
        rows = slice(b * 640, (b + 1) * 640)
        part = mm_t(gi, wih[rows]) + mm_t(gm, wm[rows]) + mm(ds10, ws[:, rows])
        part = part.astype(BF16)
        pb[:, rows] = part[:PRE]
        for j in range(8):
            for k in range(2):
                at = PRE + j * 32 + k * 16
                p[j // 4, j % 4, k, :, rows] = part[at : at + 16]
    go(remote(p.at[sib], psib, dsem.at[0], drem.at[0], {"seq_2": sib}))
    pb_out = remote(pb, pbsib, dsem.at[1], drem.at[1], {"seq_2": sib})

    @pl.when(c == 0)
    def _():
        pb_out.start()

    remote(yhold.at[0], yhold.at[0], ys.at[0], yr.at[0], at_y(1)).wait_recv()
    for i in range(4):
        yhold[0, i] = (rb[up, i].astype(F32) + yhold[0, i].astype(F32)).astype(BF16)
    go(remote(yhold.at[0], yin.at[0, lo], ys.at[4], yr.at[4], at_y(1)))
    remote(yhold.at[1], yhold.at[1], ys.at[1], yr.at[1], at_y(-1)).wait_recv()
    for i in range(4):
        yhold[1, i] = (rb[down, 4 + i].astype(F32) + yhold[1, i].astype(F32)).astype(BF16)
    go(remote(yhold.at[1], yin.at[1, hi], ys.at[5], yr.at[5], at_y(-1)))

    z_second(ra, 4, a3, a4, a2, zs, zr)

    remote(psib, psib, dsem.at[0], drem.at[0], {"seq_2": sib}).wait_recv()
    for k in range(4):
        for h in range(2):
            psib[k, h] = (p[c, k, h].astype(F32) + psib[k, h].astype(F32)).astype(BF16)
    xu, xd, xf = lax.rem(x + 1, 4), lax.rem(x + 3, 4), lax.rem(x + 2, 4)
    go(remote(psib.at[xf, 0], xhold.at[0], xs.at[0], xr.at[0], at_x(1)))
    go(remote(psib.at[xf, 1], xhold.at[1], xs.at[1], xr.at[1], at_x(-1)))
    go(remote(psib.at[xu, 1], xin.at[0, 1], xs.at[2], xr.at[2], at_x(1)))
    go(remote(psib.at[xd, 0], xin.at[1, 0], xs.at[3], xr.at[3], at_x(-1)))
    edge = remote(
        pbsib, pbin.at[x], es, er.at[x],
        {"seq_0": pq // 2, "seq_1": lax.rem(pq, 2), "chan": 3},
    )

    @pl.when(c == 1)
    def _():
        pb_out.wait_recv()
        pbsib[...] = (pb[...].astype(F32) + pbsib[...].astype(F32)).astype(BF16)
        edge.start()

    for k in (2, 4):
        part = hi if k == 2 else lo
        remote(yin.at[0, part], yin.at[0, part], ys.at[k], yr.at[k], at_y(1)).wait_recv()
    for k in (3, 5):
        part = lo if k == 3 else hi
        remote(yin.at[1, part], yin.at[1, part], ys.at[k], yr.at[k], at_y(-1)).wait_recv()
    for i in range(NZ):
        v = rb[y, i].astype(F32) + yin[0, i].astype(F32) + yin[1, i].astype(F32)
        sb[i] = v.astype(BF16)
    z_first(sb, 2, b3, b4, b1, qs, qr)

    z_last(a1, a2, zs, zr)
    for i in range(4):
        v = ra[z, i].astype(F32)
        for k in range(2):
            v = v + a1[k, i].astype(F32) + a2[k, i].astype(F32)
        sa[i] = v.astype(BF16)
    for off in (2, 1, 3):
        to = lax.rem(y + off, 4)
        go(remote(sa.at[to], ya.at[off], as_.at[off], ar.at[off], at_y(off)))

    remote(xhold.at[0], xhold.at[0], xs.at[0], xr.at[0], at_x(1)).wait_recv()
    xhold[0] = (psib[xu, 0].astype(F32) + xhold[0].astype(F32)).astype(BF16)
    go(remote(xhold.at[0], xin.at[0, 0], xs.at[4], xr.at[4], at_x(1)))
    remote(xhold.at[1], xhold.at[1], xs.at[1], xr.at[1], at_x(-1)).wait_recv()
    xhold[1] = (psib[xd, 1].astype(F32) + xhold[1].astype(F32)).astype(BF16)
    go(remote(xhold.at[1], xin.at[1, 1], xs.at[5], xr.at[5], at_x(-1)))
    pown[...] = psib[x]

    z_second(sb, 2, b3, b4, b2, qs, qr)

    v = sa[y].astype(F32)
    for off in range(1, 4):
        remote(ya.at[off], ya.at[off], as_.at[off], ar.at[off], at_y(off)).wait_recv()
        v = v + ya[off].astype(F32)
    fa[0] = v[:40]
    fa[1] = v[40:]
    for off in range(1, 8):
        to = lax.rem(j8 + off, 8)
        go(remote(fa.at[to // 4], tiles.at[j8], ts.at[off], tr.at[off], at_j(to)))
    tiles[j8] = fa[c]

    z_last(b1, b2, qs, qr)
    for i in range(2):
        v = sb[z, i].astype(F32)
        for k in range(2):
            v = v + b1[k, i].astype(F32) + b2[k, i].astype(F32)
        fbs[0, :, i * 128 : (i + 1) * 128] = v[:40]
        fbs[1, :, i * 128 : (i + 1) * 128] = v[40:]
    go(remote(fbs.at[sib], fb.at[c], dsem.at[2], drem.at[2], {"seq_2": sib}))
    fb[c] = fbs[c]

    for k, half in ((2, 1), (4, 0)):
        remote(xin.at[0, half], xin.at[0, half], xs.at[k], xr.at[k], at_x(1)).wait_recv()
    for k, half in ((3, 0), (5, 1)):
        remote(xin.at[1, half], xin.at[1, half], xs.at[k], xr.at[k], at_x(-1)).wait_recv()
    for off in range(1, 8):
        origin = lax.rem(j8 + 8 - off, 8)
        remote(fa.at[c], tiles.at[origin], ts.at[off], tr.at[off], at_j(origin)).wait_recv()

    @pl.when((c == 1) & (x == 3))
    def _():
        for k in range(4):
            remote(pbsib, pbin.at[k], es, er.at[k], {"chan": 0}).wait_recv()

    remote(fbs.at[c], fb.at[sib], dsem.at[2], drem.at[2], {"seq_2": sib}).wait_recv()
    for d in pending:
        d.wait_send()

    @pl.when(c == 0)
    def _():
        pb_out.wait_send()

    @pl.when(c == 1)
    def _():
        edge.wait_send()


def whole_kernel(
    norm,
    piece, og, wi_h, wm_h, ws_h, ci_h, cm_h, bias_h, dlog_h, skip_h,
    tiles, fb, pown, xin, pbin,
    xe, ogx, wi, wm, ws, ci, cm, bias, dlog, skip, wih, send, recv, back, st, gi, gm, ds, gmt,
    gs, gr, gt, hsem, lsem, s1, r1, s2, r2, *rest,
):
    dp = lax.axis_index("dp")
    z, yh, c, x = (lax.axis_index(a) for a in SEQ_CHAN)
    n = 2 * NZ
    q = z * 2 + yh
    nq, pq = lax.rem(q + 1, n), lax.rem(q + n - 1, n)
    corner = (c == 1) & (x == 3)
    barrier = pltpu.get_barrier_semaphore()

    def tell(**where):
        pl.semaphore_signal(barrier, inc=1, device_id=where, device_id_type=MESH)

    for off in range(1, 8):
        k = lax.rem(c * 4 + x + off, 8)
        tell(seq_2=k // 4, chan=lax.rem(k, 4))
    for off in (1, 3):
        k = lax.rem(yh * 2 + dp + off, 4)
        tell(seq_1=k // 2, dp=lax.rem(k, 2))
    for off in range(1, n):
        k = lax.rem(q + off, n)
        tell(seq_0=k // 2, seq_1=lax.rem(k, 2))

    @pl.when(c == 1)
    def _():
        tell(seq_0=pq // 2, seq_1=lax.rem(pq, 2), chan=3)

    @pl.when(corner)
    def _():
        for k in range(4):
            tell(seq_0=nq // 2, seq_1=lax.rem(nq, 2), chan=k)

    base = pl.multiple_of(PRE + (c * 4 + x) * 32, 16)
    loads = [pltpu.make_async_copy(piece, xe.at[pl.ds(base, 32), :], hsem.at[0])]
    loads.append(pltpu.make_async_copy(og, ogx.at[c], hsem.at[1]))
    pairs = ((wi_h, wi), (wm_h, wm), (ws_h, ws), (ci_h, ci), (cm_h, cm))
    pairs += ((bias_h, bias), (dlog_h, dlog), (skip_h, skip))
    for k, (src, dst) in enumerate(pairs):
        loads.append(pltpu.make_async_copy(src, dst, hsem.at[2 + k]))
    for d in loads:
        d.start()
    loads[0].wait()
    loads[1].wait()
    pl.semaphore_wait(
        barrier, jnp.where(corner, 7 + 2 + n - 1 + 5, jnp.where(c == 1, 7 + 2 + n, 7 + 2 + n - 1))
    )
    gather_phase(xe, ogx, gs, gr, gt)
    for d in loads[2:]:
        d.wait()
    acts = forward_phase(xe, ogx, wi, wm, ws, ci, cm, bias, dlog, wih, send)
    begin, turn, end = state_phases(send, st, recv, back, lsem, s1, r1, s2, r2)
    begin()
    local = local_phase(acts, dlog, skip)
    turn()
    end()
    carried_phase(acts, local, st, ci, cm, gi, gm, ds, gmt)
    sums_phase(norm, xe, gi, gm, ds, gmt, wih, wm, ws, tiles, fb, pown, xin, pbin, *rest)


def whole(norm, *args):
    dma = pltpu.SemaphoreType.DMA
    n = 2 * NZ

    def vm(*shape):
        return pltpu.VMEM(shape, BF16)

    return pl.pallas_call(
        functools.partial(whole_kernel, norm),
        out_shape=(
            jax.ShapeDtypeStruct((8, 40, 128), F32),
            jax.ShapeDtypeStruct((2, 40, 256), F32),
            jax.ShapeDtypeStruct((2, 16, D), BF16),
            jax.ShapeDtypeStruct((2, 2, 16, D), BF16),
            jax.ShapeDtypeStruct((4, PRE, D), BF16),
        ),
        in_specs=[pl.BlockSpec(memory_space=pltpu.HBM)] * 10,
        out_specs=(VM,) * 5,
        scratch_shapes=[
            vm(EXT, D), vm(2, TOK // 2, 2 * INNER), vm(D, 2 * INNER), vm(D, 2 * STATE), vm(10, D),
            pltpu.VMEM((4, 2 * INNER), F32), pltpu.VMEM((4, 2 * STATE), F32),
            pltpu.VMEM((1, 10), F32), pltpu.VMEM((1, 10), F32), pltpu.VMEM((1, 10), F32),
            vm(D, INNER), vm(n, CHUNK, STATE), vm(n, CHUNK, STATE), vm(n, CHUNK, STATE),
            vm(n, CHUNK, STATE), vm(EXT, INNER), vm(EXT, 2 * STATE), vm(EXT, 128), vm(8, 32, EXT),
            dma((13,)), dma((13,)), dma((4,)), dma((10,)), dma((2,)),
            dma((n,)), dma((n,)), dma((n,)), dma((n,)),
            vm(8, 32, EXT),
            vm(4, NZ, 2, ROWS, 128), vm(2, 4, 2, ROWS, 128), vm(2, NZ, 2, ROWS, 128),
            vm(NZ, 4, ROWS, 128), vm(2, 4, ROWS, 128), vm(2, 2, ROWS, 128),
            vm(2, 4, ROWS, 128), vm(2, 4, ROWS, 128), vm(4, ROWS, 128), vm(4, ROWS, 128),
            vm(NZ, 2, ROWS, 128), vm(2, 2, ROWS, 128), vm(2, 1, ROWS, 128),
            vm(2, 2, ROWS, 128), vm(2, 2, ROWS, 128),
            pltpu.VMEM((2, 40, 128), F32), pltpu.VMEM((2, 40, 256), F32),
            vm(2, 4, 2, 16, D), vm(4, 2, 16, D), vm(2, 16, D), vm(PRE, D), vm(PRE, D),
            dma((8,)), dma((8,)), dma((6,)), dma((6,)), dma((8,)), dma((8,)),
            dma((8,)), dma((8,)), dma((6,)), dma((6,)), dma(()), dma((4,)), dma((4,)), dma((4,)),
            dma((8,)), dma((8,)), dma((3,)), dma((3,)),
        ],
        compiler_params=pltpu.CompilerParams(
            collective_id=0, has_side_effects=True, vmem_limit_bytes=LIMIT
        ),
        name="whole",
    )(*args)


def finish_kernel(tiles, fb, pown, xin, pbin, ig_o, iw_o, mw_o, sw_o):
    c, x = lax.axis_index("seq_2"), lax.axis_index("chan")
    for k in range(2):
        iw_o[:, k * INNER : k * INNER + 256] = fb[k]
        own = tiles[k * 4 + x]
        iw_o[:, k * INNER + 256 : (k + 1) * INNER] = own[:, :64]
        sw_o[:, k * HEADS : (k + 1) * HEADS] = own[:, 96 : 96 + HEADS]
    rows = one_hot(iota((10, 40), 1) == iota((10, 40), 0) + 10 * x)
    for j in range(8):
        mw_o[:, j * 32 : (j + 1) * 32] = exact(rows, tiles[j])[:, 64:96]
    for h in range(2):
        acc = pown[h].astype(F32) + xin[0, h].astype(F32) + xin[1, h].astype(F32)
        ig_o[h * 16 : (h + 1) * 16, :] = acc.astype(BF16)

    @pl.when((c == 1) & (x == 3))
    def _():
        edge = pown[1].astype(F32) + xin[0, 1].astype(F32) + xin[1, 1].astype(F32)
        for j in range(4):
            edge = edge + pbin[j].astype(F32)
        ig_o[16:, :] = edge.astype(BF16)


def finish(*args):
    return pl.pallas_call(
        finish_kernel,
        out_shape=(
            jax.ShapeDtypeStruct((32, D), BF16),
            jax.ShapeDtypeStruct((40, 2 * INNER), F32),
            jax.ShapeDtypeStruct((10, 2 * STATE), F32),
            jax.ShapeDtypeStruct((40, 2 * HEADS), F32),
        ),
        in_specs=[VM] * 5,
        out_specs=(VM,) * 4,
        compiler_params=pltpu.CompilerParams(vmem_limit_bytes=LIMIT),
        name="finish",
    )(*args)


def body(
    layer_input,
    inner_weight,
    mixer_weight,
    step_weight,
    conv_inner,
    conv_mixer,
    step_bias,
    decay_log,
    skip_gain,
    output_grad,
):
    norm = 1.0 / math.sqrt(8192)
    stepw = step_weight.T
    bias, dlog, skip = (v.reshape(1, -1) for v in (step_bias, decay_log, skip_gain))
    parts = whole(
        norm, layer_input[0], output_grad[0], inner_weight, mixer_weight, stepw, conv_inner,
        conv_mixer, bias, dlog, skip,
    )
    ig, iw, mw, sw = finish(*parts)
    return ig[None], iw, mw, sw


def solution(mesh):
    split = Mesh(
        mesh.devices.reshape(mesh.shape["dp"], 8, 2, 2, mesh.shape["chan"]),
        ("dp", "seq_0", "seq_1", "seq_2", "chan"),
    )
    placed = (
        P("dp", SEQ_CHAN, None),
        P(None, "chan"),
        P(),
        P(None, "chan"),
        P(None, "chan"),
        P(),
        P("chan"),
        P("chan"),
        P("chan"),
        P("dp", SEQ, "chan"),
    )
    return jax.shard_map(
        body,
        mesh=split,
        in_specs=placed,
        out_specs=(
            P("dp", SEQ_CHAN, None),
            P(DP_SEQ, "chan"),
            P(DP_SEQ_CHAN, None),
            P(DP_SEQ, "chan"),
        ),
        check_vma=False,
    )
```

```python
import functools
import math

import jax
import jax.numpy as jnp
from jax import lax
from jax.experimental import pallas as pl
from jax.experimental.pallas import tpu as pltpu
from jax.sharding import Mesh
from jax.sharding import PartitionSpec as P

D = 2560
HDIM = 64
HEADS = 5
INNER = HEADS * HDIM
STATE = 128
TOK = 256
PRE = 16
EXT = TOK + PRE
NZ = 8
ROWS = 80
CHUNK = 48
F32 = jnp.float32
BF16 = jnp.bfloat16
SEQ = ("seq_0", "seq_1", "seq_2")
DP_SEQ = ("dp", "seq_0", "seq_1", "seq_2")
SEQ_CHAN = ("seq_0", "seq_1", "seq_2", "chan")
DP_SEQ_CHAN = ("dp", "seq_0", "seq_1", "seq_2", "chan")
MESH = pl.DeviceIdType.MESH
VM = pl.BlockSpec(memory_space=pltpu.VMEM)
LIMIT = 62 * 1024 * 1024


def roll(v, shift):
    return pltpu.roll(v, shift % v.shape[0], 0)


def mm(a, b):
    return jnp.dot(a, b, preferred_element_type=F32)


def mm_t(a, b):
    return lax.dot_general(a, b, (((1,), (1,)), ((), ())), preferred_element_type=F32)


def t_mm(a, b):
    return lax.dot_general(a, b, (((0,), (0,)), ((), ())), preferred_element_type=F32)


def exact(a, b):
    return jnp.dot(a, b, preferred_element_type=F32, precision=lax.Precision.HIGHEST)


def iota(shape, dim):
    return lax.broadcasted_iota(jnp.int32, shape, dim)


def one_hot(cond):
    return jnp.where(cond, 1.0, 0.0).astype(F32)


def head_expand():
    return one_hot(iota((128, INNER), 1) // HDIM == iota((128, INNER), 0))


def head_sum():
    return one_hot(iota((INNER, 128), 0) // HDIM == iota((INNER, 128), 1))


def head_pick(core):
    return one_hot(
        (iota((10, 128), 0) == iota((10, 128), 1) + HEADS * core) & (iota((10, 128), 1) < HEADS)
    )


def half_of(v, core):
    return jnp.where(core == 0, v[:, :INNER], v[:, INNER:])


def conv(v, k):
    return k[3:4] * v + k[2:3] * roll(v, 1) + k[1:2] * roll(v, 2) + k[0:1] * roll(v, 3)


def conv_back(g, k):
    return k[3:4] * g + k[2:3] * roll(g, -1) + k[1:2] * roll(g, -2) + k[0:1] * roll(g, -3)


def gather_phase(xe, ogx, ssem, rsem, tsem):
    z, yh, c, x = (lax.axis_index(a) for a in SEQ_CHAN)
    right, left = lax.rem(x + 1, 4), lax.rem(x + 3, 4)
    sib = 1 - c
    q = z * 2 + yh
    nq, pq = lax.rem(q + 1, 2 * NZ), lax.rem(q + 2 * NZ - 1, 2 * NZ)
    def slot(core, chan, half=None):
        base = PRE + (core * 4 + chan) * 32
        if half is None:
            return xe.at[pl.ds(pl.multiple_of(base, 16), 32), :]
        return xe.at[pl.ds(pl.multiple_of(base + 16 * half, 16), 16), :]

    def copy(src, dst, k, **where):
        return pltpu.make_async_remote_copy(
            src_ref=src, dst_ref=dst, send_sem=ssem.at[k], recv_sem=rsem.at[k],
            device_id=where, device_id_type=MESH,
        )

    mine = slot(c, x)
    own_og = ogx.at[c]

    def half(h):
        return slot(c, x, h)

    r0 = copy(half(0), slot(c, x, 0), 0, chan=right)
    l1 = copy(half(1), slot(c, x, 1), 1, chan=left)
    r1 = copy(half(1), slot(c, x, 1), 2, chan=right)
    l0 = copy(half(0), slot(c, x, 0), 3, chan=left)
    sp = copy(mine, mine, 4, seq_2=sib)
    so = copy(own_og, own_og, 5, seq_2=sib)
    for d in (r0, l1):
        d.start()

    def tails(chan):
        return pltpu.make_async_remote_copy(
            src_ref=half(1), dst_ref=xe.at[pl.ds(0, 16), :], send_sem=tsem.at[chan],
            recv_sem=rsem.at[6],
            device_id={"seq_0": nq // 2, "seq_1": lax.rem(nq, 2), "chan": chan},
            device_id_type=MESH,
        )

    @pl.when((c == 1) & (x == 3))
    def _():
        for chan in range(4):
            tails(chan).start()

    for d in (r1, l0, sp, so):
        d.start()
    far = lax.rem(x + 2, 4)
    in_r0 = copy(half(0), slot(c, left, 0), 0, chan=right)
    in_r1 = copy(half(1), slot(c, left, 1), 2, chan=right)
    in_l1 = copy(half(1), slot(c, right, 1), 1, chan=left)
    in_l0 = copy(half(0), slot(c, right, 0), 3, chan=left)
    rr = copy(slot(c, left, 0), slot(c, left, 0), 7, chan=right)
    ll = copy(slot(c, right, 1), slot(c, right, 1), 8, chan=left)
    in_r0.wait_recv()
    rr.start()
    in_l1.wait_recv()
    ll.start()
    in_r1.wait_recv()
    s_left = copy(slot(c, left), slot(c, left), 9, seq_2=sib)
    s_left.start()
    in_l0.wait_recv()
    s_right = copy(slot(c, right), slot(c, right), 10, seq_2=sib)
    s_right.start()
    tail_on = copy(xe.at[pl.ds(0, 16), :], xe.at[pl.ds(0, 16), :], 12, seq_2=sib)

    @pl.when(c == 1)
    def _():
        tails(0).wait_recv()
        tail_on.start()

    in_rr = copy(half(0), slot(c, far, 0), 7, chan=right)
    in_ll = copy(half(1), slot(c, far, 1), 8, chan=left)
    in_rr.wait_recv()
    in_ll.wait_recv()
    s_far = copy(slot(c, far), slot(c, far), 11, seq_2=sib)
    s_far.start()
    copy(mine, slot(sib, x), 4, seq_2=sib).wait_recv()
    copy(own_og, ogx.at[sib], 5, seq_2=sib).wait_recv()
    copy(mine, slot(sib, left), 9, seq_2=sib).wait_recv()
    copy(mine, slot(sib, right), 10, seq_2=sib).wait_recv()
    copy(mine, slot(sib, far), 11, seq_2=sib).wait_recv()

    @pl.when(c == 0)
    def _():
        tail_on.wait_recv()

    for d in (r0, l1, r1, l0, sp, so, rr, ll, s_left, s_right, s_far):
        d.wait_send()

    @pl.when(c == 1)
    def _():
        tail_on.wait_send()

    @pl.when((c == 1) & (x == 3))
    def _():
        for chan in range(4):
            tails(chan).wait_send()


def forward_phase(xe, ogx, wi, wm, ws, ci, cm, bias, dlog, wih_o, send_o):
    z, yh, c = (lax.axis_index(a) for a in SEQ)
    flag = jnp.where(z * 2 + yh == 0, 0.0, 1.0).astype(F32)
    pick = head_pick(c)
    wih = half_of(wi[...], c)
    wih_o[...] = wih
    xv = xe[...]
    keep = jnp.where(iota((EXT, 1), 0) < PRE, flag, 1.0)

    def masked(v):
        return jnp.where(keep > 0.0, v.astype(BF16).astype(F32), 0.0)

    pi = masked(mm(xv, wih))
    pm = masked(mm(xv, wm[...]))
    sr = exact(mm_t(xv, ws[...])[PRE:], pick)
    zi = conv(pi, half_of(ci[...], c))[PRE:]
    zm = conv(pm, cm[...])[PRE:]
    xa = zi * jax.nn.sigmoid(zi)
    ma = zm * jax.nn.sigmoid(zm)
    srb = sr + exact(bias[...], pick)
    dt = jnp.maximum(srb, 0.0) + jnp.log1p(jnp.exp(-jnp.abs(srb)))
    rate = exact(jnp.exp(dlog[...]), pick)
    a = -dt * rate
    tri = one_hot(iota((TOK, TOK), 0) >= iota((TOK, TOK), 1))
    cum = exact(tri, a)
    tot = cum[TOK - 1 : TOK]
    og = half_of(ogx[...].reshape(TOK, 2 * INNER), c)
    ex = head_expand()
    xt = (xa * exact(dt * jnp.exp(tot - cum), ex)).astype(BF16)
    yt = (og.astype(F32) * exact(jnp.exp(cum), ex)).astype(BF16)
    f_loc = t_mm(xt, ma[:, :STATE].astype(BF16))
    g_loc = t_mm(yt, ma[:, STATE:].astype(BF16))
    diag = jnp.where(iota((8, 128), 0) == iota((8, 128), 1), tot, 0.0)
    dm = exact(diag, jnp.ones((128, 128), F32))
    hi = dm.astype(BF16).astype(F32)
    drow = jnp.where(iota((8, 128), 1) < 64, hi, dm - hi)
    for zz in range(NZ):
        for which, v in ((0, f_loc), (1, g_loc)):
            rows = [v[h * HDIM + zz * 8 : h * HDIM + zz * 8 + 8] for h in range(HEADS)]
            send_o[zz * 2 + which] = jnp.concatenate(rows + [drow], axis=0).astype(BF16)
    return xa, zi, zm, dt, cum, srb, og


def state_phases(send, out, recv, back, local_sem, s1, r1, s2, r2):
    z, yh = lax.axis_index("seq_0"), lax.axis_index("seq_1")
    n = 2 * NZ
    me = z * 2 + yh
    def at(q):
        return {"seq_0": q // 2, "seq_1": lax.rem(q, 2)}

    def push(src, dst, ss, rs, off):
        to = lax.rem(me + off, n)
        return pltpu.make_async_remote_copy(
            src_ref=src.at[to], dst_ref=dst.at[me], send_sem=ss.at[off], recv_sem=rs.at[off],
            device_id=at(to), device_id_type=MESH,
        )

    def pull(src, dst, ss, rs, off):
        origin = lax.rem(me + n - off, n)
        return pltpu.make_async_remote_copy(
            src_ref=src.at[origin], dst_ref=dst.at[origin], send_sem=ss.at[off],
            recv_sem=rs.at[off], device_id=at(origin), device_id_type=MESH,
        )

    first = [push(send, recv, s1, r1, off) for off in range(1, n)]
    second = [push(back, out, s2, r2, off) for off in range(1, n)]

    def begin():
        for d in first:
            d.start()
        own = pltpu.make_async_copy(send.at[me], recv.at[me], local_sem.at[0])
        own.start()
        own.wait()

    def turn():
        for off in range(1, n):
            pull(send, recv, s1, r1, off).wait_recv()
        run = jnp.zeros((HEADS * 8, STATE), F32)
        for j in range(n):
            k = jnp.where(yh == 0, j, n - 1 - j)
            got = recv[k].astype(F32)
            rows = got[HEADS * 8 :]
            rows = rows + pltpu.roll(rows, 64, 1)
            decay = jnp.exp(rows)
            back[k] = jnp.concatenate([run, rows], axis=0).astype(BF16)
            wide = jnp.concatenate(
                [jnp.broadcast_to(decay[h : h + 1], (8, STATE)) for h in range(HEADS)], axis=0
            )
            run = wide * run + got[: HEADS * 8]
        for d in second:
            d.start()
        own = pltpu.make_async_copy(back.at[me], out.at[me], local_sem.at[1])
        own.start()
        own.wait()

    def end():
        for off in range(1, n):
            pull(back, out, s2, r2, off).wait_recv()
        for d in first + second:
            d.wait_send()

    return begin, turn, end


def local_phase(acts, dlog, skip):
    c = lax.axis_index("seq_2")
    pick = head_pick(c)
    ex = head_expand()
    xa, zi, zm, dt, cum, srb, og = acts
    dy = og.astype(F32)
    rate = exact(jnp.exp(dlog[...]), pick)
    skp = exact(skip[...], pick)
    tot = cum[TOK - 1 : TOK]
    ecum = exact(jnp.exp(cum), ex)
    etail = exact(jnp.exp(tot - cum), ex)
    dte = exact(dt, ex)
    sz = jax.nn.sigmoid(zm)
    ma = zm * sz
    bm, cmx = ma[:, :STATE].astype(BF16), ma[:, STATE:].astype(BF16)
    xdt = xa * dte
    xdtb = xdt.astype(BF16)
    xdtf = xdtb.astype(F32)
    scores = mm_t(cmx, bm)
    causal = iota((TOK, TOK), 0) >= iota((TOK, TOK), 1)
    cumt = cum.T
    dscore = jnp.zeros((TOK, TOK), F32)
    ys, us = [], []
    for h in range(HEADS):
        cols = slice(h * HDIM, (h + 1) * HDIM)
        decay = jnp.exp(jnp.where(causal, cum[:, h : h + 1] - cumt[h : h + 1, :], -1e30))
        m = (decay * scores).astype(BF16)
        ys.append(mm(m, xdtb[:, cols]))
        us.append(t_mm(m, og[:, cols]))
        dscore = dscore + decay * mm_t(og[:, cols], xdtb[:, cols])
    dsb = dscore.astype(BF16)
    d_out, d_in = mm(dsb, bm), t_mm(dsb, cmx)
    yt, xt = (dy * ecum).astype(BF16), (xdt * etail).astype(BF16)
    gate_m = sz * (1.0 + zm * (1.0 - sz))
    si = jax.nn.sigmoid(zi)
    gate_i = si * (1.0 + zi * (1.0 - si))
    return (
        jnp.concatenate(ys, axis=1), jnp.concatenate(us, axis=1), d_out, d_in, yt, xt, gate_m,
        gate_i, bm, cmx, xdtf, dy, rate, exact(skp, ex), tot, ecum, etail, dte,
    )


def carried_phase(acts, local, st, ci, cm, gi_o, gm_o, ds_o, gmt_o, send_mix):
    z, yh, c = (lax.axis_index(a) for a in SEQ)
    flag = jnp.where(z * 2 + yh == 0, 0.0, 1.0).astype(F32)
    hs = head_sum()
    xa, _, _, _, _, srb, _ = acts
    (
        y_loc, u_loc, d_out, d_in, yt, xt, gate_m, gate_i, bm, cmx, xdtf, dy, rate, skp, tot,
        ecum, etail, dte,
    ) = local
    keep = jnp.where(iota((EXT, 1), 0) < PRE, flag, 1.0)

    def collect(which):
        blocks = [st[2 * zz + which].astype(F32) for zz in range(NZ)]
        rows = [blocks[zz][h * 8 : h * 8 + 8] for h in range(HEADS) for zz in range(NZ)]
        return jnp.concatenate(rows, axis=0)

    def back(g, k):
        g = jnp.concatenate([jnp.zeros((PRE, g.shape[1]), F32), g], axis=0)
        return jnp.where(keep > 0.0, conv_back(g, k), 0.0).astype(BF16)

    h0, ge = collect(0), collect(1)
    h0b, geb = h0.astype(BF16), ge.astype(BF16)
    gm = jnp.concatenate([d_in + mm(xt, geb), d_out + mm(yt, h0b)], axis=1) * gate_m
    gme = back(gm, cm[...])
    gm_o[...] = gme
    eye = one_hot(iota((EXT, EXT), 0) == iota((EXT, EXT), 1)).astype(BF16)
    gmt = t_mm(gme, eye).astype(BF16)
    for j in range(8):
        gmt_o[j] = gmt[j * 32 : j * 32 + 32]
    ug = etail * mm_t(bm, geb)
    u = u_loc + ug
    gi_o[...] = back((dte * u + skp * dy) * gate_i, half_of(ci[...], c))
    send_mix()
    y = y_loc + ecum * mm_t(cmx, h0b)
    ddt = exact(xa * u, hs)
    dcum = exact(dy * y - xdtf * u, hs)
    e_sum = jnp.sum(exact(xdtf * ug, hs), axis=0, keepdims=True)
    hg = exact(jnp.ones((8, STATE), F32), (h0 * ge).T)
    carry = jnp.exp(tot) * exact(hg, hs)[0:1]
    upper = one_hot(iota((TOK, TOK), 0) <= iota((TOK, TOK), 1))
    da = exact(upper, dcum) + e_sum + carry
    dsr = (ddt - rate * da) * jax.nn.sigmoid(srb)
    ds_o[...] = jnp.concatenate([jnp.zeros((PRE, 128), F32), dsr], axis=0).astype(BF16)


def sums_phase(
    norm, carry_on, xe, gi_r, gm_r, ds_r, gmt, wih, wm, ws,
    mt, fat, fb, pown, xin, pbin,
    mixin, rb, yhold, yin, ra, a3, a4, a1, a2, sa, ya, sb, b3, b4, b1, b2, fa, mrows, fbs, p, psib, xhold,
    pb, pbsib,
    ms, mr, ys, yr, zs, zr, qs, qr, xs, xr, es, er, as_, ar, ts, tr, dsem, drem,
):
    dp = lax.axis_index("dp")
    z, yh, c, x = (lax.axis_index(a) for a in SEQ_CHAN)
    y = yh * 2 + dp
    j8 = c * 4 + x
    sib = 1 - c
    q = z * 2 + yh
    nq, pq = lax.rem(q + 1, 2 * NZ), lax.rem(q + 2 * NZ - 1, 2 * NZ)
    def at_z(off):
        return {"seq_0": lax.rem(z + off + NZ, NZ)}

    def at_y(off):
        k = lax.rem(y + off + 4, 4)
        return {"seq_1": k // 2, "dp": lax.rem(k, 2)}

    def at_x(off):
        return {"chan": lax.rem(x + off + 4, 4)}

    def at_j(k):
        return {"seq_2": k // 4, "chan": lax.rem(k, 4)}

    def remote(src, dst, ss, rs, where):
        return pltpu.make_async_remote_copy(
            src_ref=src, dst_ref=dst, send_sem=ss, recv_sem=rs, device_id=where,
            device_id_type=MESH,
        )

    pending = []

    def go(d):
        d.start()
        pending.append(d)
        return d

    def send_mix():
        for off in range(1, 8):
            to = lax.rem(j8 + off, 8)
            go(remote(gmt.at[to], mixin.at[off], ms.at[off], mr.at[off], at_j(to)))

    carry_on(send_mix)

    gi = gi_r[...]
    rhs = gi[:, :256]

    def inner_rows(side):
        for zhi in range(2):
            base = pl.multiple_of(side * 1280 + zhi * 640, 128)
            r = (t_mm(xe[:, pl.ds(base, 640)], rhs) * norm).astype(BF16)
            for g in range(8):
                for k in range(2):
                    rb[(g % 2) * 2 + side, zhi * 4 + g // 2, k] = r[
                        g * ROWS : (g + 1) * ROWS, k * 128 : (k + 1) * 128
                    ]

    up, down, far = lax.rem(y + 1, 4), lax.rem(y + 3, 4), lax.rem(y + 2, 4)
    lo, hi = pl.ds(0, 4), pl.ds(4, 4)
    inner_rows(dp)
    go(remote(rb.at[far, lo], yhold.at[0], ys.at[0], yr.at[0], at_y(1)))
    go(remote(rb.at[far, hi], yhold.at[1], ys.at[1], yr.at[1], at_y(-1)))
    inner_rows(1 - dp)
    go(remote(rb.at[up, hi], yin.at[0, hi], ys.at[2], yr.at[2], at_y(1)))
    go(remote(rb.at[down, lo], yin.at[1, lo], ys.at[3], yr.at[3], at_y(-1)))

    ds = ds_r[...]
    pick = head_pick(c).astype(BF16)
    ds10 = mm_t(ds, pick).astype(BF16)
    gm = gm_r[...]
    for b in range(4):
        rows = slice(b * 640, (b + 1) * 640)
        part = mm_t(gi, wih[rows]) + mm_t(gm, wm[rows]) + mm(ds10, ws[:, rows])
        part = part.astype(BF16)
        pb[:, rows] = part[:PRE]
        for j in range(8):
            for k in range(2):
                at = PRE + j * 32 + k * 16
                p[j // 4, j % 4, k, :, rows] = part[at : at + 16]
    go(remote(p.at[sib], psib, dsem.at[0], drem.at[0], {"seq_2": sib}))
    pb_out = remote(pb, pbsib, dsem.at[1], drem.at[1], {"seq_2": sib})

    @pl.when(c == 0)
    def _():
        pb_out.start()

    total = gmt[j8].astype(F32)
    for off in range(1, 8):
        origin = lax.rem(j8 + 8 - off, 8)
        remote(gmt.at[origin], mixin.at[off], ms.at[off], mr.at[off], at_j(origin)).wait_recv()
        total = total + mixin[off].astype(F32)
    place_mix = one_hot(iota((32, 128), 1) == iota((32, 128), 0) + 64).astype(BF16)
    place_step = one_hot(
        (iota((128, 128), 1) == iota((128, 128), 0) + 96) & (iota((128, 128), 0) < HEADS)
    ).astype(BF16)
    last = t_mm(total.astype(BF16), place_mix) + mm(ds, place_step)
    last = last + jnp.concatenate([gi[:, 256:].astype(F32), jnp.zeros((EXT, 64), F32)], axis=1)
    last = last.astype(BF16)
    for b in range(4):
        r = (t_mm(xe[:, b * 640 : (b + 1) * 640], last) * norm).astype(BF16)
        for g in range(8):
            ra[(b % 2) * 4 + g // 2, (g % 2) * 2 + b // 2] = r[g * ROWS : (g + 1) * ROWS]

    def z_first(src, n, r3, r4, r1, s, r):
        h = n // 2
        for k, sign in enumerate((1, -1)):
            part = pl.ds(k * h, h)
            dst = [lax.rem(z + sign * d + NZ, NZ) for d in range(5)]
            go(remote(src.at[dst[4], part], r4.at[k], s.at[4 * k], r.at[4 * k], at_z(2 * sign)))
            go(remote(src.at[dst[3]], r3.at[k], s.at[4 * k + 1], r.at[4 * k + 1], at_z(sign)))
            go(remote(src.at[dst[1]], r1.at[k], s.at[4 * k + 2], r.at[4 * k + 2], at_z(sign)))

    def z_second(src, n, r3, r4, r2, s, r):
        h = n // 2
        for k, sign in enumerate((1, -1)):
            part = pl.ds(k * h, h)
            t = lax.rem(z + 2 * sign + NZ, NZ)
            remote(r3.at[k], r3.at[k], s.at[4 * k + 1], r.at[4 * k + 1], at_z(sign)).wait_recv()
            remote(r4.at[k], r4.at[k], s.at[4 * k], r.at[4 * k], at_z(2 * sign)).wait_recv()
            for i in range(n):
                v = src[t, i].astype(F32) + r3[k, i].astype(F32)
                if k * h <= i < (k + 1) * h:
                    v = v + r4[k, i - k * h].astype(F32)
                r3[k, i] = v.astype(BF16)
            go(remote(r3.at[k], r2.at[k], s.at[4 * k + 3], r.at[4 * k + 3], at_z(2 * sign)))

    def z_last(r1, r2, s, r):
        for k, sign in enumerate((1, -1)):
            remote(r1.at[k], r1.at[k], s.at[4 * k + 2], r.at[4 * k + 2], at_z(sign)).wait_recv()
            remote(r2.at[k], r2.at[k], s.at[4 * k + 3], r.at[4 * k + 3], at_z(2 * sign)).wait_recv()

    z_first(ra, 4, a3, a4, a1, zs, zr)

    remote(yhold.at[0], yhold.at[0], ys.at[0], yr.at[0], at_y(1)).wait_recv()
    for i in range(4):
        yhold[0, i] = (rb[up, i].astype(F32) + yhold[0, i].astype(F32)).astype(BF16)
    go(remote(yhold.at[0], yin.at[0, lo], ys.at[4], yr.at[4], at_y(1)))
    remote(yhold.at[1], yhold.at[1], ys.at[1], yr.at[1], at_y(-1)).wait_recv()
    for i in range(4):
        yhold[1, i] = (rb[down, 4 + i].astype(F32) + yhold[1, i].astype(F32)).astype(BF16)
    go(remote(yhold.at[1], yin.at[1, hi], ys.at[5], yr.at[5], at_y(-1)))

    z_second(ra, 4, a3, a4, a2, zs, zr)

    remote(psib, psib, dsem.at[0], drem.at[0], {"seq_2": sib}).wait_recv()
    for k in range(4):
        for h in range(2):
            psib[k, h] = (p[c, k, h].astype(F32) + psib[k, h].astype(F32)).astype(BF16)
    xu, xd, xf = lax.rem(x + 1, 4), lax.rem(x + 3, 4), lax.rem(x + 2, 4)
    go(remote(psib.at[xf, 0], xhold.at[0], xs.at[0], xr.at[0], at_x(1)))
    go(remote(psib.at[xf, 1], xhold.at[1], xs.at[1], xr.at[1], at_x(-1)))
    go(remote(psib.at[xu, 1], xin.at[0, 1], xs.at[2], xr.at[2], at_x(1)))
    go(remote(psib.at[xd, 0], xin.at[1, 0], xs.at[3], xr.at[3], at_x(-1)))
    edge = remote(
        pbsib, pbin.at[x], es, er.at[x],
        {"seq_0": pq // 2, "seq_1": lax.rem(pq, 2), "chan": 3},
    )

    @pl.when(c == 1)
    def _():
        pb_out.wait_recv()
        pbsib[...] = (pb[...].astype(F32) + pbsib[...].astype(F32)).astype(BF16)
        edge.start()

    for k in (2, 4):
        part = hi if k == 2 else lo
        remote(yin.at[0, part], yin.at[0, part], ys.at[k], yr.at[k], at_y(1)).wait_recv()
    for k in (3, 5):
        part = lo if k == 3 else hi
        remote(yin.at[1, part], yin.at[1, part], ys.at[k], yr.at[k], at_y(-1)).wait_recv()
    for i in range(NZ):
        v = rb[y, i].astype(F32) + yin[0, i].astype(F32) + yin[1, i].astype(F32)
        sb[i] = v.astype(BF16)
    z_first(sb, 2, b3, b4, b1, qs, qr)

    z_last(a1, a2, zs, zr)
    for i in range(4):
        v = ra[z, i].astype(F32)
        for k in range(2):
            v = v + a1[k, i].astype(F32) + a2[k, i].astype(F32)
        sa[i] = v.astype(BF16)
    for off in (2, 1, 3):
        to = lax.rem(y + off, 4)
        go(remote(sa.at[to], ya.at[off], as_.at[off], ar.at[off], at_y(off)))

    remote(xhold.at[0], xhold.at[0], xs.at[0], xr.at[0], at_x(1)).wait_recv()
    xhold[0] = (psib[xu, 0].astype(F32) + xhold[0].astype(F32)).astype(BF16)
    go(remote(xhold.at[0], xin.at[0, 0], xs.at[4], xr.at[4], at_x(1)))
    remote(xhold.at[1], xhold.at[1], xs.at[1], xr.at[1], at_x(-1)).wait_recv()
    xhold[1] = (psib[xd, 1].astype(F32) + xhold[1].astype(F32)).astype(BF16)
    go(remote(xhold.at[1], xin.at[1, 1], xs.at[5], xr.at[5], at_x(-1)))
    pown[...] = psib[x]

    z_second(sb, 2, b3, b4, b2, qs, qr)

    v = sa[y].astype(F32)
    for off in range(1, 4):
        remote(ya.at[off], ya.at[off], as_.at[off], ar.at[off], at_y(off)).wait_recv()
        v = v + ya[off].astype(F32)
    fa[0] = v[:40]
    fa[1] = v[40:]
    go(remote(fa.at[sib], fat.at[c], ts.at[0], tr.at[0], {"seq_2": sib}))
    line = iota((128, 80), 0)
    wanted = (line // 64) * 40 + (lax.rem(line // 16, 4)) * 10 + lax.rem(line, 16)
    chosen = exact(one_hot((iota((128, 80), 1) == wanted) & (lax.rem(line, 16) < 10)), v)
    for j in range(8):
        mrows[j] = chosen[j * 16 : (j + 1) * 16]
    for off in range(1, 8):
        to = lax.rem(j8 + off, 8)
        go(remote(mrows.at[to], mt.at[j8], ts.at[off], tr.at[off], at_j(to)))
    fat[c] = fa[c]
    mt[j8] = mrows[j8]

    z_last(b1, b2, qs, qr)
    for i in range(2):
        v = sb[z, i].astype(F32)
        for k in range(2):
            v = v + b1[k, i].astype(F32) + b2[k, i].astype(F32)
        fbs[0, :, i * 128 : (i + 1) * 128] = v[:40]
        fbs[1, :, i * 128 : (i + 1) * 128] = v[40:]
    go(remote(fbs.at[sib], fb.at[c], dsem.at[2], drem.at[2], {"seq_2": sib}))
    fb[c] = fbs[c]

    for k, half in ((2, 1), (4, 0)):
        remote(xin.at[0, half], xin.at[0, half], xs.at[k], xr.at[k], at_x(1)).wait_recv()
    for k, half in ((3, 0), (5, 1)):
        remote(xin.at[1, half], xin.at[1, half], xs.at[k], xr.at[k], at_x(-1)).wait_recv()
    for off in range(1, 8):
        origin = lax.rem(j8 + 8 - off, 8)
        remote(mrows.at[0], mt.at[origin], ts.at[off], tr.at[off], at_j(origin)).wait_recv()
    remote(fa.at[c], fat.at[sib], ts.at[0], tr.at[0], {"seq_2": sib}).wait_recv()

    @pl.when((c == 1) & (x == 3))
    def _():
        for k in range(4):
            remote(pbsib, pbin.at[k], es, er.at[k], {"chan": 0}).wait_recv()

    remote(fbs.at[c], fb.at[sib], dsem.at[2], drem.at[2], {"seq_2": sib}).wait_recv()
    for d in pending:
        d.wait_send()

    @pl.when(c == 0)
    def _():
        pb_out.wait_send()

    @pl.when(c == 1)
    def _():
        edge.wait_send()


def whole_kernel(
    norm,
    piece, og, wi_h, wm_h, ws_h, ci_h, cm_h, bias_h, dlog_h, skip_h,
    mt, fat, fb, pown, xin, pbin,
    xe, ogx, wi, wm, ws, ci, cm, bias, dlog, skip, wih, send, recv, back, st, gi, gm, ds, gmt,
    gs, gr, gt, hsem, lsem, s1, r1, s2, r2, *rest,
):
    dp = lax.axis_index("dp")
    z, yh, c, x = (lax.axis_index(a) for a in SEQ_CHAN)
    n = 2 * NZ
    q = z * 2 + yh
    nq, pq = lax.rem(q + 1, n), lax.rem(q + n - 1, n)
    corner = (c == 1) & (x == 3)
    barrier = pltpu.get_barrier_semaphore()

    def tell(**where):
        pl.semaphore_signal(barrier, inc=1, device_id=where, device_id_type=MESH)

    for off in range(1, 8):
        k = lax.rem(c * 4 + x + off, 8)
        tell(seq_2=k // 4, chan=lax.rem(k, 4))
    for off in (1, 3):
        k = lax.rem(yh * 2 + dp + off, 4)
        tell(seq_1=k // 2, dp=lax.rem(k, 2))
    for off in range(1, n):
        k = lax.rem(q + off, n)
        tell(seq_0=k // 2, seq_1=lax.rem(k, 2))

    @pl.when(c == 1)
    def _():
        tell(seq_0=pq // 2, seq_1=lax.rem(pq, 2), chan=3)

    @pl.when(corner)
    def _():
        for k in range(4):
            tell(seq_0=nq // 2, seq_1=lax.rem(nq, 2), chan=k)

    base = pl.multiple_of(PRE + (c * 4 + x) * 32, 16)
    loads = [pltpu.make_async_copy(piece, xe.at[pl.ds(base, 32), :], hsem.at[0])]
    loads.append(pltpu.make_async_copy(og, ogx.at[c], hsem.at[1]))
    pairs = ((wi_h, wi), (wm_h, wm), (ws_h, ws), (ci_h, ci), (cm_h, cm))
    pairs += ((bias_h, bias), (dlog_h, dlog), (skip_h, skip))
    for k, (src, dst) in enumerate(pairs):
        loads.append(pltpu.make_async_copy(src, dst, hsem.at[2 + k]))
    for d in loads:
        d.start()
    loads[0].wait()
    loads[1].wait()
    pl.semaphore_wait(
        barrier, jnp.where(corner, 7 + 2 + n - 1 + 5, jnp.where(c == 1, 7 + 2 + n, 7 + 2 + n - 1))
    )
    gather_phase(xe, ogx, gs, gr, gt)
    for d in loads[2:]:
        d.wait()
    acts = forward_phase(xe, ogx, wi, wm, ws, ci, cm, bias, dlog, wih, send)
    begin, turn, end = state_phases(send, st, recv, back, lsem, s1, r1, s2, r2)
    begin()
    local = local_phase(acts, dlog, skip)
    turn()
    end()

    def carry_on(send_mix):
        carried_phase(acts, local, st, ci, cm, gi, gm, ds, gmt, send_mix)

    sums_phase(
        norm, carry_on, xe, gi, gm, ds, gmt, wih, wm, ws, mt, fat, fb, pown, xin, pbin, *rest
    )


def whole(norm, *args):
    dma = pltpu.SemaphoreType.DMA
    n = 2 * NZ

    def vm(*shape):
        return pltpu.VMEM(shape, BF16)

    return pl.pallas_call(
        functools.partial(whole_kernel, norm),
        out_shape=(
            jax.ShapeDtypeStruct((8, 16, 128), F32),
            jax.ShapeDtypeStruct((2, 40, 128), F32),
            jax.ShapeDtypeStruct((2, 40, 256), F32),
            jax.ShapeDtypeStruct((2, 16, D), BF16),
            jax.ShapeDtypeStruct((2, 2, 16, D), BF16),
            jax.ShapeDtypeStruct((4, PRE, D), BF16),
        ),
        in_specs=[pl.BlockSpec(memory_space=pltpu.HBM)] * 10,
        out_specs=(VM,) * 6,
        scratch_shapes=[
            vm(EXT, D), vm(2, TOK // 2, 2 * INNER), vm(D, 2 * INNER), vm(D, 2 * STATE), vm(10, D),
            pltpu.VMEM((4, 2 * INNER), F32), pltpu.VMEM((4, 2 * STATE), F32),
            pltpu.VMEM((1, 10), F32), pltpu.VMEM((1, 10), F32), pltpu.VMEM((1, 10), F32),
            vm(D, INNER), vm(n, CHUNK, STATE), vm(n, CHUNK, STATE), vm(n, CHUNK, STATE),
            vm(n, CHUNK, STATE), vm(EXT, INNER), vm(EXT, 2 * STATE), vm(EXT, 128), vm(8, 32, EXT),
            dma((13,)), dma((13,)), dma((4,)), dma((10,)), dma((2,)),
            dma((n,)), dma((n,)), dma((n,)), dma((n,)),
            vm(8, 32, EXT),
            vm(4, NZ, 2, ROWS, 128), vm(2, 4, 2, ROWS, 128), vm(2, NZ, 2, ROWS, 128),
            vm(NZ, 4, ROWS, 128), vm(2, 4, ROWS, 128), vm(2, 2, ROWS, 128),
            vm(2, 4, ROWS, 128), vm(2, 4, ROWS, 128), vm(4, ROWS, 128), vm(4, ROWS, 128),
            vm(NZ, 2, ROWS, 128), vm(2, 2, ROWS, 128), vm(2, 1, ROWS, 128),
            vm(2, 2, ROWS, 128), vm(2, 2, ROWS, 128),
            pltpu.VMEM((2, 40, 128), F32), pltpu.VMEM((8, 16, 128), F32),
            pltpu.VMEM((2, 40, 256), F32),
            vm(2, 4, 2, 16, D), vm(4, 2, 16, D), vm(2, 16, D), vm(PRE, D), vm(PRE, D),
            dma((8,)), dma((8,)), dma((6,)), dma((6,)), dma((8,)), dma((8,)),
            dma((8,)), dma((8,)), dma((6,)), dma((6,)), dma(()), dma((4,)), dma((4,)), dma((4,)),
            dma((8,)), dma((8,)), dma((3,)), dma((3,)),
        ],
        compiler_params=pltpu.CompilerParams(
            collective_id=0, has_side_effects=True, vmem_limit_bytes=LIMIT
        ),
        name="whole",
    )(*args)


def finish_kernel(mt, fat, fb, pown, xin, pbin, ig_o, iw_o, mw_o, sw_o):
    c, x = lax.axis_index("seq_2"), lax.axis_index("chan")
    for k in range(2):
        iw_o[:, k * INNER : k * INNER + 256] = fb[k]
        own = fat[k]
        iw_o[:, k * INNER + 256 : (k + 1) * INNER] = own[:, :64]
        pick = one_hot(iota((HEADS, 128), 1) == iota((HEADS, 128), 0) + 96)
        sw_o[k * HEADS : (k + 1) * HEADS, :] = lax.dot_general(
            pick, own, (((1,), (1,)), ((), ())), preferred_element_type=F32,
            precision=lax.Precision.HIGHEST,
        )
    for j in range(8):
        mw_o[:, j * 32 : (j + 1) * 32] = mt[j, :10, 64:96]
    for h in range(2):
        acc = pown[h].astype(F32) + xin[0, h].astype(F32) + xin[1, h].astype(F32)
        ig_o[h * 16 : (h + 1) * 16, :] = acc.astype(BF16)

    @pl.when((c == 1) & (x == 3))
    def _():
        edge = pown[1].astype(F32) + xin[0, 1].astype(F32) + xin[1, 1].astype(F32)
        for j in range(4):
            edge = edge + pbin[j].astype(F32)
        ig_o[16:, :] = edge.astype(BF16)


def finish(*args):
    return pl.pallas_call(
        finish_kernel,
        out_shape=(
            jax.ShapeDtypeStruct((32, D), BF16),
            jax.ShapeDtypeStruct((40, 2 * INNER), F32),
            jax.ShapeDtypeStruct((10, 2 * STATE), F32),
            jax.ShapeDtypeStruct((2 * HEADS, 40), F32),
        ),
        in_specs=[VM] * 6,
        out_specs=(VM,) * 4,
        compiler_params=pltpu.CompilerParams(vmem_limit_bytes=LIMIT),
        name="finish",
    )(*args)


def body(
    layer_input,
    inner_weight,
    mixer_weight,
    step_weight,
    conv_inner,
    conv_mixer,
    step_bias,
    decay_log,
    skip_gain,
    output_grad,
):
    norm = 1.0 / math.sqrt(8192)
    stepw = step_weight.T
    bias, dlog, skip = (v.reshape(1, -1) for v in (step_bias, decay_log, skip_gain))
    parts = whole(
        norm, layer_input[0], output_grad[0], inner_weight, mixer_weight, stepw, conv_inner,
        conv_mixer, bias, dlog, skip,
    )
    ig, iw, mw, sw = finish(*parts)
    return ig[None], iw, mw, sw.T


def solution(mesh):
    split = Mesh(
        mesh.devices.reshape(mesh.shape["dp"], 8, 2, 2, mesh.shape["chan"]),
        ("dp", "seq_0", "seq_1", "seq_2", "chan"),
    )
    placed = (
        P("dp", SEQ_CHAN, None),
        P(None, "chan"),
        P(),
        P(None, "chan"),
        P(None, "chan"),
        P(),
        P("chan"),
        P("chan"),
        P("chan"),
        P("dp", SEQ, "chan"),
    )
    return jax.shard_map(
        body,
        mesh=split,
        in_specs=placed,
        out_specs=(
            P("dp", SEQ_CHAN, None),
            P(DP_SEQ, "chan"),
            P(DP_SEQ_CHAN, None),
            P(DP_SEQ, "chan"),
        ),
        check_vma=False,
    )
```

```python
import functools
import math

import jax
import jax.numpy as jnp
from jax import lax
from jax.experimental import pallas as pl
from jax.experimental.pallas import tpu as pltpu
from jax.sharding import Mesh
from jax.sharding import PartitionSpec as P

D = 2560
HDIM = 64
HEADS = 5
INNER = HEADS * HDIM
STATE = 128
TOK = 256
PRE = 16
EXT = TOK + PRE
NZ = 8
ROWS = 80
CHUNK = 48
F32 = jnp.float32
BF16 = jnp.bfloat16
SEQ = ("seq_0", "seq_1", "seq_2")
DP_SEQ = ("dp", "seq_0", "seq_1", "seq_2")
SEQ_CHAN = ("seq_0", "seq_1", "seq_2", "chan")
DP_SEQ_CHAN = ("dp", "seq_0", "seq_1", "seq_2", "chan")
MESH = pl.DeviceIdType.MESH
VM = pl.BlockSpec(memory_space=pltpu.VMEM)
LIMIT = 62 * 1024 * 1024


def roll(v, shift):
    return pltpu.roll(v, shift % v.shape[0], 0)


def mm(a, b):
    return jnp.dot(a, b, preferred_element_type=F32)


def mm_t(a, b):
    return lax.dot_general(a, b, (((1,), (1,)), ((), ())), preferred_element_type=F32)


def t_mm(a, b):
    return lax.dot_general(a, b, (((0,), (0,)), ((), ())), preferred_element_type=F32)


def exact(a, b):
    return jnp.dot(a, b, preferred_element_type=F32, precision=lax.Precision.HIGHEST)


def iota(shape, dim):
    return lax.broadcasted_iota(jnp.int32, shape, dim)


def one_hot(cond):
    return jnp.where(cond, 1.0, 0.0).astype(F32)


def head_expand():
    return one_hot(iota((128, INNER), 1) // HDIM == iota((128, INNER), 0))


def head_sum():
    return one_hot(iota((INNER, 128), 0) // HDIM == iota((INNER, 128), 1))


def head_pick(core):
    return one_hot(
        (iota((10, 128), 0) == iota((10, 128), 1) + HEADS * core) & (iota((10, 128), 1) < HEADS)
    )


def half_of(v, core):
    return jnp.where(core == 0, v[:, :INNER], v[:, INNER:])


def conv(v, k):
    return k[3:4] * v + k[2:3] * roll(v, 1) + k[1:2] * roll(v, 2) + k[0:1] * roll(v, 3)


def conv_back(g, k):
    return k[3:4] * g + k[2:3] * roll(g, -1) + k[1:2] * roll(g, -2) + k[0:1] * roll(g, -3)


def gather_phase(xe, ogx, ssem, rsem, tsem):
    z, yh, c, x = (lax.axis_index(a) for a in SEQ_CHAN)
    right, left = lax.rem(x + 1, 4), lax.rem(x + 3, 4)
    sib = 1 - c
    q = z * 2 + yh
    nq, pq = lax.rem(q + 1, 2 * NZ), lax.rem(q + 2 * NZ - 1, 2 * NZ)
    def slot(core, chan, half=None):
        base = PRE + (core * 4 + chan) * 32
        if half is None:
            return xe.at[pl.ds(pl.multiple_of(base, 16), 32), :]
        return xe.at[pl.ds(pl.multiple_of(base + 16 * half, 16), 16), :]

    def copy(src, dst, k, **where):
        return pltpu.make_async_remote_copy(
            src_ref=src, dst_ref=dst, send_sem=ssem.at[k], recv_sem=rsem.at[k],
            device_id=where, device_id_type=MESH,
        )

    mine = slot(c, x)
    own_og = ogx.at[c]

    def half(h):
        return slot(c, x, h)

    r0 = copy(half(0), slot(c, x, 0), 0, chan=right)
    l1 = copy(half(1), slot(c, x, 1), 1, chan=left)
    r1 = copy(half(1), slot(c, x, 1), 2, chan=right)
    l0 = copy(half(0), slot(c, x, 0), 3, chan=left)
    sp = copy(mine, mine, 4, seq_2=sib)
    so = copy(own_og, own_og, 5, seq_2=sib)
    for d in (r0, l1):
        d.start()

    def tails(chan):
        return pltpu.make_async_remote_copy(
            src_ref=half(1), dst_ref=xe.at[pl.ds(0, 16), :], send_sem=tsem.at[chan],
            recv_sem=rsem.at[6],
            device_id={"seq_0": nq // 2, "seq_1": lax.rem(nq, 2), "chan": chan},
            device_id_type=MESH,
        )

    @pl.when((c == 1) & (x == 3))
    def _():
        for chan in range(4):
            tails(chan).start()

    for d in (r1, l0, sp, so):
        d.start()
    far = lax.rem(x + 2, 4)
    in_r0 = copy(half(0), slot(c, left, 0), 0, chan=right)
    in_r1 = copy(half(1), slot(c, left, 1), 2, chan=right)
    in_l1 = copy(half(1), slot(c, right, 1), 1, chan=left)
    in_l0 = copy(half(0), slot(c, right, 0), 3, chan=left)
    rr = copy(slot(c, left, 0), slot(c, left, 0), 7, chan=right)
    ll = copy(slot(c, right, 1), slot(c, right, 1), 8, chan=left)
    in_r0.wait_recv()
    rr.start()
    in_l1.wait_recv()
    ll.start()
    in_r1.wait_recv()
    s_left = copy(slot(c, left), slot(c, left), 9, seq_2=sib)
    s_left.start()
    in_l0.wait_recv()
    s_right = copy(slot(c, right), slot(c, right), 10, seq_2=sib)
    s_right.start()
    tail_on = copy(xe.at[pl.ds(0, 16), :], xe.at[pl.ds(0, 16), :], 12, seq_2=sib)

    @pl.when(c == 1)
    def _():
        tails(0).wait_recv()
        tail_on.start()

    in_rr = copy(half(0), slot(c, far, 0), 7, chan=right)
    in_ll = copy(half(1), slot(c, far, 1), 8, chan=left)
    in_rr.wait_recv()
    in_ll.wait_recv()
    s_far = copy(slot(c, far), slot(c, far), 11, seq_2=sib)
    s_far.start()
    copy(mine, slot(sib, x), 4, seq_2=sib).wait_recv()
    copy(own_og, ogx.at[sib], 5, seq_2=sib).wait_recv()
    copy(mine, slot(sib, left), 9, seq_2=sib).wait_recv()
    copy(mine, slot(sib, right), 10, seq_2=sib).wait_recv()
    copy(mine, slot(sib, far), 11, seq_2=sib).wait_recv()

    @pl.when(c == 0)
    def _():
        tail_on.wait_recv()

    for d in (r0, l1, r1, l0, sp, so, rr, ll, s_left, s_right, s_far):
        d.wait_send()

    @pl.when(c == 1)
    def _():
        tail_on.wait_send()

    @pl.when((c == 1) & (x == 3))
    def _():
        for chan in range(4):
            tails(chan).wait_send()


def forward_phase(xe, ogx, wi, wm, ws, ci, cm, bias, dlog, wih_o, send_o):
    z, yh, c = (lax.axis_index(a) for a in SEQ)
    flag = jnp.where(z * 2 + yh == 0, 0.0, 1.0).astype(F32)
    pick = head_pick(c)
    wih = half_of(wi[...], c)
    wih_o[...] = wih
    xv = xe[...]
    keep = jnp.where(iota((EXT, 1), 0) < PRE, flag, 1.0)

    def masked(v):
        return jnp.where(keep > 0.0, v.astype(BF16).astype(F32), 0.0)

    pi = masked(mm(xv, wih))
    pm = masked(mm(xv, wm[...]))
    sr = exact(mm_t(xv, ws[...])[PRE:], pick)
    zi = conv(pi, half_of(ci[...], c))[PRE:]
    zm = conv(pm, cm[...])[PRE:]
    xa = zi * jax.nn.sigmoid(zi)
    ma = zm * jax.nn.sigmoid(zm)
    srb = sr + exact(bias[...], pick)
    dt = jnp.maximum(srb, 0.0) + jnp.log1p(jnp.exp(-jnp.abs(srb)))
    rate = exact(jnp.exp(dlog[...]), pick)
    a = -dt * rate
    tri = one_hot(iota((TOK, TOK), 0) >= iota((TOK, TOK), 1))
    cum = exact(tri, a)
    tot = cum[TOK - 1 : TOK]
    og = half_of(ogx[...].reshape(TOK, 2 * INNER), c)
    ex = head_expand()
    xt = (xa * exact(dt * jnp.exp(tot - cum), ex)).astype(BF16)
    yt = (og.astype(F32) * exact(jnp.exp(cum), ex)).astype(BF16)
    f_loc = t_mm(xt, ma[:, :STATE].astype(BF16))
    g_loc = t_mm(yt, ma[:, STATE:].astype(BF16))
    diag = jnp.where(iota((8, 128), 0) == iota((8, 128), 1), tot, 0.0)
    dm = exact(diag, jnp.ones((128, 128), F32))
    hi = dm.astype(BF16).astype(F32)
    drow = jnp.where(iota((8, 128), 1) < 64, hi, dm - hi)
    for zz in range(NZ):
        for which, v in ((0, f_loc), (1, g_loc)):
            rows = [v[h * HDIM + zz * 8 : h * HDIM + zz * 8 + 8] for h in range(HEADS)]
            send_o[zz * 2 + which] = jnp.concatenate(rows + [drow], axis=0).astype(BF16)
    return xa, zi, zm, dt, cum, srb, og


def state_phases(send, out, recv, back, local_sem, s1, r1, s2, r2):
    z, yh = lax.axis_index("seq_0"), lax.axis_index("seq_1")
    n = 2 * NZ
    me = z * 2 + yh
    def at(q):
        return {"seq_0": q // 2, "seq_1": lax.rem(q, 2)}

    def push(src, dst, ss, rs, off):
        to = lax.rem(me + off, n)
        return pltpu.make_async_remote_copy(
            src_ref=src.at[to], dst_ref=dst.at[me], send_sem=ss.at[off], recv_sem=rs.at[off],
            device_id=at(to), device_id_type=MESH,
        )

    def pull(src, dst, ss, rs, off):
        origin = lax.rem(me + n - off, n)
        return pltpu.make_async_remote_copy(
            src_ref=src.at[origin], dst_ref=dst.at[origin], send_sem=ss.at[off],
            recv_sem=rs.at[off], device_id=at(origin), device_id_type=MESH,
        )

    order = sorted(range(1, n), key=lambda off: -min(off, n - off))
    first = [push(send, recv, s1, r1, off) for off in order]
    second = [push(back, out, s2, r2, off) for off in order]

    def begin():
        for d in first:
            d.start()
        own = pltpu.make_async_copy(send.at[me], recv.at[me], local_sem.at[0])
        own.start()
        own.wait()

    def turn():
        for off in range(1, n):
            pull(send, recv, s1, r1, off).wait_recv()
        run = jnp.zeros((HEADS * 8, STATE), F32)
        for j in range(n):
            k = jnp.where(yh == 0, j, n - 1 - j)
            got = recv[k].astype(F32)
            rows = got[HEADS * 8 :]
            rows = rows + pltpu.roll(rows, 64, 1)
            decay = jnp.exp(rows)
            back[k] = jnp.concatenate([run, rows], axis=0).astype(BF16)
            wide = jnp.concatenate(
                [jnp.broadcast_to(decay[h : h + 1], (8, STATE)) for h in range(HEADS)], axis=0
            )
            run = wide * run + got[: HEADS * 8]
        for d in second:
            d.start()
        own = pltpu.make_async_copy(back.at[me], out.at[me], local_sem.at[1])
        own.start()
        own.wait()

    def end():
        for off in range(1, n):
            pull(back, out, s2, r2, off).wait_recv()
        for d in first + second:
            d.wait_send()

    return begin, turn, end


def local_phase(acts, dlog, skip):
    c = lax.axis_index("seq_2")
    pick = head_pick(c)
    ex = head_expand()
    xa, zi, zm, dt, cum, srb, og = acts
    dy = og.astype(F32)
    rate = exact(jnp.exp(dlog[...]), pick)
    skp = exact(skip[...], pick)
    tot = cum[TOK - 1 : TOK]
    ecum = exact(jnp.exp(cum), ex)
    etail = exact(jnp.exp(tot - cum), ex)
    dte = exact(dt, ex)
    sz = jax.nn.sigmoid(zm)
    ma = zm * sz
    bm, cmx = ma[:, :STATE].astype(BF16), ma[:, STATE:].astype(BF16)
    xdt = xa * dte
    xdtb = xdt.astype(BF16)
    xdtf = xdtb.astype(F32)
    scores = mm_t(cmx, bm)
    causal = iota((TOK, TOK), 0) >= iota((TOK, TOK), 1)
    cumt = cum.T
    dscore = jnp.zeros((TOK, TOK), F32)
    ys, us = [], []
    for h in range(HEADS):
        cols = slice(h * HDIM, (h + 1) * HDIM)
        decay = jnp.exp(jnp.where(causal, cum[:, h : h + 1] - cumt[h : h + 1, :], -1e30))
        m = (decay * scores).astype(BF16)
        ys.append(mm(m, xdtb[:, cols]))
        us.append(t_mm(m, og[:, cols]))
        dscore = dscore + decay * mm_t(og[:, cols], xdtb[:, cols])
    dsb = dscore.astype(BF16)
    d_out, d_in = mm(dsb, bm), t_mm(dsb, cmx)
    yt, xt = (dy * ecum).astype(BF16), (xdt * etail).astype(BF16)
    gate_m = sz * (1.0 + zm * (1.0 - sz))
    si = jax.nn.sigmoid(zi)
    gate_i = si * (1.0 + zi * (1.0 - si))
    return (
        jnp.concatenate(ys, axis=1), jnp.concatenate(us, axis=1), d_out, d_in, yt, xt, gate_m,
        gate_i, bm, cmx, xdtf, dy, rate, exact(skp, ex), tot, ecum, etail, dte,
    )


def carried_phase(acts, local, st, ci, cm, gi_o, gm_o, ds_o, gmt_o):
    z, yh, c = (lax.axis_index(a) for a in SEQ)
    flag = jnp.where(z * 2 + yh == 0, 0.0, 1.0).astype(F32)
    hs = head_sum()
    xa, _, _, _, _, srb, _ = acts
    (
        y_loc, u_loc, d_out, d_in, yt, xt, gate_m, gate_i, bm, cmx, xdtf, dy, rate, skp, tot,
        ecum, etail, dte,
    ) = local
    keep = jnp.where(iota((EXT, 1), 0) < PRE, flag, 1.0)

    def collect(which):
        blocks = [st[2 * zz + which].astype(F32) for zz in range(NZ)]
        rows = [blocks[zz][h * 8 : h * 8 + 8] for h in range(HEADS) for zz in range(NZ)]
        return jnp.concatenate(rows, axis=0)

    def back(g, k):
        g = jnp.concatenate([jnp.zeros((PRE, g.shape[1]), F32), g], axis=0)
        return jnp.where(keep > 0.0, conv_back(g, k), 0.0).astype(BF16)

    h0, ge = collect(0), collect(1)
    h0b, geb = h0.astype(BF16), ge.astype(BF16)
    ug = etail * mm_t(bm, geb)
    u = u_loc + ug
    gi_o[...] = back((dte * u + skp * dy) * gate_i, half_of(ci[...], c))

    def mixing():
        gm = jnp.concatenate([d_in + mm(xt, geb), d_out + mm(yt, h0b)], axis=1) * gate_m
        gme = back(gm, cm[...])
        gm_o[...] = gme
        eye = one_hot(iota((EXT, EXT), 0) == iota((EXT, EXT), 1)).astype(BF16)
        gmt = t_mm(gme, eye).astype(BF16)
        for j in range(8):
            gmt_o[j] = gmt[j * 32 : j * 32 + 32]

    def stepping():
        y = y_loc + ecum * mm_t(cmx, h0b)
        ddt = exact(xa * u, hs)
        dcum = exact(dy * y - xdtf * u, hs)
        e_sum = jnp.sum(exact(xdtf * ug, hs), axis=0, keepdims=True)
        hg = exact(jnp.ones((8, STATE), F32), (h0 * ge).T)
        carry = jnp.exp(tot) * exact(hg, hs)[0:1]
        upper = one_hot(iota((TOK, TOK), 0) <= iota((TOK, TOK), 1))
        da = exact(upper, dcum) + e_sum + carry
        dsr = (ddt - rate * da) * jax.nn.sigmoid(srb)
        ds_o[...] = jnp.concatenate([jnp.zeros((PRE, 128), F32), dsr], axis=0).astype(BF16)

    return mixing, stepping


def sums_phase(
    norm, later, xe, gi_r, gm_r, ds_r, gmt, wih, wm, ws,
    mt, fat, fb, ig, xin, pbin,
    mixin, rb, yhold, yin, ra, a3, a4, a1, a2, sa, ya, sb, b3, b4, b1, b2, fa, mrows, fbs, p, psib, xhold,
    pb, pbsib,
    ms, mr, ys, yr, zs, zr, qs, qr, xs, xr, es, er, as_, ar, ts, tr, dsem, drem,
):
    dp = lax.axis_index("dp")
    z, yh, c, x = (lax.axis_index(a) for a in SEQ_CHAN)
    y = yh * 2 + dp
    j8 = c * 4 + x
    sib = 1 - c
    q = z * 2 + yh
    nq, pq = lax.rem(q + 1, 2 * NZ), lax.rem(q + 2 * NZ - 1, 2 * NZ)
    def at_z(off):
        return {"seq_0": lax.rem(z + off + NZ, NZ)}

    def at_y(off):
        k = lax.rem(y + off + 4, 4)
        return {"seq_1": k // 2, "dp": lax.rem(k, 2)}

    def at_x(off):
        return {"chan": lax.rem(x + off + 4, 4)}

    def at_j(k):
        return {"seq_2": k // 4, "chan": lax.rem(k, 4)}

    def remote(src, dst, ss, rs, where):
        return pltpu.make_async_remote_copy(
            src_ref=src, dst_ref=dst, send_sem=ss, recv_sem=rs, device_id=where,
            device_id_type=MESH,
        )

    pending = []

    def go(d):
        d.start()
        pending.append(d)
        return d

    def send_mix():
        for off in range(1, 8):
            to = lax.rem(j8 + off, 8)
            go(remote(gmt.at[to], mixin.at[off], ms.at[off], mr.at[off], at_j(to)))

    mixing, stepping = later

    gi = gi_r[...]
    rhs = gi[:, :256]

    def inner_rows(side, zhi):
        base = pl.multiple_of(side * 1280 + zhi * 640, 128)
        r = (t_mm(xe[:, pl.ds(base, 640)], rhs) * norm).astype(BF16)
        for g in range(8):
            for k in range(2):
                rb[(g % 2) * 2 + side, zhi * 4 + g // 2, k] = r[
                    g * ROWS : (g + 1) * ROWS, k * 128 : (k + 1) * 128
                ]

    up, down, far = lax.rem(y + 1, 4), lax.rem(y + 3, 4), lax.rem(y + 2, 4)
    lo, hi = pl.ds(0, 4), pl.ds(4, 4)
    inner_rows(dp, 0)
    go(remote(rb.at[far, lo], yhold.at[0], ys.at[0], yr.at[0], at_y(1)))
    inner_rows(dp, 1)
    go(remote(rb.at[far, hi], yhold.at[1], ys.at[1], yr.at[1], at_y(-1)))
    inner_rows(1 - dp, 1)
    go(remote(rb.at[up, hi], yin.at[0, hi], ys.at[2], yr.at[2], at_y(1)))
    inner_rows(1 - dp, 0)
    go(remote(rb.at[down, lo], yin.at[1, lo], ys.at[3], yr.at[3], at_y(-1)))
    mixing()
    send_mix()
    stepping()

    ds = ds_r[...]
    pick = head_pick(c).astype(BF16)
    ds10 = mm_t(ds, pick).astype(BF16)
    gm = gm_r[...]
    for b in range(4):
        rows = slice(b * 640, (b + 1) * 640)
        part = mm_t(gi, wih[rows]) + mm_t(gm, wm[rows]) + mm(ds10, ws[:, rows])
        part = part.astype(BF16)
        pb[:, rows] = part[:PRE]
        for j in range(8):
            for k in range(2):
                at = PRE + j * 32 + k * 16
                p[j // 4, j % 4, k, :, rows] = part[at : at + 16]
    go(remote(p.at[sib], psib, dsem.at[0], drem.at[0], {"seq_2": sib}))
    pb_out = remote(pb, pbsib, dsem.at[1], drem.at[1], {"seq_2": sib})

    @pl.when(c == 0)
    def _():
        pb_out.start()

    total = gmt[j8].astype(F32)
    for off in range(1, 8):
        origin = lax.rem(j8 + 8 - off, 8)
        remote(gmt.at[origin], mixin.at[off], ms.at[off], mr.at[off], at_j(origin)).wait_recv()
        total = total + mixin[off].astype(F32)
    place_mix = one_hot(iota((32, 128), 1) == iota((32, 128), 0) + 64).astype(BF16)
    place_step = one_hot(
        (iota((128, 128), 1) == iota((128, 128), 0) + 96) & (iota((128, 128), 0) < HEADS)
    ).astype(BF16)
    last = t_mm(total.astype(BF16), place_mix) + mm(ds, place_step)
    last = last + jnp.concatenate([gi[:, 256:].astype(F32), jnp.zeros((EXT, 64), F32)], axis=1)
    last = last.astype(BF16)
    for b in range(4):
        r = (t_mm(xe[:, b * 640 : (b + 1) * 640], last) * norm).astype(BF16)
        for g in range(8):
            ra[(b % 2) * 4 + g // 2, (g % 2) * 2 + b // 2] = r[g * ROWS : (g + 1) * ROWS]

    def z_first(src, n, r3, r4, r1, s, r):
        h = n // 2
        for k, sign in enumerate((1, -1)):
            part = pl.ds(k * h, h)
            dst = [lax.rem(z + sign * d + NZ, NZ) for d in range(5)]
            go(remote(src.at[dst[4], part], r4.at[k], s.at[4 * k], r.at[4 * k], at_z(2 * sign)))
            go(remote(src.at[dst[3]], r3.at[k], s.at[4 * k + 1], r.at[4 * k + 1], at_z(sign)))
            go(remote(src.at[dst[1]], r1.at[k], s.at[4 * k + 2], r.at[4 * k + 2], at_z(sign)))

    def z_second(src, n, r3, r4, r2, s, r):
        h = n // 2
        for k, sign in enumerate((1, -1)):
            part = pl.ds(k * h, h)
            t = lax.rem(z + 2 * sign + NZ, NZ)
            remote(r3.at[k], r3.at[k], s.at[4 * k + 1], r.at[4 * k + 1], at_z(sign)).wait_recv()
            remote(r4.at[k], r4.at[k], s.at[4 * k], r.at[4 * k], at_z(2 * sign)).wait_recv()
            for i in range(n):
                v = src[t, i].astype(F32) + r3[k, i].astype(F32)
                if k * h <= i < (k + 1) * h:
                    v = v + r4[k, i - k * h].astype(F32)
                r3[k, i] = v.astype(BF16)
            go(remote(r3.at[k], r2.at[k], s.at[4 * k + 3], r.at[4 * k + 3], at_z(2 * sign)))

    def z_last(r1, r2, s, r):
        for k, sign in enumerate((1, -1)):
            remote(r1.at[k], r1.at[k], s.at[4 * k + 2], r.at[4 * k + 2], at_z(sign)).wait_recv()
            remote(r2.at[k], r2.at[k], s.at[4 * k + 3], r.at[4 * k + 3], at_z(2 * sign)).wait_recv()

    z_first(ra, 4, a3, a4, a1, zs, zr)

    remote(yhold.at[0], yhold.at[0], ys.at[0], yr.at[0], at_y(1)).wait_recv()
    for i in range(4):
        yhold[0, i] = (rb[up, i].astype(F32) + yhold[0, i].astype(F32)).astype(BF16)
    go(remote(yhold.at[0], yin.at[0, lo], ys.at[4], yr.at[4], at_y(1)))
    remote(yhold.at[1], yhold.at[1], ys.at[1], yr.at[1], at_y(-1)).wait_recv()
    for i in range(4):
        yhold[1, i] = (rb[down, 4 + i].astype(F32) + yhold[1, i].astype(F32)).astype(BF16)
    go(remote(yhold.at[1], yin.at[1, hi], ys.at[5], yr.at[5], at_y(-1)))

    z_second(ra, 4, a3, a4, a2, zs, zr)

    remote(psib, psib, dsem.at[0], drem.at[0], {"seq_2": sib}).wait_recv()
    for k in range(4):
        for h in range(2):
            psib[k, h] = (p[c, k, h].astype(F32) + psib[k, h].astype(F32)).astype(BF16)
    xu, xd, xf = lax.rem(x + 1, 4), lax.rem(x + 3, 4), lax.rem(x + 2, 4)
    go(remote(psib.at[xf, 0], xhold.at[0], xs.at[0], xr.at[0], at_x(1)))
    go(remote(psib.at[xf, 1], xhold.at[1], xs.at[1], xr.at[1], at_x(-1)))
    go(remote(psib.at[xu, 1], xin.at[0, 1], xs.at[2], xr.at[2], at_x(1)))
    go(remote(psib.at[xd, 0], xin.at[1, 0], xs.at[3], xr.at[3], at_x(-1)))
    edge = remote(
        pbsib, pbin.at[x], es, er.at[x],
        {"seq_0": pq // 2, "seq_1": lax.rem(pq, 2), "chan": 3},
    )

    @pl.when(c == 1)
    def _():
        pb_out.wait_recv()
        pbsib[...] = (pb[...].astype(F32) + pbsib[...].astype(F32)).astype(BF16)
        edge.start()

    for k in (2, 4):
        part = hi if k == 2 else lo
        remote(yin.at[0, part], yin.at[0, part], ys.at[k], yr.at[k], at_y(1)).wait_recv()
    for k in (3, 5):
        part = lo if k == 3 else hi
        remote(yin.at[1, part], yin.at[1, part], ys.at[k], yr.at[k], at_y(-1)).wait_recv()
    for i in range(NZ):
        v = rb[y, i].astype(F32) + yin[0, i].astype(F32) + yin[1, i].astype(F32)
        sb[i] = v.astype(BF16)
    z_first(sb, 2, b3, b4, b1, qs, qr)

    z_last(a1, a2, zs, zr)
    for i in range(4):
        v = ra[z, i].astype(F32)
        for k in range(2):
            v = v + a1[k, i].astype(F32) + a2[k, i].astype(F32)
        sa[i] = v.astype(BF16)
    for off in (2, 1, 3):
        to = lax.rem(y + off, 4)
        go(remote(sa.at[to], ya.at[off], as_.at[off], ar.at[off], at_y(off)))

    remote(xhold.at[0], xhold.at[0], xs.at[0], xr.at[0], at_x(1)).wait_recv()
    xhold[0] = (psib[xu, 0].astype(F32) + xhold[0].astype(F32)).astype(BF16)
    go(remote(xhold.at[0], xin.at[0, 0], xs.at[4], xr.at[4], at_x(1)))
    remote(xhold.at[1], xhold.at[1], xs.at[1], xr.at[1], at_x(-1)).wait_recv()
    xhold[1] = (psib[xd, 1].astype(F32) + xhold[1].astype(F32)).astype(BF16)
    go(remote(xhold.at[1], xin.at[1, 1], xs.at[5], xr.at[5], at_x(-1)))

    z_second(sb, 2, b3, b4, b2, qs, qr)

    v = sa[y].astype(F32)
    for off in range(1, 4):
        remote(ya.at[off], ya.at[off], as_.at[off], ar.at[off], at_y(off)).wait_recv()
        v = v + ya[off].astype(F32)
    fa[0] = v[:40]
    fa[1] = v[40:]
    go(remote(fa.at[sib], fat.at[c], ts.at[0], tr.at[0], {"seq_2": sib}))
    line = iota((128, 80), 0)
    wanted = (line // 64) * 40 + (lax.rem(line // 16, 4)) * 10 + lax.rem(line, 16)
    chosen = exact(one_hot((iota((128, 80), 1) == wanted) & (lax.rem(line, 16) < 10)), v)
    for j in range(8):
        mrows[j] = chosen[j * 16 : (j + 1) * 16]
    for off in range(1, 8):
        to = lax.rem(j8 + off, 8)
        go(remote(mrows.at[to], mt.at[j8], ts.at[off], tr.at[off], at_j(to)))
    fat[c] = fa[c]
    mt[j8] = mrows[j8]

    for k, half in ((2, 1), (4, 0)):
        remote(xin.at[0, half], xin.at[0, half], xs.at[k], xr.at[k], at_x(1)).wait_recv()
    for k, half in ((3, 0), (5, 1)):
        remote(xin.at[1, half], xin.at[1, half], xs.at[k], xr.at[k], at_x(-1)).wait_recv()
    for h in range(2):
        v = psib[x, h].astype(F32) + xin[0, h].astype(F32) + xin[1, h].astype(F32)
        ig[h * 16 : (h + 1) * 16, :] = v.astype(BF16)

    @pl.when((c == 1) & (x == 3))
    def _():
        v = psib[x, 1].astype(F32) + xin[0, 1].astype(F32) + xin[1, 1].astype(F32)
        for k in range(4):
            remote(pbsib, pbin.at[k], es, er.at[k], {"chan": 0}).wait_recv()
            v = v + pbin[k].astype(F32)
        ig[16:, :] = v.astype(BF16)

    z_last(b1, b2, qs, qr)
    for i in range(2):
        v = sb[z, i].astype(F32)
        for k in range(2):
            v = v + b1[k, i].astype(F32) + b2[k, i].astype(F32)
        fbs[0, :, i * 128 : (i + 1) * 128] = v[:40]
        fbs[1, :, i * 128 : (i + 1) * 128] = v[40:]
    go(remote(fbs.at[sib], fb.at[c], dsem.at[2], drem.at[2], {"seq_2": sib}))
    fb[c] = fbs[c]

    for off in range(1, 8):
        origin = lax.rem(j8 + 8 - off, 8)
        remote(mrows.at[0], mt.at[origin], ts.at[off], tr.at[off], at_j(origin)).wait_recv()
    remote(fa.at[c], fat.at[sib], ts.at[0], tr.at[0], {"seq_2": sib}).wait_recv()

    remote(fbs.at[c], fb.at[sib], dsem.at[2], drem.at[2], {"seq_2": sib}).wait_recv()
    for d in pending:
        d.wait_send()

    @pl.when(c == 0)
    def _():
        pb_out.wait_send()

    @pl.when(c == 1)
    def _():
        edge.wait_send()


def whole_kernel(
    norm,
    piece, og, wi_h, wm_h, ws_h, ci_h, cm_h, bias_h, dlog_h, skip_h,
    mt, fat, fb, ig,
    xe, ogx, wi, wm, ws, ci, cm, bias, dlog, skip, wih, send, recv, back, st, gi, gm, ds, gmt,
    gs, gr, gt, hsem, lsem, s1, r1, s2, r2, *rest,
):
    dp = lax.axis_index("dp")
    z, yh, c, x = (lax.axis_index(a) for a in SEQ_CHAN)
    n = 2 * NZ
    q = z * 2 + yh
    nq, pq = lax.rem(q + 1, n), lax.rem(q + n - 1, n)
    corner = (c == 1) & (x == 3)
    barrier = pltpu.get_barrier_semaphore()

    def tell(**where):
        pl.semaphore_signal(barrier, inc=1, device_id=where, device_id_type=MESH)

    for off in range(1, 8):
        k = lax.rem(c * 4 + x + off, 8)
        tell(seq_2=k // 4, chan=lax.rem(k, 4))
    for off in (1, 3):
        k = lax.rem(yh * 2 + dp + off, 4)
        tell(seq_1=k // 2, dp=lax.rem(k, 2))
    for off in range(1, n):
        k = lax.rem(q + off, n)
        tell(seq_0=k // 2, seq_1=lax.rem(k, 2))

    @pl.when(c == 1)
    def _():
        tell(seq_0=pq // 2, seq_1=lax.rem(pq, 2), chan=3)

    @pl.when(corner)
    def _():
        for k in range(4):
            tell(seq_0=nq // 2, seq_1=lax.rem(nq, 2), chan=k)

    base = pl.multiple_of(PRE + (c * 4 + x) * 32, 16)
    loads = [pltpu.make_async_copy(piece, xe.at[pl.ds(base, 32), :], hsem.at[0])]
    loads.append(pltpu.make_async_copy(og, ogx.at[c], hsem.at[1]))
    pairs = ((wi_h, wi), (wm_h, wm), (ws_h, ws), (ci_h, ci), (cm_h, cm))
    pairs += ((bias_h, bias), (dlog_h, dlog), (skip_h, skip))
    for k, (src, dst) in enumerate(pairs):
        loads.append(pltpu.make_async_copy(src, dst, hsem.at[2 + k]))
    for d in loads:
        d.start()
    loads[0].wait()
    loads[1].wait()
    pl.semaphore_wait(
        barrier, jnp.where(corner, 7 + 2 + n - 1 + 5, jnp.where(c == 1, 7 + 2 + n, 7 + 2 + n - 1))
    )
    gather_phase(xe, ogx, gs, gr, gt)
    for d in loads[2:]:
        d.wait()
    acts = forward_phase(xe, ogx, wi, wm, ws, ci, cm, bias, dlog, wih, send)
    begin, turn, end = state_phases(send, st, recv, back, lsem, s1, r1, s2, r2)
    begin()
    local = local_phase(acts, dlog, skip)
    turn()
    end()
    later = carried_phase(acts, local, st, ci, cm, gi, gm, ds, gmt)
    sums_phase(
        norm, later, xe, gi, gm, ds, gmt, wih, wm, ws, mt, fat, fb, ig, *rest
    )


def whole(norm, *args):
    dma = pltpu.SemaphoreType.DMA
    n = 2 * NZ

    def vm(*shape):
        return pltpu.VMEM(shape, BF16)

    return pl.pallas_call(
        functools.partial(whole_kernel, norm),
        out_shape=(
            jax.ShapeDtypeStruct((8, 16, 128), F32),
            jax.ShapeDtypeStruct((2, 40, 128), F32),
            jax.ShapeDtypeStruct((2, 40, 256), F32),
            jax.ShapeDtypeStruct((32, D), BF16),
        ),
        in_specs=[pl.BlockSpec(memory_space=pltpu.HBM)] * 10,
        out_specs=(VM,) * 4,
        scratch_shapes=[
            vm(EXT, D), vm(2, TOK // 2, 2 * INNER), vm(D, 2 * INNER), vm(D, 2 * STATE), vm(10, D),
            pltpu.VMEM((4, 2 * INNER), F32), pltpu.VMEM((4, 2 * STATE), F32),
            pltpu.VMEM((1, 10), F32), pltpu.VMEM((1, 10), F32), pltpu.VMEM((1, 10), F32),
            vm(D, INNER), vm(n, CHUNK, STATE), vm(n, CHUNK, STATE), vm(n, CHUNK, STATE),
            vm(n, CHUNK, STATE), vm(EXT, INNER), vm(EXT, 2 * STATE), vm(EXT, 128), vm(8, 32, EXT),
            dma((13,)), dma((13,)), dma((4,)), dma((10,)), dma((2,)),
            dma((n,)), dma((n,)), dma((n,)), dma((n,)),
            vm(2, 2, 16, D), vm(4, PRE, D), vm(8, 32, EXT),
            vm(4, NZ, 2, ROWS, 128), vm(2, 4, 2, ROWS, 128), vm(2, NZ, 2, ROWS, 128),
            vm(NZ, 4, ROWS, 128), vm(2, 4, ROWS, 128), vm(2, 2, ROWS, 128),
            vm(2, 4, ROWS, 128), vm(2, 4, ROWS, 128), vm(4, ROWS, 128), vm(4, ROWS, 128),
            vm(NZ, 2, ROWS, 128), vm(2, 2, ROWS, 128), vm(2, 1, ROWS, 128),
            vm(2, 2, ROWS, 128), vm(2, 2, ROWS, 128),
            pltpu.VMEM((2, 40, 128), F32), pltpu.VMEM((8, 16, 128), F32),
            pltpu.VMEM((2, 40, 256), F32),
            vm(2, 4, 2, 16, D), vm(4, 2, 16, D), vm(2, 16, D), vm(PRE, D), vm(PRE, D),
            dma((8,)), dma((8,)), dma((6,)), dma((6,)), dma((8,)), dma((8,)),
            dma((8,)), dma((8,)), dma((6,)), dma((6,)), dma(()), dma((4,)), dma((4,)), dma((4,)),
            dma((8,)), dma((8,)), dma((3,)), dma((3,)),
        ],
        compiler_params=pltpu.CompilerParams(
            collective_id=0, has_side_effects=True, vmem_limit_bytes=LIMIT
        ),
        name="whole",
    )(*args)


def finish_kernel(mt, fat, fb, ig, ig_o, iw_o, mw_o, sw_o):
    pick = one_hot(iota((HEADS, 128), 1) == iota((HEADS, 128), 0) + 96)
    for k in range(2):
        iw_o[:, k * INNER : k * INNER + 256] = fb[k]
        own = fat[k]
        iw_o[:, k * INNER + 256 : (k + 1) * INNER] = own[:, :64]
        sw_o[k * HEADS : (k + 1) * HEADS, :] = lax.dot_general(
            pick, own, (((1,), (1,)), ((), ())), preferred_element_type=F32,
            precision=lax.Precision.HIGHEST,
        )
    for j in range(8):
        mw_o[:, j * 32 : (j + 1) * 32] = mt[j, :10, 64:96]
    ig_o[...] = ig[...]


def finish(*args):
    return pl.pallas_call(
        finish_kernel,
        out_shape=(
            jax.ShapeDtypeStruct((32, D), BF16),
            jax.ShapeDtypeStruct((40, 2 * INNER), F32),
            jax.ShapeDtypeStruct((10, 2 * STATE), F32),
            jax.ShapeDtypeStruct((2 * HEADS, 40), F32),
        ),
        in_specs=[VM] * 4,
        out_specs=(VM,) * 4,
        compiler_params=pltpu.CompilerParams(vmem_limit_bytes=LIMIT),
        name="finish",
    )(*args)


def body(
    layer_input,
    inner_weight,
    mixer_weight,
    step_weight,
    conv_inner,
    conv_mixer,
    step_bias,
    decay_log,
    skip_gain,
    output_grad,
):
    norm = 1.0 / math.sqrt(8192)
    stepw = step_weight.T
    bias, dlog, skip = (v.reshape(1, -1) for v in (step_bias, decay_log, skip_gain))
    parts = whole(
        norm, layer_input[0], output_grad[0], inner_weight, mixer_weight, stepw, conv_inner,
        conv_mixer, bias, dlog, skip,
    )
    ig, iw, mw, sw = finish(*parts)
    return ig[None], iw, mw, sw.T


def solution(mesh):
    split = Mesh(
        mesh.devices.reshape(mesh.shape["dp"], 8, 2, 2, mesh.shape["chan"]),
        ("dp", "seq_0", "seq_1", "seq_2", "chan"),
    )
    placed = (
        P("dp", SEQ_CHAN, None),
        P(None, "chan"),
        P(),
        P(None, "chan"),
        P(None, "chan"),
        P(),
        P("chan"),
        P("chan"),
        P("chan"),
        P("dp", SEQ, "chan"),
    )
    return jax.shard_map(
        body,
        mesh=split,
        in_specs=placed,
        out_specs=(
            P("dp", SEQ_CHAN, None),
            P(DP_SEQ, "chan"),
            P(DP_SEQ_CHAN, None),
            P(DP_SEQ, "chan"),
        ),
        check_vma=False,
    )
```

```python
import functools
import math

import jax
import jax.numpy as jnp
from jax import lax
from jax.experimental import pallas as pl
from jax.experimental.pallas import tpu as pltpu
from jax.sharding import Mesh
from jax.sharding import PartitionSpec as P

D = 2560
HDIM = 64
HEADS = 5
INNER = HEADS * HDIM
STATE = 128
TOK = 256
PRE = 16
EXT = TOK + PRE
NZ = 8
ROWS = 80
CHUNK = 48
F32 = jnp.float32
BF16 = jnp.bfloat16
SEQ = ("seq_0", "seq_1", "seq_2")
DP_SEQ = ("dp", "seq_0", "seq_1", "seq_2")
SEQ_CHAN = ("seq_0", "seq_1", "seq_2", "chan")
DP_SEQ_CHAN = ("dp", "seq_0", "seq_1", "seq_2", "chan")
MESH = pl.DeviceIdType.MESH
VM = pl.BlockSpec(memory_space=pltpu.VMEM)
LIMIT = 62 * 1024 * 1024


def roll(v, shift):
    return pltpu.roll(v, shift % v.shape[0], 0)


def mm(a, b):
    return jnp.dot(a, b, preferred_element_type=F32)


def mm_t(a, b):
    return lax.dot_general(a, b, (((1,), (1,)), ((), ())), preferred_element_type=F32)


def t_mm(a, b):
    return lax.dot_general(a, b, (((0,), (0,)), ((), ())), preferred_element_type=F32)


def exact(a, b):
    return jnp.dot(a, b, preferred_element_type=F32, precision=lax.Precision.HIGHEST)


def iota(shape, dim):
    return lax.broadcasted_iota(jnp.int32, shape, dim)


def one_hot(cond):
    return jnp.where(cond, 1.0, 0.0).astype(F32)


def head_expand():
    return one_hot(iota((128, INNER), 1) // HDIM == iota((128, INNER), 0))


def head_sum():
    return one_hot(iota((INNER, 128), 0) // HDIM == iota((INNER, 128), 1))


def head_pick(core):
    return one_hot(
        (iota((10, 128), 0) == iota((10, 128), 1) + HEADS * core) & (iota((10, 128), 1) < HEADS)
    )


def half_of(v, core):
    return jnp.where(core == 0, v[:, :INNER], v[:, INNER:])


def conv(v, k):
    return k[3:4] * v + k[2:3] * roll(v, 1) + k[1:2] * roll(v, 2) + k[0:1] * roll(v, 3)


def conv_back(g, k):
    return k[3:4] * g + k[2:3] * roll(g, -1) + k[1:2] * roll(g, -2) + k[0:1] * roll(g, -3)


def gather_phase(xe, ogx, ssem, rsem, tsem):
    z, yh, c, x = (lax.axis_index(a) for a in SEQ_CHAN)
    right, left = lax.rem(x + 1, 4), lax.rem(x + 3, 4)
    sib = 1 - c
    q = z * 2 + yh
    nq, pq = lax.rem(q + 1, 2 * NZ), lax.rem(q + 2 * NZ - 1, 2 * NZ)
    def slot(core, chan, half=None):
        base = PRE + (core * 4 + chan) * 32
        if half is None:
            return xe.at[pl.ds(pl.multiple_of(base, 16), 32), :]
        return xe.at[pl.ds(pl.multiple_of(base + 16 * half, 16), 16), :]

    def copy(src, dst, k, **where):
        return pltpu.make_async_remote_copy(
            src_ref=src, dst_ref=dst, send_sem=ssem.at[k], recv_sem=rsem.at[k],
            device_id=where, device_id_type=MESH,
        )

    mine = slot(c, x)
    own_og = ogx.at[c]

    def half(h):
        return slot(c, x, h)

    r0 = copy(half(0), slot(c, x, 0), 0, chan=right)
    l1 = copy(half(1), slot(c, x, 1), 1, chan=left)
    r1 = copy(half(1), slot(c, x, 1), 2, chan=right)
    l0 = copy(half(0), slot(c, x, 0), 3, chan=left)
    sp = copy(mine, mine, 4, seq_2=sib)
    so = copy(own_og, own_og, 5, seq_2=sib)
    for d in (r0, l1):
        d.start()

    def tails(chan):
        return pltpu.make_async_remote_copy(
            src_ref=half(1), dst_ref=xe.at[pl.ds(0, 16), :], send_sem=tsem.at[chan],
            recv_sem=rsem.at[6],
            device_id={"seq_0": nq // 2, "seq_1": lax.rem(nq, 2), "chan": chan},
            device_id_type=MESH,
        )

    @pl.when((c == 1) & (x == 3))
    def _():
        for chan in range(4):
            tails(chan).start()

    for d in (r1, l0, sp, so):
        d.start()
    far = lax.rem(x + 2, 4)
    in_r0 = copy(half(0), slot(c, left, 0), 0, chan=right)
    in_r1 = copy(half(1), slot(c, left, 1), 2, chan=right)
    in_l1 = copy(half(1), slot(c, right, 1), 1, chan=left)
    in_l0 = copy(half(0), slot(c, right, 0), 3, chan=left)
    rr = copy(slot(c, left, 0), slot(c, left, 0), 7, chan=right)
    ll = copy(slot(c, right, 1), slot(c, right, 1), 8, chan=left)
    in_r0.wait_recv()
    rr.start()
    in_l1.wait_recv()
    ll.start()
    in_r1.wait_recv()
    s_left = copy(slot(c, left), slot(c, left), 9, seq_2=sib)
    s_left.start()
    in_l0.wait_recv()
    s_right = copy(slot(c, right), slot(c, right), 10, seq_2=sib)
    s_right.start()
    tail_on = copy(xe.at[pl.ds(0, 16), :], xe.at[pl.ds(0, 16), :], 12, seq_2=sib)

    @pl.when(c == 1)
    def _():
        tails(0).wait_recv()
        tail_on.start()

    in_rr = copy(half(0), slot(c, far, 0), 7, chan=right)
    in_ll = copy(half(1), slot(c, far, 1), 8, chan=left)
    in_rr.wait_recv()
    in_ll.wait_recv()
    s_far = copy(slot(c, far), slot(c, far), 11, seq_2=sib)
    s_far.start()
    copy(mine, slot(sib, x), 4, seq_2=sib).wait_recv()
    copy(own_og, ogx.at[sib], 5, seq_2=sib).wait_recv()
    copy(mine, slot(sib, left), 9, seq_2=sib).wait_recv()
    copy(mine, slot(sib, right), 10, seq_2=sib).wait_recv()
    copy(mine, slot(sib, far), 11, seq_2=sib).wait_recv()

    @pl.when(c == 0)
    def _():
        tail_on.wait_recv()

    for d in (r0, l1, r1, l0, sp, so, rr, ll, s_left, s_right, s_far):
        d.wait_send()

    @pl.when(c == 1)
    def _():
        tail_on.wait_send()

    @pl.when((c == 1) & (x == 3))
    def _():
        for chan in range(4):
            tails(chan).wait_send()


def forward_phase(xe, ogx, wi, wm, ws, ci, cm, bias, dlog, wih_o, send_o):
    z, yh, c = (lax.axis_index(a) for a in SEQ)
    flag = jnp.where(z * 2 + yh == 0, 0.0, 1.0).astype(F32)
    pick = head_pick(c)
    wih = half_of(wi[...], c)
    wih_o[...] = wih
    xv = xe[...]
    keep = jnp.where(iota((EXT, 1), 0) < PRE, flag, 1.0)

    def masked(v):
        return jnp.where(keep > 0.0, v.astype(BF16).astype(F32), 0.0)

    pi = masked(mm(xv, wih))
    pm = masked(mm(xv, wm[...]))
    sr = exact(mm_t(xv, ws[...])[PRE:], pick)
    zi = conv(pi, half_of(ci[...], c))[PRE:]
    zm = conv(pm, cm[...])[PRE:]
    xa = zi * jax.nn.sigmoid(zi)
    ma = zm * jax.nn.sigmoid(zm)
    srb = sr + exact(bias[...], pick)
    dt = jnp.maximum(srb, 0.0) + jnp.log1p(jnp.exp(-jnp.abs(srb)))
    rate = exact(jnp.exp(dlog[...]), pick)
    a = -dt * rate
    tri = one_hot(iota((TOK, TOK), 0) >= iota((TOK, TOK), 1))
    cum = exact(tri, a)
    tot = cum[TOK - 1 : TOK]
    og = half_of(ogx[...].reshape(TOK, 2 * INNER), c)
    ex = head_expand()
    xt = (xa * exact(dt * jnp.exp(tot - cum), ex)).astype(BF16)
    yt = (og.astype(F32) * exact(jnp.exp(cum), ex)).astype(BF16)
    f_loc = t_mm(xt, ma[:, :STATE].astype(BF16))
    g_loc = t_mm(yt, ma[:, STATE:].astype(BF16))
    diag = jnp.where(iota((8, 128), 0) == iota((8, 128), 1), tot, 0.0)
    dm = exact(diag, jnp.ones((128, 128), F32))
    hi = dm.astype(BF16).astype(F32)
    drow = jnp.where(iota((8, 128), 1) < 64, hi, dm - hi)
    for zz in range(NZ):
        for which, v in ((0, f_loc), (1, g_loc)):
            rows = [v[h * HDIM + zz * 8 : h * HDIM + zz * 8 + 8] for h in range(HEADS)]
            send_o[zz * 2 + which] = jnp.concatenate(rows + [drow], axis=0).astype(BF16)
    return xa, zi, zm, dt, cum, srb, og


def state_phases(send, out, recv, back, local_sem, s1, r1, s2, r2):
    z, yh = lax.axis_index("seq_0"), lax.axis_index("seq_1")
    n = 2 * NZ
    me = z * 2 + yh
    def at(q):
        return {"seq_0": q // 2, "seq_1": lax.rem(q, 2)}

    def push(src, dst, ss, rs, off):
        to = lax.rem(me + off, n)
        return pltpu.make_async_remote_copy(
            src_ref=src.at[to], dst_ref=dst.at[me], send_sem=ss.at[off], recv_sem=rs.at[off],
            device_id=at(to), device_id_type=MESH,
        )

    def pull(src, dst, ss, rs, off):
        origin = lax.rem(me + n - off, n)
        return pltpu.make_async_remote_copy(
            src_ref=src.at[origin], dst_ref=dst.at[origin], send_sem=ss.at[off],
            recv_sem=rs.at[off], device_id=at(origin), device_id_type=MESH,
        )

    order = sorted(range(1, n), key=lambda off: -min(off, n - off))
    first = [push(send, recv, s1, r1, off) for off in order]
    second = [push(back, out, s2, r2, off) for off in order]

    def begin():
        for d in first:
            d.start()
        own = pltpu.make_async_copy(send.at[me], recv.at[me], local_sem.at[0])
        own.start()
        own.wait()

    def turn():
        for off in range(1, n):
            pull(send, recv, s1, r1, off).wait_recv()
        run = jnp.zeros((HEADS * 8, STATE), F32)
        for j in range(n):
            k = jnp.where(yh == 0, j, n - 1 - j)
            got = recv[k].astype(F32)
            rows = got[HEADS * 8 :]
            rows = rows + pltpu.roll(rows, 64, 1)
            decay = jnp.exp(rows)
            back[k] = run.astype(BF16)
            wide = jnp.concatenate(
                [jnp.broadcast_to(decay[h : h + 1], (8, STATE)) for h in range(HEADS)], axis=0
            )
            run = wide * run + got[: HEADS * 8]
        for d in second:
            d.start()
        own = pltpu.make_async_copy(back.at[me], out.at[me], local_sem.at[1])
        own.start()
        own.wait()

    def end():
        for off in range(1, n):
            pull(back, out, s2, r2, off).wait_recv()
        for d in first + second:
            d.wait_send()

    return begin, turn, end


def local_phase(acts, dlog, skip):
    c = lax.axis_index("seq_2")
    pick = head_pick(c)
    ex = head_expand()
    xa, zi, zm, dt, cum, srb, og = acts
    dy = og.astype(F32)
    rate = exact(jnp.exp(dlog[...]), pick)
    skp = exact(skip[...], pick)
    tot = cum[TOK - 1 : TOK]
    ecum = exact(jnp.exp(cum), ex)
    etail = exact(jnp.exp(tot - cum), ex)
    dte = exact(dt, ex)
    sz = jax.nn.sigmoid(zm)
    ma = zm * sz
    bm, cmx = ma[:, :STATE].astype(BF16), ma[:, STATE:].astype(BF16)
    xdt = xa * dte
    xdtb = xdt.astype(BF16)
    xdtf = xdtb.astype(F32)
    scores = mm_t(cmx, bm)
    causal = iota((TOK, TOK), 0) >= iota((TOK, TOK), 1)
    cumt = cum.T
    dscore = jnp.zeros((TOK, TOK), F32)
    ys, us = [], []
    for h in range(HEADS):
        cols = slice(h * HDIM, (h + 1) * HDIM)
        decay = jnp.exp(jnp.where(causal, cum[:, h : h + 1] - cumt[h : h + 1, :], -1e30))
        m = (decay * scores).astype(BF16)
        ys.append(mm(m, xdtb[:, cols]))
        us.append(t_mm(m, og[:, cols]))
        dscore = dscore + decay * mm_t(og[:, cols], xdtb[:, cols])
    dsb = dscore.astype(BF16)
    d_out, d_in = mm(dsb, bm), t_mm(dsb, cmx)
    yt, xt = (dy * ecum).astype(BF16), (xdt * etail).astype(BF16)
    gate_m = sz * (1.0 + zm * (1.0 - sz))
    si = jax.nn.sigmoid(zi)
    gate_i = si * (1.0 + zi * (1.0 - si))
    return (
        jnp.concatenate(ys, axis=1), jnp.concatenate(us, axis=1), d_out, d_in, yt, xt, gate_m,
        gate_i, bm, cmx, xdtf, dy, rate, exact(skp, ex), tot, ecum, etail, dte,
    )


def carried_phase(acts, local, st, ci, cm, gi_o, gm_o, ds_o, gmt_o):
    z, yh, c = (lax.axis_index(a) for a in SEQ)
    flag = jnp.where(z * 2 + yh == 0, 0.0, 1.0).astype(F32)
    hs = head_sum()
    xa, _, _, _, _, srb, _ = acts
    (
        y_loc, u_loc, d_out, d_in, yt, xt, gate_m, gate_i, bm, cmx, xdtf, dy, rate, skp, tot,
        ecum, etail, dte,
    ) = local
    keep = jnp.where(iota((EXT, 1), 0) < PRE, flag, 1.0)

    def collect(which):
        blocks = [st[2 * zz + which].astype(F32) for zz in range(NZ)]
        rows = [blocks[zz][h * 8 : h * 8 + 8] for h in range(HEADS) for zz in range(NZ)]
        return jnp.concatenate(rows, axis=0)

    def back(g, k):
        g = jnp.concatenate([jnp.zeros((PRE, g.shape[1]), F32), g], axis=0)
        return jnp.where(keep > 0.0, conv_back(g, k), 0.0).astype(BF16)

    h0, ge = collect(0), collect(1)
    h0b, geb = h0.astype(BF16), ge.astype(BF16)
    ug = etail * mm_t(bm, geb)
    u = u_loc + ug
    gi_o[...] = back((dte * u + skp * dy) * gate_i, half_of(ci[...], c))

    def mixing():
        gm = jnp.concatenate([d_in + mm(xt, geb), d_out + mm(yt, h0b)], axis=1) * gate_m
        gm_o[...] = back(gm, cm[...])
        eye = one_hot(iota((TOK, TOK), 0) == iota((TOK, TOK), 1)).astype(BF16)
        gmt = t_mm(gm.astype(BF16), eye).astype(BF16)
        for j in range(8):
            gmt_o[j] = gmt[j * 32 : j * 32 + 32]

    def mixed(total):
        j8 = c * 4 + lax.axis_index("chan")
        place = one_hot(iota((32, 128), 1) == iota((32, 128), 0) + 64).astype(BF16)
        cols = one_hot(iota((2 * STATE, 128), 0) == j8 * 32 + iota((2 * STATE, 128), 1) - 64)
        lanes = iota((2 * STATE, 128), 1)
        cols = jnp.where((lanes >= 64) & (lanes < 96), cols, 0.0)
        return back(t_mm(total.astype(BF16), place), exact(cm[...], cols))

    def stepping():
        y = y_loc + ecum * mm_t(cmx, h0b)
        ddt = exact(xa * u, hs)
        dcum = exact(dy * y - xdtf * u, hs)
        e_sum = jnp.sum(exact(xdtf * ug, hs), axis=0, keepdims=True)
        hg = exact(jnp.ones((8, STATE), F32), (h0 * ge).T)
        carry = jnp.exp(tot) * exact(hg, hs)[0:1]
        upper = one_hot(iota((TOK, TOK), 0) <= iota((TOK, TOK), 1))
        da = exact(upper, dcum) + e_sum + carry
        dsr = (ddt - rate * da) * jax.nn.sigmoid(srb)
        ds_o[...] = jnp.concatenate([jnp.zeros((PRE, 128), F32), dsr], axis=0).astype(BF16)

    return mixing, mixed, stepping


def sums_phase(
    norm, later, xet, gi_r, gm_r, ds_r, gmt, wih, wm, ws,
    mt, fat, fb, ig, xin, pbin,
    mixin, rb, yhold, yin, ra, a3, a4, a1, a2, sa, ya, sb, b3, b4, b1, b2, fa, mrows, fbs, p, psib, xhold,
    pb, pbsib,
    ms, mr, ys, yr, zs, zr, qs, qr, xs, xr, es, er, as_, ar, ts, tr, dsem, drem,
):
    dp = lax.axis_index("dp")
    z, yh, c, x = (lax.axis_index(a) for a in SEQ_CHAN)
    y = yh * 2 + dp
    j8 = c * 4 + x
    sib = 1 - c
    q = z * 2 + yh
    nq, pq = lax.rem(q + 1, 2 * NZ), lax.rem(q + 2 * NZ - 1, 2 * NZ)
    def at_z(off):
        return {"seq_0": lax.rem(z + off + NZ, NZ)}

    def at_y(off):
        k = lax.rem(y + off + 4, 4)
        return {"seq_1": k // 2, "dp": lax.rem(k, 2)}

    def at_x(off):
        return {"chan": lax.rem(x + off + 4, 4)}

    def at_j(k):
        return {"seq_2": k // 4, "chan": lax.rem(k, 4)}

    def remote(src, dst, ss, rs, where):
        return pltpu.make_async_remote_copy(
            src_ref=src, dst_ref=dst, send_sem=ss, recv_sem=rs, device_id=where,
            device_id_type=MESH,
        )

    pending = []

    def go(d):
        d.start()
        pending.append(d)
        return d

    def send_mix():
        for off in range(1, 8):
            to = lax.rem(j8 + off, 8)
            go(remote(gmt.at[to], mixin.at[off], ms.at[off], mr.at[off], at_j(to)))

    mixing, mixed, stepping = later

    gi = gi_r[...]
    rhs = gi[:, :256]

    def inner_rows(side, zhi):
        base = pl.multiple_of(side * 1280 + zhi * 640, 128)
        r = (mm(xet[pl.ds(base, 640), :], rhs) * norm).astype(BF16)
        for g in range(8):
            for k in range(2):
                rb[k, (g % 2) * 2 + side, zhi * 4 + g // 2] = r[
                    g * ROWS : (g + 1) * ROWS, k * 128 : (k + 1) * 128
                ]

    up, down, far = lax.rem(y + 1, 4), lax.rem(y + 3, 4), lax.rem(y + 2, 4)
    lo, hi = pl.ds(0, 4), pl.ds(4, 4)

    def hold(k, sign):
        i = 0 if sign == 1 else 1
        part = lo if sign == 1 else hi
        return remote(
            rb.at[k, far, part], yhold.at[k, i], ys.at[6 * k + i], yr.at[6 * k + i], at_y(sign)
        )

    def plain(k, sign):
        i = 0 if sign == 1 else 1
        to, part = (up, hi) if sign == 1 else (down, lo)
        return remote(
            rb.at[k, to, part], yin.at[k, i, part], ys.at[6 * k + 2 + i], yr.at[6 * k + 2 + i],
            at_y(sign),
        )

    def second(k, sign):
        i = 0 if sign == 1 else 1
        part = lo if sign == 1 else hi
        return remote(
            yhold.at[k, i], yin.at[k, i, part], ys.at[6 * k + 4 + i], yr.at[6 * k + 4 + i],
            at_y(sign),
        )

    def ring_on(k):
        for sign, to, first in ((1, up, 0), (-1, down, 4)):
            i = 0 if sign == 1 else 1
            hold(k, sign).wait_recv()
            for e in range(4):
                v = rb[k, to, first + e].astype(F32) + yhold[k, i, e].astype(F32)
                yhold[k, i, e] = v.astype(BF16)
            go(second(k, sign))

    def ring_end(k):
        for sign in (1, -1):
            plain(k, sign).wait_recv()
            second(k, sign).wait_recv()
        for e in range(NZ):
            v = rb[k, y, e].astype(F32) + yin[k, 0, e].astype(F32) + yin[k, 1, e].astype(F32)
            v = v.astype(BF16)
            sb[k, e, 0] = v[:40]
            sb[k, e, 1] = v[40:]

    inner_rows(dp, 0)
    go(hold(0, 1))
    inner_rows(dp, 1)
    go(hold(0, -1))
    mixing()
    send_mix()
    inner_rows(1 - dp, 1)
    go(plain(0, 1))
    inner_rows(1 - dp, 0)
    go(plain(0, -1))
    go(hold(1, 1))
    go(hold(1, -1))
    stepping()
    ring_on(0)
    go(plain(1, 1))
    go(plain(1, -1))

    ds = ds_r[...]
    pick = head_pick(c).astype(BF16)
    ds10 = mm_t(ds, pick).astype(BF16)
    gm = gm_r[...]
    for b in range(4):
        rows = slice(b * 640, (b + 1) * 640)
        part = mm_t(gi, wih[rows]) + mm_t(gm, wm[rows]) + mm(ds10, ws[:, rows])
        part = part.astype(BF16)
        pb[:, rows] = part[:PRE]
        for j in range(8):
            for k in range(2):
                at = PRE + j * 32 + k * 16
                p[j // 4, j % 4, k, :, rows] = part[at : at + 16]
    go(remote(p.at[sib], psib, dsem.at[0], drem.at[0], {"seq_2": sib}))
    pb_out = remote(pb, pbsib, dsem.at[1], drem.at[1], {"seq_2": sib})

    @pl.when(c == 0)
    def _():
        pb_out.start()

    total = gmt[j8].astype(F32)
    for off in range(1, 8):
        origin = lax.rem(j8 + 8 - off, 8)
        remote(gmt.at[origin], mixin.at[off], ms.at[off], mr.at[off], at_j(origin)).wait_recv()
        total = total + mixin[off].astype(F32)
    place_step = one_hot(
        (iota((128, 128), 1) == iota((128, 128), 0) + 96) & (iota((128, 128), 0) < HEADS)
    ).astype(BF16)
    last = mixed(total).astype(F32) + mm(ds, place_step)
    last = last + jnp.concatenate([gi[:, 256:].astype(F32), jnp.zeros((EXT, 64), F32)], axis=1)
    last = last.astype(BF16)
    for b in range(4):
        r = (mm(xet[b * 640 : (b + 1) * 640, :], last) * norm).astype(BF16)
        for g in range(8):
            ra[(b % 2) * 4 + g // 2, (g % 2) * 2 + b // 2] = r[g * ROWS : (g + 1) * ROWS]

    def z_first(src, n, r3, r4, r1, s, r, o=0):
        h = n // 2
        for k, sign in enumerate((1, -1)):
            part = pl.ds(k * h, h)
            dst = [lax.rem(z + sign * d + NZ, NZ) for d in range(5)]
            go(remote(src.at[dst[4], part], r4.at[k], s.at[o + 4 * k], r.at[o + 4 * k], at_z(2 * sign)))
            go(remote(src.at[dst[3]], r3.at[k], s.at[o + 4 * k + 1], r.at[o + 4 * k + 1], at_z(sign)))
            go(remote(src.at[dst[1]], r1.at[k], s.at[o + 4 * k + 2], r.at[o + 4 * k + 2], at_z(sign)))

    def z_second(src, n, r3, r4, r2, s, r, o=0):
        h = n // 2
        for k, sign in enumerate((1, -1)):
            part = pl.ds(k * h, h)
            t = lax.rem(z + 2 * sign + NZ, NZ)
            remote(r3.at[k], r3.at[k], s.at[o + 4 * k + 1], r.at[o + 4 * k + 1], at_z(sign)).wait_recv()
            remote(r4.at[k], r4.at[k], s.at[o + 4 * k], r.at[o + 4 * k], at_z(2 * sign)).wait_recv()
            for i in range(n):
                v = src[t, i].astype(F32) + r3[k, i].astype(F32)
                if k * h <= i < (k + 1) * h:
                    v = v + r4[k, i - k * h].astype(F32)
                r3[k, i] = v.astype(BF16)
            go(remote(r3.at[k], r2.at[k], s.at[o + 4 * k + 3], r.at[o + 4 * k + 3], at_z(2 * sign)))

    def z_last(r1, r2, s, r, o=0):
        for k, sign in enumerate((1, -1)):
            remote(r1.at[k], r1.at[k], s.at[o + 4 * k + 2], r.at[o + 4 * k + 2], at_z(sign)).wait_recv()
            remote(r2.at[k], r2.at[k], s.at[o + 4 * k + 3], r.at[o + 4 * k + 3], at_z(2 * sign)).wait_recv()

    z_first(ra, 4, a3, a4, a1, zs, zr)

    ring_on(1)

    remote(psib, psib, dsem.at[0], drem.at[0], {"seq_2": sib}).wait_recv()
    for k in range(4):
        for h in range(2):
            psib[k, h] = (p[c, k, h].astype(F32) + psib[k, h].astype(F32)).astype(BF16)
    xu, xd, xf = lax.rem(x + 1, 4), lax.rem(x + 3, 4), lax.rem(x + 2, 4)
    go(remote(psib.at[xf, 0], xhold.at[0], xs.at[0], xr.at[0], at_x(1)))
    go(remote(psib.at[xf, 1], xhold.at[1], xs.at[1], xr.at[1], at_x(-1)))
    go(remote(psib.at[xu, 1], xin.at[0, 1], xs.at[2], xr.at[2], at_x(1)))
    go(remote(psib.at[xd, 0], xin.at[1, 0], xs.at[3], xr.at[3], at_x(-1)))
    edge = remote(
        pbsib, pbin.at[x], es, er.at[x],
        {"seq_0": pq // 2, "seq_1": lax.rem(pq, 2), "chan": 3},
    )

    @pl.when(c == 1)
    def _():
        pb_out.wait_recv()
        pbsib[...] = (pb[...].astype(F32) + pbsib[...].astype(F32)).astype(BF16)
        edge.start()

    ring_end(0)
    z_first(sb.at[0], 2, b3.at[0], b4.at[0], b1.at[0], qs, qr)
    z_second(ra, 4, a3, a4, a2, zs, zr)
    ring_end(1)
    z_first(sb.at[1], 2, b3.at[1], b4.at[1], b1.at[1], qs, qr, 8)
    z_second(sb.at[0], 2, b3.at[0], b4.at[0], b2.at[0], qs, qr)

    z_last(a1, a2, zs, zr)
    for i in range(4):
        v = ra[z, i].astype(F32)
        for k in range(2):
            v = v + a1[k, i].astype(F32) + a2[k, i].astype(F32)
        sa[i] = v.astype(BF16)
    for off in (2, 1, 3):
        to = lax.rem(y + off, 4)
        go(remote(sa.at[to], ya.at[off], as_.at[off], ar.at[off], at_y(off)))

    remote(xhold.at[0], xhold.at[0], xs.at[0], xr.at[0], at_x(1)).wait_recv()
    xhold[0] = (psib[xu, 0].astype(F32) + xhold[0].astype(F32)).astype(BF16)
    go(remote(xhold.at[0], xin.at[0, 0], xs.at[4], xr.at[4], at_x(1)))
    remote(xhold.at[1], xhold.at[1], xs.at[1], xr.at[1], at_x(-1)).wait_recv()
    xhold[1] = (psib[xd, 1].astype(F32) + xhold[1].astype(F32)).astype(BF16)
    go(remote(xhold.at[1], xin.at[1, 1], xs.at[5], xr.at[5], at_x(-1)))

    z_second(sb.at[1], 2, b3.at[1], b4.at[1], b2.at[1], qs, qr, 8)

    v = sa[y].astype(F32)
    for off in range(1, 4):
        remote(ya.at[off], ya.at[off], as_.at[off], ar.at[off], at_y(off)).wait_recv()
        v = v + ya[off].astype(F32)
    fa[0] = v[:40]
    fa[1] = v[40:]
    go(remote(fa.at[sib], fat.at[c], ts.at[0], tr.at[0], {"seq_2": sib}))
    line = iota((128, 80), 0)
    wanted = (line // 64) * 40 + (lax.rem(line // 16, 4)) * 10 + lax.rem(line, 16)
    chosen = exact(one_hot((iota((128, 80), 1) == wanted) & (lax.rem(line, 16) < 10)), v)
    for j in range(8):
        mrows[j] = chosen[j * 16 : (j + 1) * 16]
    for off in range(1, 8):
        to = lax.rem(j8 + off, 8)
        go(remote(mrows.at[to], mt.at[j8], ts.at[off], tr.at[off], at_j(to)))
    fat[c] = fa[c]
    mt[j8] = mrows[j8]

    for k, half in ((2, 1), (4, 0)):
        remote(xin.at[0, half], xin.at[0, half], xs.at[k], xr.at[k], at_x(1)).wait_recv()
    for k, half in ((3, 0), (5, 1)):
        remote(xin.at[1, half], xin.at[1, half], xs.at[k], xr.at[k], at_x(-1)).wait_recv()
    for h in range(2):
        v = psib[x, h].astype(F32) + xin[0, h].astype(F32) + xin[1, h].astype(F32)
        ig[h * 16 : (h + 1) * 16, :] = v.astype(BF16)

    @pl.when((c == 1) & (x == 3))
    def _():
        v = psib[x, 1].astype(F32) + xin[0, 1].astype(F32) + xin[1, 1].astype(F32)
        for k in range(4):
            remote(pbsib, pbin.at[k], es, er.at[k], {"chan": 0}).wait_recv()
            v = v + pbin[k].astype(F32)
        ig[16:, :] = v.astype(BF16)

    for t in range(2):
        z_last(b1.at[t], b2.at[t], qs, qr, 8 * t)
        for i in range(2):
            v = sb[t, z, i].astype(F32)
            for k in range(2):
                v = v + b1[t, k, i].astype(F32) + b2[t, k, i].astype(F32)
            fbs[i, :, t * 128 : (t + 1) * 128] = v
    go(remote(fbs.at[sib], fb.at[c], dsem.at[2], drem.at[2], {"seq_2": sib}))
    fb[c] = fbs[c]

    for off in range(1, 8):
        origin = lax.rem(j8 + 8 - off, 8)
        remote(mrows.at[0], mt.at[origin], ts.at[off], tr.at[off], at_j(origin)).wait_recv()
    remote(fa.at[c], fat.at[sib], ts.at[0], tr.at[0], {"seq_2": sib}).wait_recv()

    remote(fbs.at[c], fb.at[sib], dsem.at[2], drem.at[2], {"seq_2": sib}).wait_recv()
    for d in pending:
        d.wait_send()

    @pl.when(c == 0)
    def _():
        pb_out.wait_send()

    @pl.when(c == 1)
    def _():
        edge.wait_send()


def whole_kernel(
    norm,
    piece, og, wi_h, wm_h, ws_h, ci_h, cm_h, bias_h, dlog_h, skip_h,
    mt, fat, fb, ig,
    xe, ogx, wi, wm, ws, ci, cm, bias, dlog, skip, wih, send, recv, back, st, gi, gm, ds, gmt, xet,
    gs, gr, gt, hsem, lsem, s1, r1, s2, r2, *rest,
):
    dp = lax.axis_index("dp")
    z, yh, c, x = (lax.axis_index(a) for a in SEQ_CHAN)
    n = 2 * NZ
    q = z * 2 + yh
    nq, pq = lax.rem(q + 1, n), lax.rem(q + n - 1, n)
    corner = (c == 1) & (x == 3)
    barrier = pltpu.get_barrier_semaphore()

    def tell(**where):
        pl.semaphore_signal(barrier, inc=1, device_id=where, device_id_type=MESH)

    for off in range(1, 8):
        k = lax.rem(c * 4 + x + off, 8)
        tell(seq_2=k // 4, chan=lax.rem(k, 4))
    for off in (1, 3):
        k = lax.rem(yh * 2 + dp + off, 4)
        tell(seq_1=k // 2, dp=lax.rem(k, 2))
    for off in range(1, n):
        k = lax.rem(q + off, n)
        tell(seq_0=k // 2, seq_1=lax.rem(k, 2))

    @pl.when(c == 1)
    def _():
        tell(seq_0=pq // 2, seq_1=lax.rem(pq, 2), chan=3)

    @pl.when(corner)
    def _():
        for k in range(4):
            tell(seq_0=nq // 2, seq_1=lax.rem(nq, 2), chan=k)

    base = pl.multiple_of(PRE + (c * 4 + x) * 32, 16)
    loads = [pltpu.make_async_copy(piece, xe.at[pl.ds(base, 32), :], hsem.at[0])]
    loads.append(pltpu.make_async_copy(og, ogx.at[c], hsem.at[1]))
    pairs = ((wi_h, wi), (wm_h, wm), (ws_h, ws), (ci_h, ci), (cm_h, cm))
    pairs += ((bias_h, bias), (dlog_h, dlog), (skip_h, skip))
    for k, (src, dst) in enumerate(pairs):
        loads.append(pltpu.make_async_copy(src, dst, hsem.at[2 + k]))
    for d in loads:
        d.start()
    loads[0].wait()
    loads[1].wait()
    pl.semaphore_wait(
        barrier, jnp.where(corner, 7 + 2 + n - 1 + 5, jnp.where(c == 1, 7 + 2 + n, 7 + 2 + n - 1))
    )
    gather_phase(xe, ogx, gs, gr, gt)
    for d in loads[2:]:
        d.wait()
    acts = forward_phase(xe, ogx, wi, wm, ws, ci, cm, bias, dlog, wih, send)
    begin, turn, end = state_phases(send, st, recv, back, lsem, s1, r1, s2, r2)
    begin()
    local = local_phase(acts, dlog, skip)
    turn()
    for b in range(4):
        cols = slice(b * 640, (b + 1) * 640)
        xet[cols, :] = xe[:, cols].T
    end()
    later = carried_phase(acts, local, st, ci, cm, gi, gm, ds, gmt)
    sums_phase(
        norm, later, xet, gi, gm, ds, gmt, wih, wm, ws, mt, fat, fb, ig, *rest
    )


def whole(norm, *args):
    dma = pltpu.SemaphoreType.DMA
    n = 2 * NZ

    def vm(*shape):
        return pltpu.VMEM(shape, BF16)

    return pl.pallas_call(
        functools.partial(whole_kernel, norm),
        out_shape=(
            jax.ShapeDtypeStruct((8, 16, 128), F32),
            jax.ShapeDtypeStruct((2, 40, 128), F32),
            jax.ShapeDtypeStruct((2, 40, 256), F32),
            jax.ShapeDtypeStruct((32, D), BF16),
        ),
        in_specs=[pl.BlockSpec(memory_space=pltpu.HBM)] * 10,
        out_specs=(VM,) * 4,
        scratch_shapes=[
            vm(EXT, D), vm(2, TOK // 2, 2 * INNER), vm(D, 2 * INNER), vm(D, 2 * STATE), vm(10, D),
            pltpu.VMEM((4, 2 * INNER), F32), pltpu.VMEM((4, 2 * STATE), F32),
            pltpu.VMEM((1, 10), F32), pltpu.VMEM((1, 10), F32), pltpu.VMEM((1, 10), F32),
            vm(D, INNER), vm(n, CHUNK, STATE), vm(n, CHUNK, STATE), vm(n, 8 * HEADS, STATE),
            vm(n, 8 * HEADS, STATE), vm(EXT, INNER), vm(EXT, 2 * STATE), vm(EXT, 128), vm(8, 32, TOK),
            vm(D, EXT),
            dma((13,)), dma((13,)), dma((4,)), dma((10,)), dma((2,)),
            dma((n,)), dma((n,)), dma((n,)), dma((n,)),
            vm(2, 2, 16, D), vm(4, PRE, D), vm(8, 32, TOK),
            vm(2, 4, NZ, ROWS, 128), vm(2, 2, 4, ROWS, 128), vm(2, 2, NZ, ROWS, 128),
            vm(NZ, 4, ROWS, 128), vm(2, 4, ROWS, 128), vm(2, 2, ROWS, 128),
            vm(2, 4, ROWS, 128), vm(2, 4, ROWS, 128), vm(4, ROWS, 128), vm(4, ROWS, 128),
            vm(2, NZ, 2, 40, 128), vm(2, 2, 2, 40, 128), vm(2, 2, 1, 40, 128),
            vm(2, 2, 2, 40, 128), vm(2, 2, 2, 40, 128),
            pltpu.VMEM((2, 40, 128), F32), pltpu.VMEM((8, 16, 128), F32),
            pltpu.VMEM((2, 40, 256), F32),
            vm(2, 4, 2, 16, D), vm(4, 2, 16, D), vm(2, 16, D), vm(PRE, D), vm(PRE, D),
            dma((8,)), dma((8,)), dma((12,)), dma((12,)), dma((8,)), dma((8,)),
            dma((16,)), dma((16,)), dma((6,)), dma((6,)), dma(()), dma((4,)), dma((4,)), dma((4,)),
            dma((8,)), dma((8,)), dma((3,)), dma((3,)),
        ],
        compiler_params=pltpu.CompilerParams(
            collective_id=0, has_side_effects=True, vmem_limit_bytes=LIMIT
        ),
        name="whole",
    )(*args)


def finish_kernel(mt, fat, fb, ig, ig_o, iw_o, mw_o, sw_o):
    pick = one_hot(iota((HEADS, 128), 1) == iota((HEADS, 128), 0) + 96)
    for k in range(2):
        iw_o[:, k * INNER : k * INNER + 256] = fb[k]
        own = fat[k]
        iw_o[:, k * INNER + 256 : (k + 1) * INNER] = own[:, :64]
        sw_o[k * HEADS : (k + 1) * HEADS, :] = lax.dot_general(
            pick, own, (((1,), (1,)), ((), ())), preferred_element_type=F32,
            precision=lax.Precision.HIGHEST,
        )
    for j in range(8):
        mw_o[:, j * 32 : (j + 1) * 32] = mt[j, :10, 64:96]
    ig_o[...] = ig[...]


def finish(*args):
    return pl.pallas_call(
        finish_kernel,
        out_shape=(
            jax.ShapeDtypeStruct((32, D), BF16),
            jax.ShapeDtypeStruct((40, 2 * INNER), F32),
            jax.ShapeDtypeStruct((10, 2 * STATE), F32),
            jax.ShapeDtypeStruct((2 * HEADS, 40), F32),
        ),
        in_specs=[VM] * 4,
        out_specs=(VM,) * 4,
        compiler_params=pltpu.CompilerParams(vmem_limit_bytes=LIMIT),
        name="finish",
    )(*args)


def body(
    layer_input,
    inner_weight,
    mixer_weight,
    step_weight,
    conv_inner,
    conv_mixer,
    step_bias,
    decay_log,
    skip_gain,
    output_grad,
):
    norm = 1.0 / math.sqrt(8192)
    stepw = step_weight.T
    bias, dlog, skip = (v.reshape(1, -1) for v in (step_bias, decay_log, skip_gain))
    parts = whole(
        norm, layer_input[0], output_grad[0], inner_weight, mixer_weight, stepw, conv_inner,
        conv_mixer, bias, dlog, skip,
    )
    ig, iw, mw, sw = finish(*parts)
    return ig[None], iw, mw, sw.T


def solution(mesh):
    split = Mesh(
        mesh.devices.reshape(mesh.shape["dp"], 8, 2, 2, mesh.shape["chan"]),
        ("dp", "seq_0", "seq_1", "seq_2", "chan"),
    )
    placed = (
        P("dp", SEQ_CHAN, None),
        P(None, "chan"),
        P(),
        P(None, "chan"),
        P(None, "chan"),
        P(),
        P("chan"),
        P("chan"),
        P("chan"),
        P("dp", SEQ, "chan"),
    )
    return jax.shard_map(
        body,
        mesh=split,
        in_specs=placed,
        out_specs=(
            P("dp", SEQ_CHAN, None),
            P(DP_SEQ, "chan"),
            P(DP_SEQ_CHAN, None),
            P(DP_SEQ, "chan"),
        ),
        check_vma=False,
    )
```

```python
import functools
import math

import jax
import jax.numpy as jnp
from jax import lax
from jax.experimental import pallas as pl
from jax.experimental.pallas import tpu as pltpu
from jax.sharding import Mesh
from jax.sharding import PartitionSpec as P

D = 2560
HDIM = 64
HEADS = 5
INNER = HEADS * HDIM
STATE = 128
TOK = 256
PRE = 16
EXT = TOK + PRE
NZ = 8
ROWS = 80
CHUNK = 48
F32 = jnp.float32
BF16 = jnp.bfloat16
SEQ = ("seq_0", "seq_1", "seq_2")
DP_SEQ = ("dp", "seq_0", "seq_1", "seq_2")
SEQ_CHAN = ("seq_0", "seq_1", "seq_2", "chan")
DP_SEQ_CHAN = ("dp", "seq_0", "seq_1", "seq_2", "chan")
MESH = pl.DeviceIdType.MESH
VM = pl.BlockSpec(memory_space=pltpu.VMEM)
LIMIT = 62 * 1024 * 1024


def roll(v, shift):
    return pltpu.roll(v, shift % v.shape[0], 0)


def mm(a, b):
    return jnp.dot(a, b, preferred_element_type=F32)


def mm_t(a, b):
    return lax.dot_general(a, b, (((1,), (1,)), ((), ())), preferred_element_type=F32)


def t_mm(a, b):
    return lax.dot_general(a, b, (((0,), (0,)), ((), ())), preferred_element_type=F32)


def exact(a, b):
    return jnp.dot(a, b, preferred_element_type=F32, precision=lax.Precision.HIGHEST)


def iota(shape, dim):
    return lax.broadcasted_iota(jnp.int32, shape, dim)


def one_hot(cond):
    return jnp.where(cond, 1.0, 0.0).astype(F32)


def head_expand():
    return one_hot(iota((128, INNER), 1) // HDIM == iota((128, INNER), 0))


def head_sum():
    return one_hot(iota((INNER, 128), 0) // HDIM == iota((INNER, 128), 1))


def head_pick(core):
    return one_hot(
        (iota((10, 128), 0) == iota((10, 128), 1) + HEADS * core) & (iota((10, 128), 1) < HEADS)
    )


def half_of(v, core):
    return jnp.where(core == 0, v[:, :INNER], v[:, INNER:])


def conv(v, k):
    return k[3:4] * v + k[2:3] * roll(v, 1) + k[1:2] * roll(v, 2) + k[0:1] * roll(v, 3)


def conv_back(g, k):
    return k[3:4] * g + k[2:3] * roll(g, -1) + k[1:2] * roll(g, -2) + k[0:1] * roll(g, -3)


def gather_phase(xe, ogx, ssem, rsem, tsem):
    z, yh, c, x = (lax.axis_index(a) for a in SEQ_CHAN)
    right, left = lax.rem(x + 1, 4), lax.rem(x + 3, 4)
    sib = 1 - c
    q = z * 2 + yh
    nq, pq = lax.rem(q + 1, 2 * NZ), lax.rem(q + 2 * NZ - 1, 2 * NZ)
    def slot(core, chan, half=None):
        base = PRE + (core * 4 + chan) * 32
        if half is None:
            return xe.at[pl.ds(pl.multiple_of(base, 16), 32), :]
        return xe.at[pl.ds(pl.multiple_of(base + 16 * half, 16), 16), :]

    def copy(src, dst, k, **where):
        return pltpu.make_async_remote_copy(
            src_ref=src, dst_ref=dst, send_sem=ssem.at[k], recv_sem=rsem.at[k],
            device_id=where, device_id_type=MESH,
        )

    mine = slot(c, x)
    own_og = ogx.at[c]

    def half(h):
        return slot(c, x, h)

    r0 = copy(half(0), slot(c, x, 0), 0, chan=right)
    l1 = copy(half(1), slot(c, x, 1), 1, chan=left)
    r1 = copy(half(1), slot(c, x, 1), 2, chan=right)
    l0 = copy(half(0), slot(c, x, 0), 3, chan=left)
    sp = copy(mine, mine, 4, seq_2=sib)
    so = copy(own_og, own_og, 5, seq_2=sib)
    for d in (r0, l1):
        d.start()

    def tails(chan):
        return pltpu.make_async_remote_copy(
            src_ref=half(1), dst_ref=xe.at[pl.ds(0, 16), :], send_sem=tsem.at[chan],
            recv_sem=rsem.at[6],
            device_id={"seq_0": nq // 2, "seq_1": lax.rem(nq, 2), "chan": chan},
            device_id_type=MESH,
        )

    @pl.when((c == 1) & (x == 3))
    def _():
        for chan in range(4):
            tails(chan).start()

    for d in (r1, l0, sp, so):
        d.start()
    far = lax.rem(x + 2, 4)
    in_r0 = copy(half(0), slot(c, left, 0), 0, chan=right)
    in_r1 = copy(half(1), slot(c, left, 1), 2, chan=right)
    in_l1 = copy(half(1), slot(c, right, 1), 1, chan=left)
    in_l0 = copy(half(0), slot(c, right, 0), 3, chan=left)
    rr = copy(slot(c, left, 0), slot(c, left, 0), 7, chan=right)
    ll = copy(slot(c, right, 1), slot(c, right, 1), 8, chan=left)
    in_r0.wait_recv()
    rr.start()
    in_l1.wait_recv()
    ll.start()
    in_r1.wait_recv()
    s_left = copy(slot(c, left), slot(c, left), 9, seq_2=sib)
    s_left.start()
    in_l0.wait_recv()
    s_right = copy(slot(c, right), slot(c, right), 10, seq_2=sib)
    s_right.start()
    tail_on = copy(xe.at[pl.ds(0, 16), :], xe.at[pl.ds(0, 16), :], 12, seq_2=sib)

    @pl.when(c == 1)
    def _():
        tails(0).wait_recv()
        tail_on.start()

    in_rr = copy(half(0), slot(c, far, 0), 7, chan=right)
    in_ll = copy(half(1), slot(c, far, 1), 8, chan=left)
    in_rr.wait_recv()
    in_ll.wait_recv()
    s_far = copy(slot(c, far), slot(c, far), 11, seq_2=sib)
    s_far.start()
    copy(mine, slot(sib, x), 4, seq_2=sib).wait_recv()
    copy(own_og, ogx.at[sib], 5, seq_2=sib).wait_recv()
    copy(mine, slot(sib, left), 9, seq_2=sib).wait_recv()
    copy(mine, slot(sib, right), 10, seq_2=sib).wait_recv()
    copy(mine, slot(sib, far), 11, seq_2=sib).wait_recv()

    @pl.when(c == 0)
    def _():
        tail_on.wait_recv()

    for d in (r0, l1, r1, l0, sp, so, rr, ll, s_left, s_right, s_far):
        d.wait_send()

    @pl.when(c == 1)
    def _():
        tail_on.wait_send()

    @pl.when((c == 1) & (x == 3))
    def _():
        for chan in range(4):
            tails(chan).wait_send()


def forward_phase(xe, ogx, wi, wm, ws, ci, cm, bias, dlog, wih_o, send_o):
    z, yh, c = (lax.axis_index(a) for a in SEQ)
    flag = jnp.where(z * 2 + yh == 0, 0.0, 1.0).astype(F32)
    pick = head_pick(c)
    wih = half_of(wi[...], c)
    wih_o[...] = wih
    xv = xe[...]
    keep = jnp.where(iota((EXT, 1), 0) < PRE, flag, 1.0)

    def masked(v):
        return jnp.where(keep > 0.0, v.astype(BF16).astype(F32), 0.0)

    pi = masked(mm(xv, wih))
    pm = masked(mm(xv, wm[...]))
    sr = exact(mm_t(xv, ws[...])[PRE:], pick)
    zi = conv(pi, half_of(ci[...], c))[PRE:]
    zm = conv(pm, cm[...])[PRE:]
    xa = zi * jax.nn.sigmoid(zi)
    ma = zm * jax.nn.sigmoid(zm)
    srb = sr + exact(bias[...], pick)
    dt = jnp.maximum(srb, 0.0) + jnp.log1p(jnp.exp(-jnp.abs(srb)))
    rate = exact(jnp.exp(dlog[...]), pick)
    a = -dt * rate
    tri = one_hot(iota((TOK, TOK), 0) >= iota((TOK, TOK), 1))
    cum = exact(tri, a)
    tot = cum[TOK - 1 : TOK]
    og = half_of(ogx[...].reshape(TOK, 2 * INNER), c)
    ex = head_expand()
    xt = (xa * exact(dt * jnp.exp(tot - cum), ex)).astype(BF16)
    yt = (og.astype(F32) * exact(jnp.exp(cum), ex)).astype(BF16)
    f_loc = t_mm(xt, ma[:, :STATE].astype(BF16))
    g_loc = t_mm(yt, ma[:, STATE:].astype(BF16))
    diag = jnp.where(iota((8, 128), 0) == iota((8, 128), 1), tot, 0.0)
    dm = exact(diag, jnp.ones((128, 128), F32))
    hi = dm.astype(BF16).astype(F32)
    drow = jnp.where(iota((8, 128), 1) < 64, hi, dm - hi)
    for zz in range(NZ):
        for which, v in ((0, f_loc), (1, g_loc)):
            rows = [v[h * HDIM + zz * 8 : h * HDIM + zz * 8 + 8] for h in range(HEADS)]
            send_o[zz * 2 + which] = jnp.concatenate(rows + [drow], axis=0).astype(BF16)
    return xa, zi, zm, dt, cum, srb, og


def state_phases(send, out, recv, back, local_sem, s1, r1, s2, r2):
    z, yh = lax.axis_index("seq_0"), lax.axis_index("seq_1")
    n = 2 * NZ
    me = z * 2 + yh
    def at(q):
        return {"seq_0": q // 2, "seq_1": lax.rem(q, 2)}

    def push(src, dst, ss, rs, off):
        to = lax.rem(me + off, n)
        return pltpu.make_async_remote_copy(
            src_ref=src.at[to], dst_ref=dst.at[me], send_sem=ss.at[off], recv_sem=rs.at[off],
            device_id=at(to), device_id_type=MESH,
        )

    def pull(src, dst, ss, rs, off):
        origin = lax.rem(me + n - off, n)
        return pltpu.make_async_remote_copy(
            src_ref=src.at[origin], dst_ref=dst.at[origin], send_sem=ss.at[off],
            recv_sem=rs.at[off], device_id=at(origin), device_id_type=MESH,
        )

    order = sorted(range(1, n), key=lambda off: -min(off, n - off))
    first = [push(send, recv, s1, r1, off) for off in order]
    second = [push(back, out, s2, r2, off) for off in order]

    def begin():
        for d in first:
            d.start()
        own = pltpu.make_async_copy(send.at[me], recv.at[me], local_sem.at[0])
        own.start()
        own.wait()

    def turn():
        for off in range(1, n):
            pull(send, recv, s1, r1, off).wait_recv()
        run = jnp.zeros((HEADS * 8, STATE), F32)
        for j in range(n):
            k = jnp.where(yh == 0, j, n - 1 - j)
            got = recv[k].astype(F32)
            rows = got[HEADS * 8 :]
            rows = rows + pltpu.roll(rows, 64, 1)
            decay = jnp.exp(rows)
            back[k] = run.astype(BF16)
            wide = jnp.concatenate(
                [jnp.broadcast_to(decay[h : h + 1], (8, STATE)) for h in range(HEADS)], axis=0
            )
            run = wide * run + got[: HEADS * 8]
        for d in second:
            d.start()
        own = pltpu.make_async_copy(back.at[me], out.at[me], local_sem.at[1])
        own.start()
        own.wait()

    def end():
        for off in range(1, n):
            pull(back, out, s2, r2, off).wait_recv()
        for d in first + second:
            d.wait_send()

    return begin, turn, end


def local_phase(acts, dlog, skip):
    c = lax.axis_index("seq_2")
    pick = head_pick(c)
    ex = head_expand()
    xa, zi, zm, dt, cum, srb, og = acts
    dy = og.astype(F32)
    rate = exact(jnp.exp(dlog[...]), pick)
    skp = exact(skip[...], pick)
    tot = cum[TOK - 1 : TOK]
    ecum = exact(jnp.exp(cum), ex)
    etail = exact(jnp.exp(tot - cum), ex)
    dte = exact(dt, ex)
    sz = jax.nn.sigmoid(zm)
    ma = zm * sz
    bm, cmx = ma[:, :STATE].astype(BF16), ma[:, STATE:].astype(BF16)
    xdt = xa * dte
    xdtb = xdt.astype(BF16)
    xdtf = xdtb.astype(F32)
    scores = mm_t(cmx, bm)
    causal = iota((TOK, TOK), 0) >= iota((TOK, TOK), 1)
    cumt = cum.T
    dscore = jnp.zeros((TOK, TOK), F32)
    ys, us = [], []
    for h in range(HEADS):
        cols = slice(h * HDIM, (h + 1) * HDIM)
        decay = jnp.exp(jnp.where(causal, cum[:, h : h + 1] - cumt[h : h + 1, :], -1e30))
        m = (decay * scores).astype(BF16)
        ys.append(mm(m, xdtb[:, cols]))
        us.append(t_mm(m, og[:, cols]))
        dscore = dscore + decay * mm_t(og[:, cols], xdtb[:, cols])
    dsb = dscore.astype(BF16)
    d_out, d_in = mm(dsb, bm), t_mm(dsb, cmx)
    yt, xt = (dy * ecum).astype(BF16), (xdt * etail).astype(BF16)
    gate_m = sz * (1.0 + zm * (1.0 - sz))
    si = jax.nn.sigmoid(zi)
    gate_i = si * (1.0 + zi * (1.0 - si))
    return (
        jnp.concatenate(ys, axis=1), jnp.concatenate(us, axis=1), d_out, d_in, yt, xt, gate_m,
        gate_i, bm, cmx, xdtf, dy, rate, exact(skp, ex), tot, ecum, etail, dte,
    )


def carried_phase(acts, local, st, ci, cm, gi_o, gm_o, ds_o, gmt_o):
    z, yh, c = (lax.axis_index(a) for a in SEQ)
    flag = jnp.where(z * 2 + yh == 0, 0.0, 1.0).astype(F32)
    hs = head_sum()
    xa, _, _, _, _, srb, _ = acts
    (
        y_loc, u_loc, d_out, d_in, yt, xt, gate_m, gate_i, bm, cmx, xdtf, dy, rate, skp, tot,
        ecum, etail, dte,
    ) = local
    keep = jnp.where(iota((EXT, 1), 0) < PRE, flag, 1.0)

    def collect(which):
        blocks = [st[2 * zz + which].astype(F32) for zz in range(NZ)]
        rows = [blocks[zz][h * 8 : h * 8 + 8] for h in range(HEADS) for zz in range(NZ)]
        return jnp.concatenate(rows, axis=0)

    def back(g, k):
        g = jnp.concatenate([jnp.zeros((PRE, g.shape[1]), F32), g], axis=0)
        return jnp.where(keep > 0.0, conv_back(g, k), 0.0).astype(BF16)

    h0, ge = collect(0), collect(1)
    h0b, geb = h0.astype(BF16), ge.astype(BF16)
    kept = []

    def inner():
        ug = etail * mm_t(bm, geb)
        u = u_loc + ug
        gi_o[...] = back((dte * u + skp * dy) * gate_i, half_of(ci[...], c))
        kept.extend((u, ug))

    def mixing():
        gm = jnp.concatenate([d_in + mm(xt, geb), d_out + mm(yt, h0b)], axis=1) * gate_m
        gm_o[...] = back(gm, cm[...])
        eye = one_hot(iota((TOK, TOK), 0) == iota((TOK, TOK), 1)).astype(BF16)
        gmt = t_mm(gm.astype(BF16), eye).astype(BF16)
        for j in range(8):
            gmt_o[j] = gmt[j * 32 : j * 32 + 32]

    def mixed(total):
        j8 = c * 4 + lax.axis_index("chan")
        place = one_hot(iota((32, 128), 1) == iota((32, 128), 0) + 64).astype(BF16)
        cols = one_hot(iota((2 * STATE, 128), 0) == j8 * 32 + iota((2 * STATE, 128), 1) - 64)
        lanes = iota((2 * STATE, 128), 1)
        cols = jnp.where((lanes >= 64) & (lanes < 96), cols, 0.0)
        return back(t_mm(total.astype(BF16), place), exact(cm[...], cols))

    def stepping():
        u, ug = kept
        y = y_loc + ecum * mm_t(cmx, h0b)
        ddt = exact(xa * u, hs)
        dcum = exact(dy * y - xdtf * u, hs)
        e_sum = jnp.sum(exact(xdtf * ug, hs), axis=0, keepdims=True)
        hg = exact(jnp.ones((8, STATE), F32), (h0 * ge).T)
        carry = jnp.exp(tot) * exact(hg, hs)[0:1]
        upper = one_hot(iota((TOK, TOK), 0) <= iota((TOK, TOK), 1))
        da = exact(upper, dcum) + e_sum + carry
        dsr = (ddt - rate * da) * jax.nn.sigmoid(srb)
        ds_o[...] = jnp.concatenate([jnp.zeros((PRE, 128), F32), dsr], axis=0).astype(BF16)

    return inner, mixing, mixed, stepping


def sums_phase(
    norm, later, xet, gi_r, gm_r, ds_r, gmt, wih, wm, ws,
    mt, fat, fb, ig, xin, pbin,
    mixin, rb, yhold, yin, ra, a3, a4, a1, a2, sa, ya, sb, b3, b4, b1, b2, fa, mrows, fbs, p, psib, xhold,
    pb, pbsib,
    ms, mr, ys, yr, zs, zr, qs, qr, xs, xr, es, er, as_, ar, ts, tr, dsem, drem,
):
    dp = lax.axis_index("dp")
    z, yh, c, x = (lax.axis_index(a) for a in SEQ_CHAN)
    y = yh * 2 + dp
    j8 = c * 4 + x
    sib = 1 - c
    q = z * 2 + yh
    nq, pq = lax.rem(q + 1, 2 * NZ), lax.rem(q + 2 * NZ - 1, 2 * NZ)
    def at_z(off):
        return {"seq_0": lax.rem(z + off + NZ, NZ)}

    def at_y(off):
        k = lax.rem(y + off + 4, 4)
        return {"seq_1": k // 2, "dp": lax.rem(k, 2)}

    def at_x(off):
        return {"chan": lax.rem(x + off + 4, 4)}

    def at_j(k):
        return {"seq_2": k // 4, "chan": lax.rem(k, 4)}

    def remote(src, dst, ss, rs, where):
        return pltpu.make_async_remote_copy(
            src_ref=src, dst_ref=dst, send_sem=ss, recv_sem=rs, device_id=where,
            device_id_type=MESH,
        )

    pending = []

    def go(d):
        d.start()
        pending.append(d)
        return d

    def send_mix():
        for off in range(1, 8):
            to = lax.rem(j8 + off, 8)
            go(remote(gmt.at[to], mixin.at[off], ms.at[off], mr.at[off], at_j(to)))

    inner, mixing, mixed, stepping = later
    mixing()
    send_mix()
    inner()

    gi = gi_r[...]
    rhs = gi[:, :256]

    def inner_rows(side, zhi):
        base = pl.multiple_of(side * 1280 + zhi * 640, 128)
        r = (mm(xet[pl.ds(base, 640), :], rhs) * norm).astype(BF16)
        for g in range(8):
            for k in range(2):
                rb[k, (g % 2) * 2 + side, zhi * 4 + g // 2] = r[
                    g * ROWS : (g + 1) * ROWS, k * 128 : (k + 1) * 128
                ]

    up, down, far = lax.rem(y + 1, 4), lax.rem(y + 3, 4), lax.rem(y + 2, 4)
    lo, hi = pl.ds(0, 4), pl.ds(4, 4)

    def hold(k, sign):
        i = 0 if sign == 1 else 1
        part = lo if sign == 1 else hi
        return remote(
            rb.at[k, far, part], yhold.at[k, i], ys.at[6 * k + i], yr.at[6 * k + i], at_y(sign)
        )

    def plain(k, sign):
        i = 0 if sign == 1 else 1
        to, part = (up, hi) if sign == 1 else (down, lo)
        return remote(
            rb.at[k, to, part], yin.at[k, i, part], ys.at[6 * k + 2 + i], yr.at[6 * k + 2 + i],
            at_y(sign),
        )

    def second(k, sign):
        i = 0 if sign == 1 else 1
        part = lo if sign == 1 else hi
        return remote(
            yhold.at[k, i], yin.at[k, i, part], ys.at[6 * k + 4 + i], yr.at[6 * k + 4 + i],
            at_y(sign),
        )

    def ring_on(k):
        for sign, to, first in ((1, up, 0), (-1, down, 4)):
            i = 0 if sign == 1 else 1
            hold(k, sign).wait_recv()
            for e in range(4):
                v = rb[k, to, first + e].astype(F32) + yhold[k, i, e].astype(F32)
                yhold[k, i, e] = v.astype(BF16)
            go(second(k, sign))

    def ring_end(k):
        for sign in (1, -1):
            plain(k, sign).wait_recv()
            second(k, sign).wait_recv()
        for e in range(NZ):
            v = rb[k, y, e].astype(F32) + yin[k, 0, e].astype(F32) + yin[k, 1, e].astype(F32)
            v = v.astype(BF16)
            sb[k, e, 0] = v[:40]
            sb[k, e, 1] = v[40:]

    inner_rows(dp, 0)
    go(hold(0, 1))
    inner_rows(dp, 1)
    go(hold(0, -1))
    inner_rows(1 - dp, 1)
    go(plain(0, 1))
    inner_rows(1 - dp, 0)
    go(plain(0, -1))
    go(hold(1, 1))
    go(hold(1, -1))
    stepping()
    ds = ds_r[...]

    total = gmt[j8].astype(F32)
    for off in range(1, 8):
        origin = lax.rem(j8 + 8 - off, 8)
        remote(gmt.at[origin], mixin.at[off], ms.at[off], mr.at[off], at_j(origin)).wait_recv()
        total = total + mixin[off].astype(F32)
    place_step = one_hot(
        (iota((128, 128), 1) == iota((128, 128), 0) + 96) & (iota((128, 128), 0) < HEADS)
    ).astype(BF16)
    last = mixed(total).astype(F32) + mm(ds, place_step)
    last = last + jnp.concatenate([gi[:, 256:].astype(F32), jnp.zeros((EXT, 64), F32)], axis=1)
    last = last.astype(BF16)
    for b in range(4):
        r = (mm(xet[b * 640 : (b + 1) * 640, :], last) * norm).astype(BF16)
        for g in range(8):
            ra[(b % 2) * 4 + g // 2, (g % 2) * 2 + b // 2] = r[g * ROWS : (g + 1) * ROWS]

    def z_first(src, n, r3, r4, r1, s, r, o=0):
        h = n // 2
        for k, sign in enumerate((1, -1)):
            part = pl.ds(k * h, h)
            dst = [lax.rem(z + sign * d + NZ, NZ) for d in range(5)]
            go(remote(src.at[dst[4], part], r4.at[k], s.at[o + 4 * k], r.at[o + 4 * k], at_z(2 * sign)))
            go(remote(src.at[dst[3]], r3.at[k], s.at[o + 4 * k + 1], r.at[o + 4 * k + 1], at_z(sign)))
            go(remote(src.at[dst[1]], r1.at[k], s.at[o + 4 * k + 2], r.at[o + 4 * k + 2], at_z(sign)))

    def z_second(src, n, r3, r4, r2, s, r, o=0):
        h = n // 2
        for k, sign in enumerate((1, -1)):
            part = pl.ds(k * h, h)
            t = lax.rem(z + 2 * sign + NZ, NZ)
            remote(r3.at[k], r3.at[k], s.at[o + 4 * k + 1], r.at[o + 4 * k + 1], at_z(sign)).wait_recv()
            remote(r4.at[k], r4.at[k], s.at[o + 4 * k], r.at[o + 4 * k], at_z(2 * sign)).wait_recv()
            for i in range(n):
                v = src[t, i].astype(F32) + r3[k, i].astype(F32)
                if k * h <= i < (k + 1) * h:
                    v = v + r4[k, i - k * h].astype(F32)
                r3[k, i] = v.astype(BF16)
            go(remote(r3.at[k], r2.at[k], s.at[o + 4 * k + 3], r.at[o + 4 * k + 3], at_z(2 * sign)))

    def z_last(r1, r2, s, r, o=0):
        for k, sign in enumerate((1, -1)):
            remote(r1.at[k], r1.at[k], s.at[o + 4 * k + 2], r.at[o + 4 * k + 2], at_z(sign)).wait_recv()
            remote(r2.at[k], r2.at[k], s.at[o + 4 * k + 3], r.at[o + 4 * k + 3], at_z(2 * sign)).wait_recv()

    z_first(ra, 4, a3, a4, a1, zs, zr)

    ring_on(0)
    go(plain(1, 1))
    go(plain(1, -1))

    pick = head_pick(c).astype(BF16)
    ds10 = mm_t(ds, pick).astype(BF16)
    gm = gm_r[...]
    for b in range(4):
        rows = slice(b * 640, (b + 1) * 640)
        part = mm_t(gi, wih[rows]) + mm_t(gm, wm[rows]) + mm(ds10, ws[:, rows])
        part = part.astype(BF16)
        pb[:, rows] = part[:PRE]
        for j in range(8):
            for k in range(2):
                at = PRE + j * 32 + k * 16
                p[j // 4, j % 4, k, :, rows] = part[at : at + 16]
    go(remote(p.at[sib], psib, dsem.at[0], drem.at[0], {"seq_2": sib}))
    pb_out = remote(pb, pbsib, dsem.at[1], drem.at[1], {"seq_2": sib})

    @pl.when(c == 0)
    def _():
        pb_out.start()

    ring_on(1)

    remote(psib, psib, dsem.at[0], drem.at[0], {"seq_2": sib}).wait_recv()
    for k in range(4):
        for h in range(2):
            psib[k, h] = (p[c, k, h].astype(F32) + psib[k, h].astype(F32)).astype(BF16)
    xu, xd, xf = lax.rem(x + 1, 4), lax.rem(x + 3, 4), lax.rem(x + 2, 4)
    go(remote(psib.at[xf, 0], xhold.at[0], xs.at[0], xr.at[0], at_x(1)))
    go(remote(psib.at[xf, 1], xhold.at[1], xs.at[1], xr.at[1], at_x(-1)))
    go(remote(psib.at[xu, 1], xin.at[0, 1], xs.at[2], xr.at[2], at_x(1)))
    go(remote(psib.at[xd, 0], xin.at[1, 0], xs.at[3], xr.at[3], at_x(-1)))
    edge = remote(
        pbsib, pbin.at[x], es, er.at[x],
        {"seq_0": pq // 2, "seq_1": lax.rem(pq, 2), "chan": 3},
    )

    @pl.when(c == 1)
    def _():
        pb_out.wait_recv()
        pbsib[...] = (pb[...].astype(F32) + pbsib[...].astype(F32)).astype(BF16)
        edge.start()

    z_second(ra, 4, a3, a4, a2, zs, zr)
    ring_end(0)
    z_first(sb.at[0], 2, b3.at[0], b4.at[0], b1.at[0], qs, qr)
    ring_end(1)
    z_first(sb.at[1], 2, b3.at[1], b4.at[1], b1.at[1], qs, qr, 8)
    z_second(sb.at[0], 2, b3.at[0], b4.at[0], b2.at[0], qs, qr)

    z_last(a1, a2, zs, zr)
    for i in range(4):
        v = ra[z, i].astype(F32)
        for k in range(2):
            v = v + a1[k, i].astype(F32) + a2[k, i].astype(F32)
        sa[i] = v.astype(BF16)
    for off in (2, 1, 3):
        to = lax.rem(y + off, 4)
        go(remote(sa.at[to], ya.at[off], as_.at[off], ar.at[off], at_y(off)))

    remote(xhold.at[0], xhold.at[0], xs.at[0], xr.at[0], at_x(1)).wait_recv()
    xhold[0] = (psib[xu, 0].astype(F32) + xhold[0].astype(F32)).astype(BF16)
    go(remote(xhold.at[0], xin.at[0, 0], xs.at[4], xr.at[4], at_x(1)))
    remote(xhold.at[1], xhold.at[1], xs.at[1], xr.at[1], at_x(-1)).wait_recv()
    xhold[1] = (psib[xd, 1].astype(F32) + xhold[1].astype(F32)).astype(BF16)
    go(remote(xhold.at[1], xin.at[1, 1], xs.at[5], xr.at[5], at_x(-1)))

    z_second(sb.at[1], 2, b3.at[1], b4.at[1], b2.at[1], qs, qr, 8)

    v = sa[y].astype(F32)
    for off in range(1, 4):
        remote(ya.at[off], ya.at[off], as_.at[off], ar.at[off], at_y(off)).wait_recv()
        v = v + ya[off].astype(F32)
    fa[0] = v[:40]
    fa[1] = v[40:]
    go(remote(fa.at[sib], fat.at[c], ts.at[0], tr.at[0], {"seq_2": sib}))
    line = iota((128, 80), 0)
    wanted = (line // 64) * 40 + (lax.rem(line // 16, 4)) * 10 + lax.rem(line, 16)
    chosen = exact(one_hot((iota((128, 80), 1) == wanted) & (lax.rem(line, 16) < 10)), v)
    for j in range(8):
        mrows[j] = chosen[j * 16 : (j + 1) * 16]
    for off in range(1, 8):
        to = lax.rem(j8 + off, 8)
        go(remote(mrows.at[to], mt.at[j8], ts.at[off], tr.at[off], at_j(to)))
    fat[c] = fa[c]
    mt[j8] = mrows[j8]

    for k, half in ((2, 1), (4, 0)):
        remote(xin.at[0, half], xin.at[0, half], xs.at[k], xr.at[k], at_x(1)).wait_recv()
    for k, half in ((3, 0), (5, 1)):
        remote(xin.at[1, half], xin.at[1, half], xs.at[k], xr.at[k], at_x(-1)).wait_recv()
    for h in range(2):
        v = psib[x, h].astype(F32) + xin[0, h].astype(F32) + xin[1, h].astype(F32)
        ig[h * 16 : (h + 1) * 16, :] = v.astype(BF16)

    @pl.when((c == 1) & (x == 3))
    def _():
        v = psib[x, 1].astype(F32) + xin[0, 1].astype(F32) + xin[1, 1].astype(F32)
        for k in range(4):
            remote(pbsib, pbin.at[k], es, er.at[k], {"chan": 0}).wait_recv()
            v = v + pbin[k].astype(F32)
        ig[16:, :] = v.astype(BF16)

    for t in range(2):
        z_last(b1.at[t], b2.at[t], qs, qr, 8 * t)
        for i in range(2):
            v = sb[t, z, i].astype(F32)
            for k in range(2):
                v = v + b1[t, k, i].astype(F32) + b2[t, k, i].astype(F32)
            fbs[i, :, t * 128 : (t + 1) * 128] = v
    go(remote(fbs.at[sib], fb.at[c], dsem.at[2], drem.at[2], {"seq_2": sib}))
    fb[c] = fbs[c]

    for off in range(1, 8):
        origin = lax.rem(j8 + 8 - off, 8)
        remote(mrows.at[0], mt.at[origin], ts.at[off], tr.at[off], at_j(origin)).wait_recv()
    remote(fa.at[c], fat.at[sib], ts.at[0], tr.at[0], {"seq_2": sib}).wait_recv()

    remote(fbs.at[c], fb.at[sib], dsem.at[2], drem.at[2], {"seq_2": sib}).wait_recv()
    for d in pending:
        d.wait_send()

    @pl.when(c == 0)
    def _():
        pb_out.wait_send()

    @pl.when(c == 1)
    def _():
        edge.wait_send()


def whole_kernel(
    norm,
    piece, og, wi_h, wm_h, ws_h, ci_h, cm_h, bias_h, dlog_h, skip_h,
    mt, fat, fb, ig,
    xe, ogx, wi, wm, ws, ci, cm, bias, dlog, skip, wih, send, recv, back, st, gi, gm, ds, gmt, xet,
    gs, gr, gt, hsem, lsem, s1, r1, s2, r2, *rest,
):
    dp = lax.axis_index("dp")
    z, yh, c, x = (lax.axis_index(a) for a in SEQ_CHAN)
    n = 2 * NZ
    q = z * 2 + yh
    nq, pq = lax.rem(q + 1, n), lax.rem(q + n - 1, n)
    corner = (c == 1) & (x == 3)
    barrier = pltpu.get_barrier_semaphore()

    def tell(**where):
        pl.semaphore_signal(barrier, inc=1, device_id=where, device_id_type=MESH)

    for off in range(1, 8):
        k = lax.rem(c * 4 + x + off, 8)
        tell(seq_2=k // 4, chan=lax.rem(k, 4))
    for off in (1, 3):
        k = lax.rem(yh * 2 + dp + off, 4)
        tell(seq_1=k // 2, dp=lax.rem(k, 2))
    for off in range(1, n):
        k = lax.rem(q + off, n)
        tell(seq_0=k // 2, seq_1=lax.rem(k, 2))

    @pl.when(c == 1)
    def _():
        tell(seq_0=pq // 2, seq_1=lax.rem(pq, 2), chan=3)

    @pl.when(corner)
    def _():
        for k in range(4):
            tell(seq_0=nq // 2, seq_1=lax.rem(nq, 2), chan=k)

    base = pl.multiple_of(PRE + (c * 4 + x) * 32, 16)
    loads = [pltpu.make_async_copy(piece, xe.at[pl.ds(base, 32), :], hsem.at[0])]
    loads.append(pltpu.make_async_copy(og, ogx.at[c], hsem.at[1]))
    pairs = ((wi_h, wi), (wm_h, wm), (ws_h, ws), (ci_h, ci), (cm_h, cm))
    pairs += ((bias_h, bias), (dlog_h, dlog), (skip_h, skip))
    for k, (src, dst) in enumerate(pairs):
        loads.append(pltpu.make_async_copy(src, dst, hsem.at[2 + k]))
    for d in loads:
        d.start()
    loads[0].wait()
    loads[1].wait()
    pl.semaphore_wait(
        barrier, jnp.where(corner, 7 + 2 + n - 1 + 5, jnp.where(c == 1, 7 + 2 + n, 7 + 2 + n - 1))
    )
    gather_phase(xe, ogx, gs, gr, gt)
    for d in loads[2:]:
        d.wait()
    acts = forward_phase(xe, ogx, wi, wm, ws, ci, cm, bias, dlog, wih, send)
    begin, turn, end = state_phases(send, st, recv, back, lsem, s1, r1, s2, r2)
    begin()
    local = local_phase(acts, dlog, skip)
    turn()
    for b in range(4):
        cols = slice(b * 640, (b + 1) * 640)
        xet[cols, :] = xe[:, cols].T
    end()
    later = carried_phase(acts, local, st, ci, cm, gi, gm, ds, gmt)
    sums_phase(
        norm, later, xet, gi, gm, ds, gmt, wih, wm, ws, mt, fat, fb, ig, *rest
    )


def whole(norm, *args):
    dma = pltpu.SemaphoreType.DMA
    n = 2 * NZ

    def vm(*shape):
        return pltpu.VMEM(shape, BF16)

    return pl.pallas_call(
        functools.partial(whole_kernel, norm),
        out_shape=(
            jax.ShapeDtypeStruct((8, 16, 128), F32),
            jax.ShapeDtypeStruct((2, 40, 128), F32),
            jax.ShapeDtypeStruct((2, 40, 256), F32),
            jax.ShapeDtypeStruct((32, D), BF16),
        ),
        in_specs=[pl.BlockSpec(memory_space=pltpu.HBM)] * 10,
        out_specs=(VM,) * 4,
        scratch_shapes=[
            vm(EXT, D), vm(2, TOK // 2, 2 * INNER), vm(D, 2 * INNER), vm(D, 2 * STATE), vm(10, D),
            pltpu.VMEM((4, 2 * INNER), F32), pltpu.VMEM((4, 2 * STATE), F32),
            pltpu.VMEM((1, 10), F32), pltpu.VMEM((1, 10), F32), pltpu.VMEM((1, 10), F32),
            vm(D, INNER), vm(n, CHUNK, STATE), vm(n, CHUNK, STATE), vm(n, 8 * HEADS, STATE),
            vm(n, 8 * HEADS, STATE), vm(EXT, INNER), vm(EXT, 2 * STATE), vm(EXT, 128), vm(8, 32, TOK),
            vm(D, EXT),
            dma((13,)), dma((13,)), dma((4,)), dma((10,)), dma((2,)),
            dma((n,)), dma((n,)), dma((n,)), dma((n,)),
            vm(2, 2, 16, D), vm(4, PRE, D), vm(8, 32, TOK),
            vm(2, 4, NZ, ROWS, 128), vm(2, 2, 4, ROWS, 128), vm(2, 2, NZ, ROWS, 128),
            vm(NZ, 4, ROWS, 128), vm(2, 4, ROWS, 128), vm(2, 2, ROWS, 128),
            vm(2, 4, ROWS, 128), vm(2, 4, ROWS, 128), vm(4, ROWS, 128), vm(4, ROWS, 128),
            vm(2, NZ, 2, 40, 128), vm(2, 2, 2, 40, 128), vm(2, 2, 1, 40, 128),
            vm(2, 2, 2, 40, 128), vm(2, 2, 2, 40, 128),
            pltpu.VMEM((2, 40, 128), F32), pltpu.VMEM((8, 16, 128), F32),
            pltpu.VMEM((2, 40, 256), F32),
            vm(2, 4, 2, 16, D), vm(4, 2, 16, D), vm(2, 16, D), vm(PRE, D), vm(PRE, D),
            dma((8,)), dma((8,)), dma((12,)), dma((12,)), dma((8,)), dma((8,)),
            dma((16,)), dma((16,)), dma((6,)), dma((6,)), dma(()), dma((4,)), dma((4,)), dma((4,)),
            dma((8,)), dma((8,)), dma((3,)), dma((3,)),
        ],
        compiler_params=pltpu.CompilerParams(
            collective_id=0, has_side_effects=True, vmem_limit_bytes=LIMIT
        ),
        name="whole",
    )(*args)


def finish_kernel(mt, fat, fb, ig, ig_o, iw_o, mw_o, sw_o):
    pick = one_hot(iota((HEADS, 128), 1) == iota((HEADS, 128), 0) + 96)
    for k in range(2):
        iw_o[:, k * INNER : k * INNER + 256] = fb[k]
        own = fat[k]
        iw_o[:, k * INNER + 256 : (k + 1) * INNER] = own[:, :64]
        sw_o[k * HEADS : (k + 1) * HEADS, :] = lax.dot_general(
            pick, own, (((1,), (1,)), ((), ())), preferred_element_type=F32,
            precision=lax.Precision.HIGHEST,
        )
    for j in range(8):
        mw_o[:, j * 32 : (j + 1) * 32] = mt[j, :10, 64:96]
    ig_o[...] = ig[...]


def finish(*args):
    return pl.pallas_call(
        finish_kernel,
        out_shape=(
            jax.ShapeDtypeStruct((32, D), BF16),
            jax.ShapeDtypeStruct((40, 2 * INNER), F32),
            jax.ShapeDtypeStruct((10, 2 * STATE), F32),
            jax.ShapeDtypeStruct((2 * HEADS, 40), F32),
        ),
        in_specs=[VM] * 4,
        out_specs=(VM,) * 4,
        compiler_params=pltpu.CompilerParams(vmem_limit_bytes=LIMIT),
        name="finish",
    )(*args)


def body(
    layer_input,
    inner_weight,
    mixer_weight,
    step_weight,
    conv_inner,
    conv_mixer,
    step_bias,
    decay_log,
    skip_gain,
    output_grad,
):
    norm = 1.0 / math.sqrt(8192)
    stepw = step_weight.T
    bias, dlog, skip = (v.reshape(1, -1) for v in (step_bias, decay_log, skip_gain))
    parts = whole(
        norm, layer_input[0], output_grad[0], inner_weight, mixer_weight, stepw, conv_inner,
        conv_mixer, bias, dlog, skip,
    )
    ig, iw, mw, sw = finish(*parts)
    return ig[None], iw, mw, sw.T


def solution(mesh):
    split = Mesh(
        mesh.devices.reshape(mesh.shape["dp"], 8, 2, 2, mesh.shape["chan"]),
        ("dp", "seq_0", "seq_1", "seq_2", "chan"),
    )
    placed = (
        P("dp", SEQ_CHAN, None),
        P(None, "chan"),
        P(),
        P(None, "chan"),
        P(None, "chan"),
        P(),
        P("chan"),
        P("chan"),
        P("chan"),
        P("dp", SEQ, "chan"),
    )
    return jax.shard_map(
        body,
        mesh=split,
        in_specs=placed,
        out_specs=(
            P("dp", SEQ_CHAN, None),
            P(DP_SEQ, "chan"),
            P(DP_SEQ_CHAN, None),
            P(DP_SEQ, "chan"),
        ),
        check_vma=False,
    )
```

```python
import functools
import math

import jax
import jax.numpy as jnp
from jax import lax
from jax.experimental import pallas as pl
from jax.experimental.pallas import tpu as pltpu
from jax.sharding import Mesh
from jax.sharding import PartitionSpec as P

D = 2560
HDIM = 64
HEADS = 5
INNER = HEADS * HDIM
STATE = 128
TOK = 256
PRE = 16
EXT = TOK + PRE
NZ = 8
ROWS = 80
CHUNK = 48
F32 = jnp.float32
BF16 = jnp.bfloat16
SEQ = ("seq_0", "seq_1", "seq_2")
DP_SEQ = ("dp", "seq_0", "seq_1", "seq_2")
SEQ_CHAN = ("seq_0", "seq_1", "seq_2", "chan")
DP_SEQ_CHAN = ("dp", "seq_0", "seq_1", "seq_2", "chan")
MESH = pl.DeviceIdType.MESH
VM = pl.BlockSpec(memory_space=pltpu.VMEM)
LIMIT = 62 * 1024 * 1024


def roll(v, shift):
    return pltpu.roll(v, shift % v.shape[0], 0)


def mm(a, b):
    return jnp.dot(a, b, preferred_element_type=F32)


def mm_t(a, b):
    return lax.dot_general(a, b, (((1,), (1,)), ((), ())), preferred_element_type=F32)


def t_mm(a, b):
    return lax.dot_general(a, b, (((0,), (0,)), ((), ())), preferred_element_type=F32)


def exact(a, b):
    return jnp.dot(a, b, preferred_element_type=F32, precision=lax.Precision.HIGHEST)


def iota(shape, dim):
    return lax.broadcasted_iota(jnp.int32, shape, dim)


def one_hot(cond):
    return jnp.where(cond, 1.0, 0.0).astype(F32)


def head_expand():
    return one_hot(iota((128, INNER), 1) // HDIM == iota((128, INNER), 0))


def head_sum():
    return one_hot(iota((INNER, 128), 0) // HDIM == iota((INNER, 128), 1))


def head_pick(core):
    return one_hot(
        (iota((10, 128), 0) == iota((10, 128), 1) + HEADS * core) & (iota((10, 128), 1) < HEADS)
    )


def half_of(v, core):
    return jnp.where(core == 0, v[:, :INNER], v[:, INNER:])


def conv(v, k):
    return k[3:4] * v + k[2:3] * roll(v, 1) + k[1:2] * roll(v, 2) + k[0:1] * roll(v, 3)


def conv_back(g, k):
    return k[3:4] * g + k[2:3] * roll(g, -1) + k[1:2] * roll(g, -2) + k[0:1] * roll(g, -3)


def gather_phase(xe, ogx, ssem, rsem, tsem):
    z, yh, c, x = (lax.axis_index(a) for a in SEQ_CHAN)
    right, left = lax.rem(x + 1, 4), lax.rem(x + 3, 4)
    sib = 1 - c
    q = z * 2 + yh
    nq, pq = lax.rem(q + 1, 2 * NZ), lax.rem(q + 2 * NZ - 1, 2 * NZ)
    def slot(core, chan, half=None):
        base = PRE + (core * 4 + chan) * 32
        if half is None:
            return xe.at[pl.ds(pl.multiple_of(base, 16), 32), :]
        return xe.at[pl.ds(pl.multiple_of(base + 16 * half, 16), 16), :]

    def copy(src, dst, k, **where):
        return pltpu.make_async_remote_copy(
            src_ref=src, dst_ref=dst, send_sem=ssem.at[k], recv_sem=rsem.at[k],
            device_id=where, device_id_type=MESH,
        )

    mine = slot(c, x)
    own_og = ogx.at[c]

    def half(h):
        return slot(c, x, h)

    r0 = copy(half(0), slot(c, x, 0), 0, chan=right)
    l1 = copy(half(1), slot(c, x, 1), 1, chan=left)
    r1 = copy(half(1), slot(c, x, 1), 2, chan=right)
    l0 = copy(half(0), slot(c, x, 0), 3, chan=left)
    sp = copy(mine, mine, 4, seq_2=sib)
    so = copy(own_og, own_og, 5, seq_2=sib)
    for d in (r0, l1):
        d.start()

    def tails(chan):
        return pltpu.make_async_remote_copy(
            src_ref=half(1), dst_ref=xe.at[pl.ds(0, 16), :], send_sem=tsem.at[chan],
            recv_sem=rsem.at[6],
            device_id={"seq_0": nq // 2, "seq_1": lax.rem(nq, 2), "chan": chan},
            device_id_type=MESH,
        )

    @pl.when((c == 1) & (x == 3))
    def _():
        for chan in range(4):
            tails(chan).start()

    for d in (r1, l0, sp, so):
        d.start()
    far = lax.rem(x + 2, 4)
    in_r0 = copy(half(0), slot(c, left, 0), 0, chan=right)
    in_r1 = copy(half(1), slot(c, left, 1), 2, chan=right)
    in_l1 = copy(half(1), slot(c, right, 1), 1, chan=left)
    in_l0 = copy(half(0), slot(c, right, 0), 3, chan=left)
    rr = copy(slot(c, left, 0), slot(c, left, 0), 7, chan=right)
    ll = copy(slot(c, right, 1), slot(c, right, 1), 8, chan=left)
    in_r0.wait_recv()
    rr.start()
    in_l1.wait_recv()
    ll.start()
    in_r1.wait_recv()
    s_left = copy(slot(c, left), slot(c, left), 9, seq_2=sib)
    s_left.start()
    in_l0.wait_recv()
    s_right = copy(slot(c, right), slot(c, right), 10, seq_2=sib)
    s_right.start()
    tail_on = copy(xe.at[pl.ds(0, 16), :], xe.at[pl.ds(0, 16), :], 12, seq_2=sib)

    @pl.when(c == 1)
    def _():
        tails(0).wait_recv()
        tail_on.start()

    in_rr = copy(half(0), slot(c, far, 0), 7, chan=right)
    in_ll = copy(half(1), slot(c, far, 1), 8, chan=left)
    in_rr.wait_recv()
    in_ll.wait_recv()
    s_far = copy(slot(c, far), slot(c, far), 11, seq_2=sib)
    s_far.start()
    copy(mine, slot(sib, x), 4, seq_2=sib).wait_recv()
    copy(own_og, ogx.at[sib], 5, seq_2=sib).wait_recv()
    copy(mine, slot(sib, left), 9, seq_2=sib).wait_recv()
    copy(mine, slot(sib, right), 10, seq_2=sib).wait_recv()
    copy(mine, slot(sib, far), 11, seq_2=sib).wait_recv()

    @pl.when(c == 0)
    def _():
        tail_on.wait_recv()

    for d in (r0, l1, r1, l0, sp, so, rr, ll, s_left, s_right, s_far):
        d.wait_send()

    @pl.when(c == 1)
    def _():
        tail_on.wait_send()

    @pl.when((c == 1) & (x == 3))
    def _():
        for chan in range(4):
            tails(chan).wait_send()


def forward_phase(xe, ogx, wi, wm, ws, ci, cm, bias, dlog, wih_o, send_o):
    z, yh, c = (lax.axis_index(a) for a in SEQ)
    flag = jnp.where(z * 2 + yh == 0, 0.0, 1.0).astype(F32)
    pick = head_pick(c)
    wih = half_of(wi[...], c)
    wih_o[...] = wih
    xv = xe[...]
    keep = jnp.where(iota((EXT, 1), 0) < PRE, flag, 1.0)

    def masked(v):
        return jnp.where(keep > 0.0, v.astype(BF16).astype(F32), 0.0)

    pi = masked(mm(xv, wih))
    pm = masked(mm(xv, wm[...]))
    sr = exact(mm_t(xv, ws[...])[PRE:], pick)
    zi = conv(pi, half_of(ci[...], c))[PRE:]
    zm = conv(pm, cm[...])[PRE:]
    xa = zi * jax.nn.sigmoid(zi)
    ma = zm * jax.nn.sigmoid(zm)
    srb = sr + exact(bias[...], pick)
    dt = jnp.maximum(srb, 0.0) + jnp.log1p(jnp.exp(-jnp.abs(srb)))
    rate = exact(jnp.exp(dlog[...]), pick)
    a = -dt * rate
    tri = one_hot(iota((TOK, TOK), 0) >= iota((TOK, TOK), 1))
    cum = exact(tri, a)
    tot = cum[TOK - 1 : TOK]
    og = half_of(ogx[...].reshape(TOK, 2 * INNER), c)
    ex = head_expand()
    xt = (xa * exact(dt * jnp.exp(tot - cum), ex)).astype(BF16)
    yt = (og.astype(F32) * exact(jnp.exp(cum), ex)).astype(BF16)
    f_loc = t_mm(xt, ma[:, :STATE].astype(BF16))
    g_loc = t_mm(yt, ma[:, STATE:].astype(BF16))
    diag = jnp.where(iota((8, 128), 0) == iota((8, 128), 1), tot, 0.0)
    dm = exact(diag, jnp.ones((128, 128), F32))
    hi = dm.astype(BF16).astype(F32)
    drow = jnp.where(iota((8, 128), 1) < 64, hi, dm - hi)
    for zz in range(NZ):
        for which, v in ((0, f_loc), (1, g_loc)):
            rows = [v[h * HDIM + zz * 8 : h * HDIM + zz * 8 + 8] for h in range(HEADS)]
            send_o[zz * 2 + which] = jnp.concatenate(rows + [drow], axis=0).astype(BF16)
    return xa, zi, zm, dt, cum, srb, og


def state_phases(send, out, recv, back, local_sem, s1, r1, s2, r2):
    z, yh = lax.axis_index("seq_0"), lax.axis_index("seq_1")
    n = 2 * NZ
    me = z * 2 + yh
    def at(q):
        return {"seq_0": q // 2, "seq_1": lax.rem(q, 2)}

    def push(src, dst, ss, rs, off):
        to = lax.rem(me + off, n)
        return pltpu.make_async_remote_copy(
            src_ref=src.at[to], dst_ref=dst.at[me], send_sem=ss.at[off], recv_sem=rs.at[off],
            device_id=at(to), device_id_type=MESH,
        )

    def pull(src, dst, ss, rs, off):
        origin = lax.rem(me + n - off, n)
        return pltpu.make_async_remote_copy(
            src_ref=src.at[origin], dst_ref=dst.at[origin], send_sem=ss.at[off],
            recv_sem=rs.at[off], device_id=at(origin), device_id_type=MESH,
        )

    order = sorted(range(1, n), key=lambda off: -min(off, n - off))
    first = [push(send, recv, s1, r1, off) for off in order]
    second = [push(back, out, s2, r2, off) for off in order]

    def begin():
        for d in first:
            d.start()
        own = pltpu.make_async_copy(send.at[me], recv.at[me], local_sem.at[0])
        own.start()
        own.wait()

    def turn():
        for off in range(1, n):
            pull(send, recv, s1, r1, off).wait_recv()
        run = jnp.zeros((HEADS * 8, STATE), F32)
        for j in range(n):
            k = jnp.where(yh == 0, j, n - 1 - j)
            got = recv[k].astype(F32)
            rows = got[HEADS * 8 :]
            rows = rows + pltpu.roll(rows, 64, 1)
            decay = jnp.exp(rows)
            back[k] = run.astype(BF16)
            wide = jnp.concatenate(
                [jnp.broadcast_to(decay[h : h + 1], (8, STATE)) for h in range(HEADS)], axis=0
            )
            run = wide * run + got[: HEADS * 8]
        for d in second:
            d.start()
        own = pltpu.make_async_copy(back.at[me], out.at[me], local_sem.at[1])
        own.start()
        own.wait()

    def end():
        for off in range(1, n):
            pull(back, out, s2, r2, off).wait_recv()
        for d in first + second:
            d.wait_send()

    return begin, turn, end


def local_phase(acts, dlog, skip):
    c = lax.axis_index("seq_2")
    pick = head_pick(c)
    ex = head_expand()
    xa, zi, zm, dt, cum, srb, og = acts
    dy = og.astype(F32)
    rate = exact(jnp.exp(dlog[...]), pick)
    skp = exact(skip[...], pick)
    tot = cum[TOK - 1 : TOK]
    ecum = exact(jnp.exp(cum), ex)
    etail = exact(jnp.exp(tot - cum), ex)
    dte = exact(dt, ex)
    sz = jax.nn.sigmoid(zm)
    ma = zm * sz
    bm, cmx = ma[:, :STATE].astype(BF16), ma[:, STATE:].astype(BF16)
    xdt = xa * dte
    xdtb = xdt.astype(BF16)
    xdtf = xdtb.astype(F32)
    scores = mm_t(cmx, bm)
    causal = iota((TOK, TOK), 0) >= iota((TOK, TOK), 1)
    cumt = cum.T
    dscore = jnp.zeros((TOK, TOK), F32)
    ys, us = [], []
    for h in range(HEADS):
        cols = slice(h * HDIM, (h + 1) * HDIM)
        decay = jnp.exp(jnp.where(causal, cum[:, h : h + 1] - cumt[h : h + 1, :], -1e30))
        m = (decay * scores).astype(BF16)
        ys.append(mm(m, xdtb[:, cols]))
        us.append(t_mm(m, og[:, cols]))
        dscore = dscore + decay * mm_t(og[:, cols], xdtb[:, cols])
    dsb = dscore.astype(BF16)
    d_out, d_in = mm(dsb, bm), t_mm(dsb, cmx)
    yt, xt = (dy * ecum).astype(BF16), (xdt * etail).astype(BF16)
    gate_m = sz * (1.0 + zm * (1.0 - sz))
    si = jax.nn.sigmoid(zi)
    gate_i = si * (1.0 + zi * (1.0 - si))
    return (
        jnp.concatenate(ys, axis=1), jnp.concatenate(us, axis=1), d_out, d_in, yt, xt, gate_m,
        gate_i, bm, cmx, xdtf, dy, rate, exact(skp, ex), tot, ecum, etail, dte,
    )


def carried_phase(acts, local, st, ci, cm, gi_o, gm_o, ds_o, gmt_o):
    z, yh, c = (lax.axis_index(a) for a in SEQ)
    flag = jnp.where(z * 2 + yh == 0, 0.0, 1.0).astype(F32)
    hs = head_sum()
    xa, _, _, _, _, srb, _ = acts
    (
        y_loc, u_loc, d_out, d_in, yt, xt, gate_m, gate_i, bm, cmx, xdtf, dy, rate, skp, tot,
        ecum, etail, dte,
    ) = local
    keep = jnp.where(iota((EXT, 1), 0) < PRE, flag, 1.0)

    def collect(which):
        blocks = [st[2 * zz + which].astype(F32) for zz in range(NZ)]
        rows = [blocks[zz][h * 8 : h * 8 + 8] for h in range(HEADS) for zz in range(NZ)]
        return jnp.concatenate(rows, axis=0)

    def back(g, k):
        g = jnp.concatenate([jnp.zeros((PRE, g.shape[1]), F32), g], axis=0)
        return jnp.where(keep > 0.0, conv_back(g, k), 0.0).astype(BF16)

    h0, ge = collect(0), collect(1)
    h0b, geb = h0.astype(BF16), ge.astype(BF16)
    kept = []

    def inner():
        ug = etail * mm_t(bm, geb)
        u = u_loc + ug
        gi_o[...] = back((dte * u + skp * dy) * gate_i, half_of(ci[...], c))
        kept.extend((u, ug))

    def mixing():
        gm = jnp.concatenate([d_in + mm(xt, geb), d_out + mm(yt, h0b)], axis=1) * gate_m
        gm_o[...] = back(gm, cm[...])
        eye = one_hot(iota((TOK, TOK), 0) == iota((TOK, TOK), 1)).astype(BF16)
        gmt = t_mm(gm.astype(BF16), eye).astype(BF16)
        for j in range(8):
            gmt_o[j] = gmt[j * 32 : j * 32 + 32]

    def mixed(total):
        j8 = c * 4 + lax.axis_index("chan")
        place = one_hot(iota((32, 128), 1) == iota((32, 128), 0) + 64).astype(BF16)
        cols = one_hot(iota((2 * STATE, 128), 0) == j8 * 32 + iota((2 * STATE, 128), 1) - 64)
        lanes = iota((2 * STATE, 128), 1)
        cols = jnp.where((lanes >= 64) & (lanes < 96), cols, 0.0)
        return back(t_mm(total.astype(BF16), place), exact(cm[...], cols))

    def stepping():
        u, ug = kept
        y = y_loc + ecum * mm_t(cmx, h0b)
        ddt = exact(xa * u, hs)
        dcum = exact(dy * y - xdtf * u, hs)
        e_sum = jnp.sum(exact(xdtf * ug, hs), axis=0, keepdims=True)
        hg = exact(jnp.ones((8, STATE), F32), (h0 * ge).T)
        carry = jnp.exp(tot) * exact(hg, hs)[0:1]
        upper = one_hot(iota((TOK, TOK), 0) <= iota((TOK, TOK), 1))
        da = exact(upper, dcum) + e_sum + carry
        dsr = (ddt - rate * da) * jax.nn.sigmoid(srb)
        ds_o[...] = jnp.concatenate([jnp.zeros((PRE, 128), F32), dsr], axis=0).astype(BF16)

    return inner, mixing, mixed, stepping


def sums_phase(
    norm, later, xet, gi_r, gm_r, ds_r, gmt, wih, wm, ws,
    mt, fat, fb, ig, xin, pbin,
    mixin, rb, yhold, yin, ra, a3, a4, a1, a2, sa, ya, sb, b3, b4, b1, b2, fa, mrows, fbs, p, psib, xhold,
    pb, pbsib,
    ms, mr, ys, yr, zs, zr, qs, qr, xs, xr, es, er, as_, ar, ts, tr, dsem, drem,
):
    dp = lax.axis_index("dp")
    z, yh, c, x = (lax.axis_index(a) for a in SEQ_CHAN)
    y = yh * 2 + dp
    j8 = c * 4 + x
    sib = 1 - c
    q = z * 2 + yh
    nq, pq = lax.rem(q + 1, 2 * NZ), lax.rem(q + 2 * NZ - 1, 2 * NZ)
    def at_z(off):
        return {"seq_0": lax.rem(z + off + NZ, NZ)}

    def at_y(off):
        k = lax.rem(y + off + 4, 4)
        return {"seq_1": k // 2, "dp": lax.rem(k, 2)}

    def at_x(off):
        return {"chan": lax.rem(x + off + 4, 4)}

    def at_j(k):
        return {"seq_2": k // 4, "chan": lax.rem(k, 4)}

    def remote(src, dst, ss, rs, where):
        return pltpu.make_async_remote_copy(
            src_ref=src, dst_ref=dst, send_sem=ss, recv_sem=rs, device_id=where,
            device_id_type=MESH,
        )

    pending = []

    def go(d):
        d.start()
        pending.append(d)
        return d

    def send_mix():
        for off in range(1, 8):
            to = lax.rem(j8 + off, 8)
            go(remote(gmt.at[to], mixin.at[off], ms.at[off], mr.at[off], at_j(to)))

    inner, mixing, mixed, stepping = later
    mixing()
    send_mix()
    inner()

    gi = gi_r[...]
    rhs = gi[:, :256]

    def inner_rows(side, zhi):
        base = pl.multiple_of(side * 1280 + zhi * 640, 128)
        r = (mm(xet[pl.ds(base, 640), :], rhs) * norm).astype(BF16)
        for g in range(8):
            for k in range(2):
                rb[k, (g % 2) * 2 + side, zhi * 4 + g // 2] = r[
                    g * ROWS : (g + 1) * ROWS, k * 128 : (k + 1) * 128
                ]

    up, down, far = lax.rem(y + 1, 4), lax.rem(y + 3, 4), lax.rem(y + 2, 4)
    lo, hi = pl.ds(0, 4), pl.ds(4, 4)

    def hold(k, sign):
        i = 0 if sign == 1 else 1
        part = lo if sign == 1 else hi
        return remote(
            rb.at[k, far, part], yhold.at[k, i], ys.at[6 * k + i], yr.at[6 * k + i], at_y(sign)
        )

    def plain(k, sign):
        i = 0 if sign == 1 else 1
        to, part = (up, hi) if sign == 1 else (down, lo)
        return remote(
            rb.at[k, to, part], yin.at[k, i, part], ys.at[6 * k + 2 + i], yr.at[6 * k + 2 + i],
            at_y(sign),
        )

    def second(k, sign):
        i = 0 if sign == 1 else 1
        part = lo if sign == 1 else hi
        return remote(
            yhold.at[k, i], yin.at[k, i, part], ys.at[6 * k + 4 + i], yr.at[6 * k + 4 + i],
            at_y(sign),
        )

    def ring_on(k):
        for sign, to, first in ((1, up, 0), (-1, down, 4)):
            i = 0 if sign == 1 else 1
            hold(k, sign).wait_recv()
            for e in range(4):
                v = rb[k, to, first + e].astype(F32) + yhold[k, i, e].astype(F32)
                yhold[k, i, e] = v.astype(BF16)
            go(second(k, sign))

    def ring_end(k):
        for sign in (1, -1):
            plain(k, sign).wait_recv()
            second(k, sign).wait_recv()
        for e in range(NZ):
            v = rb[k, y, e].astype(F32) + yin[k, 0, e].astype(F32) + yin[k, 1, e].astype(F32)
            v = v.astype(BF16)
            sb[k, e, 0] = v[:40]
            sb[k, e, 1] = v[40:]

    inner_rows(dp, 0)
    go(hold(0, 1))
    inner_rows(dp, 1)
    go(hold(0, -1))
    inner_rows(1 - dp, 1)
    go(plain(0, 1))
    inner_rows(1 - dp, 0)
    go(plain(0, -1))
    go(hold(1, 1))
    go(hold(1, -1))
    stepping()
    ds = ds_r[...]

    total = gmt[j8].astype(F32)
    for off in range(1, 8):
        origin = lax.rem(j8 + 8 - off, 8)
        remote(gmt.at[origin], mixin.at[off], ms.at[off], mr.at[off], at_j(origin)).wait_recv()
        total = total + mixin[off].astype(F32)
    place_step = one_hot(
        (iota((128, 128), 1) == iota((128, 128), 0) + 96) & (iota((128, 128), 0) < HEADS)
    ).astype(BF16)
    last = mixed(total).astype(F32) + mm(ds, place_step)
    last = last + jnp.concatenate([gi[:, 256:].astype(F32), jnp.zeros((EXT, 64), F32)], axis=1)
    last = last.astype(BF16)
    for b in range(4):
        r = (mm(xet[b * 640 : (b + 1) * 640, :], last) * norm).astype(BF16)
        for g in range(8):
            ra[(b % 2) * 4 + g // 2, (g % 2) * 2 + b // 2] = r[g * ROWS : (g + 1) * ROWS]

    def z_first(src, n, r3, r4, r1, s, r, o=0):
        h = n // 2
        for k, sign in enumerate((1, -1)):
            part = pl.ds(k * h, h)
            dst = [lax.rem(z + sign * d + NZ, NZ) for d in range(5)]
            go(remote(src.at[dst[4], part], r4.at[k], s.at[o + 4 * k], r.at[o + 4 * k], at_z(2 * sign)))
            go(remote(src.at[dst[3]], r3.at[k], s.at[o + 4 * k + 1], r.at[o + 4 * k + 1], at_z(sign)))
            go(remote(src.at[dst[1]], r1.at[k], s.at[o + 4 * k + 2], r.at[o + 4 * k + 2], at_z(sign)))

    def z_second(src, n, r3, r4, r2, s, r, o=0):
        h = n // 2
        for k, sign in enumerate((1, -1)):
            part = pl.ds(k * h, h)
            t = lax.rem(z + 2 * sign + NZ, NZ)
            remote(r3.at[k], r3.at[k], s.at[o + 4 * k + 1], r.at[o + 4 * k + 1], at_z(sign)).wait_recv()
            remote(r4.at[k], r4.at[k], s.at[o + 4 * k], r.at[o + 4 * k], at_z(2 * sign)).wait_recv()
            for i in range(n):
                v = src[t, i].astype(F32) + r3[k, i].astype(F32)
                if k * h <= i < (k + 1) * h:
                    v = v + r4[k, i - k * h].astype(F32)
                r3[k, i] = v.astype(BF16)
            go(remote(r3.at[k], r2.at[k], s.at[o + 4 * k + 3], r.at[o + 4 * k + 3], at_z(2 * sign)))

    def z_last(r1, r2, s, r, o=0):
        for k, sign in enumerate((1, -1)):
            remote(r1.at[k], r1.at[k], s.at[o + 4 * k + 2], r.at[o + 4 * k + 2], at_z(sign)).wait_recv()
            remote(r2.at[k], r2.at[k], s.at[o + 4 * k + 3], r.at[o + 4 * k + 3], at_z(2 * sign)).wait_recv()

    z_first(ra, 4, a3, a4, a1, zs, zr)

    ring_on(0)
    go(plain(1, 1))
    go(plain(1, -1))

    pick = head_pick(c).astype(BF16)
    ds10 = mm_t(ds, pick).astype(BF16)
    gm = gm_r[...]
    for b in range(4):
        rows = slice(b * 640, (b + 1) * 640)
        part = mm_t(gi, wih[rows]) + mm_t(gm, wm[rows]) + mm(ds10, ws[:, rows])
        part = part.astype(BF16)
        pb[:, rows] = part[:PRE]
        for j in range(8):
            for k in range(2):
                at = PRE + j * 32 + k * 16
                p[j // 4, j % 4, k, :, rows] = part[at : at + 16]
    go(remote(p.at[sib], psib, dsem.at[0], drem.at[0], {"seq_2": sib}))
    pb_out = remote(pb, pbsib, dsem.at[1], drem.at[1], {"seq_2": sib})

    @pl.when(c == 0)
    def _():
        pb_out.start()

    ring_on(1)

    z_second(ra, 4, a3, a4, a2, zs, zr)

    remote(psib, psib, dsem.at[0], drem.at[0], {"seq_2": sib}).wait_recv()
    for k in range(4):
        for h in range(2):
            psib[k, h] = (p[c, k, h].astype(F32) + psib[k, h].astype(F32)).astype(BF16)
    xu, xd, xf = lax.rem(x + 1, 4), lax.rem(x + 3, 4), lax.rem(x + 2, 4)
    go(remote(psib.at[xf, 0], xhold.at[0], xs.at[0], xr.at[0], at_x(1)))
    go(remote(psib.at[xf, 1], xhold.at[1], xs.at[1], xr.at[1], at_x(-1)))
    go(remote(psib.at[xu, 1], xin.at[0, 1], xs.at[2], xr.at[2], at_x(1)))
    go(remote(psib.at[xd, 0], xin.at[1, 0], xs.at[3], xr.at[3], at_x(-1)))
    edge = remote(
        pbsib, pbin.at[x], es, er.at[x],
        {"seq_0": pq // 2, "seq_1": lax.rem(pq, 2), "chan": 3},
    )

    @pl.when(c == 1)
    def _():
        pb_out.wait_recv()
        pbsib[...] = (pb[...].astype(F32) + pbsib[...].astype(F32)).astype(BF16)
        edge.start()

    ring_end(0)
    z_first(sb.at[0], 2, b3.at[0], b4.at[0], b1.at[0], qs, qr)
    ring_end(1)
    z_first(sb.at[1], 2, b3.at[1], b4.at[1], b1.at[1], qs, qr, 8)
    z_second(sb.at[0], 2, b3.at[0], b4.at[0], b2.at[0], qs, qr)

    z_last(a1, a2, zs, zr)
    for i in range(4):
        v = ra[z, i].astype(F32)
        for k in range(2):
            v = v + a1[k, i].astype(F32) + a2[k, i].astype(F32)
        sa[i] = v.astype(BF16)
    for off in (2, 1, 3):
        to = lax.rem(y + off, 4)
        go(remote(sa.at[to], ya.at[off], as_.at[off], ar.at[off], at_y(off)))

    remote(xhold.at[0], xhold.at[0], xs.at[0], xr.at[0], at_x(1)).wait_recv()
    xhold[0] = (psib[xu, 0].astype(F32) + xhold[0].astype(F32)).astype(BF16)
    go(remote(xhold.at[0], xin.at[0, 0], xs.at[4], xr.at[4], at_x(1)))
    remote(xhold.at[1], xhold.at[1], xs.at[1], xr.at[1], at_x(-1)).wait_recv()
    xhold[1] = (psib[xd, 1].astype(F32) + xhold[1].astype(F32)).astype(BF16)
    go(remote(xhold.at[1], xin.at[1, 1], xs.at[5], xr.at[5], at_x(-1)))

    z_second(sb.at[1], 2, b3.at[1], b4.at[1], b2.at[1], qs, qr, 8)

    v = sa[y].astype(F32)
    for off in range(1, 4):
        remote(ya.at[off], ya.at[off], as_.at[off], ar.at[off], at_y(off)).wait_recv()
        v = v + ya[off].astype(F32)
    fa[0] = v[:40]
    fa[1] = v[40:]
    go(remote(fa.at[sib], fat.at[c], ts.at[0], tr.at[0], {"seq_2": sib}))
    line = iota((128, 80), 0)
    wanted = (line // 64) * 40 + (lax.rem(line // 16, 4)) * 10 + lax.rem(line, 16)
    chosen = exact(one_hot((iota((128, 80), 1) == wanted) & (lax.rem(line, 16) < 10)), v)
    for j in range(8):
        mrows[j] = chosen[j * 16 : (j + 1) * 16]
    for off in range(1, 8):
        to = lax.rem(j8 + off, 8)
        go(remote(mrows.at[to], mt.at[j8], ts.at[off], tr.at[off], at_j(to)))
    fat[c] = fa[c]
    mt[j8] = mrows[j8]

    for k, half in ((2, 1), (4, 0)):
        remote(xin.at[0, half], xin.at[0, half], xs.at[k], xr.at[k], at_x(1)).wait_recv()
    for k, half in ((3, 0), (5, 1)):
        remote(xin.at[1, half], xin.at[1, half], xs.at[k], xr.at[k], at_x(-1)).wait_recv()
    for h in range(2):
        v = psib[x, h].astype(F32) + xin[0, h].astype(F32) + xin[1, h].astype(F32)
        ig[h * 16 : (h + 1) * 16, :] = v.astype(BF16)

    @pl.when((c == 1) & (x == 3))
    def _():
        v = psib[x, 1].astype(F32) + xin[0, 1].astype(F32) + xin[1, 1].astype(F32)
        for k in range(4):
            remote(pbsib, pbin.at[k], es, er.at[k], {"chan": 0}).wait_recv()
            v = v + pbin[k].astype(F32)
        ig[16:, :] = v.astype(BF16)

    for t in range(2):
        z_last(b1.at[t], b2.at[t], qs, qr, 8 * t)
        for i in range(2):
            v = sb[t, z, i].astype(F32)
            for k in range(2):
                v = v + b1[t, k, i].astype(F32) + b2[t, k, i].astype(F32)
            fbs[i, :, t * 128 : (t + 1) * 128] = v
    go(remote(fbs.at[sib], fb.at[c], dsem.at[2], drem.at[2], {"seq_2": sib}))
    fb[c] = fbs[c]

    for off in range(1, 8):
        origin = lax.rem(j8 + 8 - off, 8)
        remote(mrows.at[0], mt.at[origin], ts.at[off], tr.at[off], at_j(origin)).wait_recv()
    remote(fa.at[c], fat.at[sib], ts.at[0], tr.at[0], {"seq_2": sib}).wait_recv()

    remote(fbs.at[c], fb.at[sib], dsem.at[2], drem.at[2], {"seq_2": sib}).wait_recv()
    for d in pending:
        d.wait_send()

    @pl.when(c == 0)
    def _():
        pb_out.wait_send()

    @pl.when(c == 1)
    def _():
        edge.wait_send()


def whole_kernel(
    norm,
    piece, og, wi_h, wm_h, ws_h, ci_h, cm_h, bias_h, dlog_h, skip_h,
    mt, fat, fb, ig,
    xe, ogx, wi, wm, ws, ci, cm, bias, dlog, skip, wih, send, recv, back, st, gi, gm, ds, gmt, xet,
    gs, gr, gt, hsem, lsem, s1, r1, s2, r2, *rest,
):
    dp = lax.axis_index("dp")
    z, yh, c, x = (lax.axis_index(a) for a in SEQ_CHAN)
    n = 2 * NZ
    q = z * 2 + yh
    nq, pq = lax.rem(q + 1, n), lax.rem(q + n - 1, n)
    corner = (c == 1) & (x == 3)
    barrier = pltpu.get_barrier_semaphore()

    def tell(**where):
        pl.semaphore_signal(barrier, inc=1, device_id=where, device_id_type=MESH)

    for off in range(1, 8):
        k = lax.rem(c * 4 + x + off, 8)
        tell(seq_2=k // 4, chan=lax.rem(k, 4))
    for off in (1, 3):
        k = lax.rem(yh * 2 + dp + off, 4)
        tell(seq_1=k // 2, dp=lax.rem(k, 2))
    for off in range(1, n):
        k = lax.rem(q + off, n)
        tell(seq_0=k // 2, seq_1=lax.rem(k, 2))

    @pl.when(c == 1)
    def _():
        tell(seq_0=pq // 2, seq_1=lax.rem(pq, 2), chan=3)

    @pl.when(corner)
    def _():
        for k in range(4):
            tell(seq_0=nq // 2, seq_1=lax.rem(nq, 2), chan=k)

    base = pl.multiple_of(PRE + (c * 4 + x) * 32, 16)
    loads = [pltpu.make_async_copy(piece, xe.at[pl.ds(base, 32), :], hsem.at[0])]
    loads.append(pltpu.make_async_copy(og, ogx.at[c], hsem.at[1]))
    pairs = ((wi_h, wi), (wm_h, wm), (ws_h, ws), (ci_h, ci), (cm_h, cm))
    pairs += ((bias_h, bias), (dlog_h, dlog), (skip_h, skip))
    for k, (src, dst) in enumerate(pairs):
        loads.append(pltpu.make_async_copy(src, dst, hsem.at[2 + k]))
    for d in loads:
        d.start()
    loads[0].wait()
    loads[1].wait()
    pl.semaphore_wait(
        barrier, jnp.where(corner, 7 + 2 + n - 1 + 5, jnp.where(c == 1, 7 + 2 + n, 7 + 2 + n - 1))
    )
    gather_phase(xe, ogx, gs, gr, gt)
    for d in loads[2:]:
        d.wait()
    acts = forward_phase(xe, ogx, wi, wm, ws, ci, cm, bias, dlog, wih, send)
    begin, turn, end = state_phases(send, st, recv, back, lsem, s1, r1, s2, r2)
    begin()
    local = local_phase(acts, dlog, skip)
    turn()
    for b in range(4):
        cols = slice(b * 640, (b + 1) * 640)
        xet[cols, :] = xe[:, cols].T
    end()
    later = carried_phase(acts, local, st, ci, cm, gi, gm, ds, gmt)
    sums_phase(
        norm, later, xet, gi, gm, ds, gmt, wih, wm, ws, mt, fat, fb, ig, *rest
    )


def whole(norm, *args):
    dma = pltpu.SemaphoreType.DMA
    n = 2 * NZ

    def vm(*shape):
        return pltpu.VMEM(shape, BF16)

    return pl.pallas_call(
        functools.partial(whole_kernel, norm),
        out_shape=(
            jax.ShapeDtypeStruct((8, 16, 128), F32),
            jax.ShapeDtypeStruct((2, 40, 128), F32),
            jax.ShapeDtypeStruct((2, 40, 256), F32),
            jax.ShapeDtypeStruct((32, D), BF16),
        ),
        in_specs=[pl.BlockSpec(memory_space=pltpu.HBM)] * 10,
        out_specs=(VM,) * 4,
        scratch_shapes=[
            vm(EXT, D), vm(2, TOK // 2, 2 * INNER), vm(D, 2 * INNER), vm(D, 2 * STATE), vm(10, D),
            pltpu.VMEM((4, 2 * INNER), F32), pltpu.VMEM((4, 2 * STATE), F32),
            pltpu.VMEM((1, 10), F32), pltpu.VMEM((1, 10), F32), pltpu.VMEM((1, 10), F32),
            vm(D, INNER), vm(n, CHUNK, STATE), vm(n, CHUNK, STATE), vm(n, 8 * HEADS, STATE),
            vm(n, 8 * HEADS, STATE), vm(EXT, INNER), vm(EXT, 2 * STATE), vm(EXT, 128), vm(8, 32, TOK),
            vm(D, EXT),
            dma((13,)), dma((13,)), dma((4,)), dma((10,)), dma((2,)),
            dma((n,)), dma((n,)), dma((n,)), dma((n,)),
            vm(2, 2, 16, D), vm(4, PRE, D), vm(8, 32, TOK),
            vm(2, 4, NZ, ROWS, 128), vm(2, 2, 4, ROWS, 128), vm(2, 2, NZ, ROWS, 128),
            vm(NZ, 4, ROWS, 128), vm(2, 4, ROWS, 128), vm(2, 2, ROWS, 128),
            vm(2, 4, ROWS, 128), vm(2, 4, ROWS, 128), vm(4, ROWS, 128), vm(4, ROWS, 128),
            vm(2, NZ, 2, 40, 128), vm(2, 2, 2, 40, 128), vm(2, 2, 1, 40, 128),
            vm(2, 2, 2, 40, 128), vm(2, 2, 2, 40, 128),
            pltpu.VMEM((2, 40, 128), F32), pltpu.VMEM((8, 16, 128), F32),
            pltpu.VMEM((2, 40, 256), F32),
            vm(2, 4, 2, 16, D), vm(4, 2, 16, D), vm(2, 16, D), vm(PRE, D), vm(PRE, D),
            dma((8,)), dma((8,)), dma((12,)), dma((12,)), dma((8,)), dma((8,)),
            dma((16,)), dma((16,)), dma((6,)), dma((6,)), dma(()), dma((4,)), dma((4,)), dma((4,)),
            dma((8,)), dma((8,)), dma((3,)), dma((3,)),
        ],
        compiler_params=pltpu.CompilerParams(
            collective_id=0, has_side_effects=True, vmem_limit_bytes=LIMIT
        ),
        name="whole",
    )(*args)


def finish_kernel(mt, fat, fb, ig, ig_o, iw_o, mw_o, sw_o):
    pick = one_hot(iota((HEADS, 128), 1) == iota((HEADS, 128), 0) + 96)
    for k in range(2):
        iw_o[:, k * INNER : k * INNER + 256] = fb[k]
        own = fat[k]
        iw_o[:, k * INNER + 256 : (k + 1) * INNER] = own[:, :64]
        sw_o[k * HEADS : (k + 1) * HEADS, :] = lax.dot_general(
            pick, own, (((1,), (1,)), ((), ())), preferred_element_type=F32,
            precision=lax.Precision.HIGHEST,
        )
    for j in range(8):
        mw_o[:, j * 32 : (j + 1) * 32] = mt[j, :10, 64:96]
    ig_o[...] = ig[...]


def finish(*args):
    return pl.pallas_call(
        finish_kernel,
        out_shape=(
            jax.ShapeDtypeStruct((32, D), BF16),
            jax.ShapeDtypeStruct((40, 2 * INNER), F32),
            jax.ShapeDtypeStruct((10, 2 * STATE), F32),
            jax.ShapeDtypeStruct((2 * HEADS, 40), F32),
        ),
        in_specs=[VM] * 4,
        out_specs=(VM,) * 4,
        compiler_params=pltpu.CompilerParams(vmem_limit_bytes=LIMIT),
        name="finish",
    )(*args)


def body(
    layer_input,
    inner_weight,
    mixer_weight,
    step_weight,
    conv_inner,
    conv_mixer,
    step_bias,
    decay_log,
    skip_gain,
    output_grad,
):
    norm = 1.0 / math.sqrt(8192)
    stepw = step_weight.T
    bias, dlog, skip = (v.reshape(1, -1) for v in (step_bias, decay_log, skip_gain))
    parts = whole(
        norm, layer_input[0], output_grad[0], inner_weight, mixer_weight, stepw, conv_inner,
        conv_mixer, bias, dlog, skip,
    )
    ig, iw, mw, sw = finish(*parts)
    return ig[None], iw, mw, sw.T


def solution(mesh):
    split = Mesh(
        mesh.devices.reshape(mesh.shape["dp"], 8, 2, 2, mesh.shape["chan"]),
        ("dp", "seq_0", "seq_1", "seq_2", "chan"),
    )
    placed = (
        P("dp", SEQ_CHAN, None),
        P(None, "chan"),
        P(),
        P(None, "chan"),
        P(None, "chan"),
        P(),
        P("chan"),
        P("chan"),
        P("chan"),
        P("dp", SEQ, "chan"),
    )
    return jax.shard_map(
        body,
        mesh=split,
        in_specs=placed,
        out_specs=(
            P("dp", SEQ_CHAN, None),
            P(DP_SEQ, "chan"),
            P(DP_SEQ_CHAN, None),
            P(DP_SEQ, "chan"),
        ),
        check_vma=False,
    )
```
